32 devices in a mesh: fsdp: 2 (over x), ctx: 4 (over z), tp: 4 (over y, core).
Axes of the slice: x: 2, y: 2, z: 4, core: 2. Of those that a mesh axis runs over, the one named last changes fastest.
Arguments:
- block_input: bfloat16 [2, 2048, 1024], P('fsdp', 'ctx'), may hold values from -6 to 6
- cotangent: bfloat16 [2, 2048, 1024], P('fsdp', 'ctx'), may hold values from -6 to 6
- seq_lengths: int32 [2], P('fsdp'), may hold values from 512 to 2048, as said below
- positions: int32 [2, 2048], P('fsdp', 'ctx'), may hold values from 0 to 2047, as said below
- w_qkv: float32 [1024, 2048], P('fsdp', 'tp'), may hold values from -0.1875 to 0.1875
- w_out: float32 [1024, 1024], P('tp', 'fsdp'), may hold values from -4 to 4
- w_gate_up: float32 [1024, 2, 4608], P('fsdp', None, 'tp'), may hold values from -0.1875 to 0.1875
- w_down: float32 [4608, 1024], P('tp', 'fsdp'), may hold values from -0.09375 to 0.09375
- gain_attn: float32 [1024], replicated, may hold values from 0.5 to 1.5
- gain_ffn: float32 [1024], replicated, may hold values from 0.5 to 1.5
- gain_query: float32 [64], replicated, may hold values from 0.5 to 1.5
- gain_key: float32 [64], replicated, may hold values from 0.5 to 1.5
- row_qkv_old: float32 [1024], P('fsdp'), may hold values from 409.6 to 40960
- col_qkv_old: float32 [2048], P('tp'), may hold values from 409.6 to 40960
- row_out_old: float32 [1024], P('tp'), may hold values from 0.6 to 60
- col_out_old: float32 [1024], P('fsdp'), may hold values from 0.6 to 60
- row_gate_up_old: float32 [1024], P('fsdp'), may hold values from 20.48 to 2048
- col_gate_up_old: float32 [2, 4608], P(None, 'tp'), may hold values from 20.48 to 2048
- row_down_old: float32 [4608], P('tp'), may hold values from 81.92 to 8192
- col_down_old: float32 [1024], P('fsdp'), may hold values from 81.92 to 8192
- var_attn_old: float32 [1024], replicated, may hold values from 819.2 to 81920
- var_ffn_old: float32 [1024], replicated, may hold values from 204.8 to 20480
- var_query_old: float32 [64], replicated, may hold values from 6553.6 to 655360
- var_key_old: float32 [64], replicated, may hold values from 3276.8 to 327680
Outputs:
- block_output: float32 [2, 2048, 1024], P('fsdp', 'ctx')
- input_grad: float32 [2, 2048, 1024], P('fsdp', 'ctx')
- grad_qkv: float32 [1024, 2048], P('fsdp', 'tp')
- grad_out: float32 [1024, 1024], P('tp', 'fsdp')
- grad_gate_up: float32 [1024, 2, 4608], P('fsdp', None, 'tp')
- grad_down: float32 [4608, 1024], P('tp', 'fsdp')
- grad_attn_gain: float32 [1024], replicated
- grad_ffn_gain: float32 [1024], replicated
- grad_query_gain: float32 [64], replicated
- grad_key_gain: float32 [64], replicated
- row_qkv: float32 [1024], P('fsdp')
- col_qkv: float32 [2048], P('tp')
- row_out: float32 [1024], P('tp')
- col_out: float32 [1024], P('fsdp')
- row_gate_up: float32 [1024], P('fsdp')
- col_gate_up: float32 [2, 4608], P(None, 'tp')
- row_down: float32 [4608], P('tp')
- col_down: float32 [1024], P('fsdp')
- var_attn: float32 [1024], replicated
- var_ffn: float32 [1024], replicated
- var_query: float32 [64], replicated
- var_key: float32 [64], replicated
- step_qkv: float32 [1024, 2048], P('fsdp', 'tp')
- step_out: float32 [1024, 1024], P('tp', 'fsdp')
- step_gate_up: float32 [1024, 2, 4608], P('fsdp', None, 'tp')
- step_down: float32 [4608, 1024], P('tp', 'fsdp')
- step_attn_gain: float32 [1024], replicated
- step_ffn_gain: float32 [1024], replicated
- step_query_gain: float32 [64], replicated
- step_key_gain: float32 [64], replicated
- update_rms: float32 [], replicated
The draws below stay inside these ranges and needn't reach their ends.
Inputs may be any that keep to these rules, and one draw needn't show every extreme that they name: seq_lengths[b] counts the real tokens of sequence b; some sequence has exactly 2048. positions count up by one from token to token and start at 0 at the first token and wherever a new document begins; some sequence holds a single document.
All inputs are finite; a program needn't handle non-finite values.
Results may differ from the reference program's by a relative error of at most 0.02.
The reference program's roundings to bfloat16 on the way count: a program that leaves them out, or rounds other values in their place, can miss the bound.
Values may be sent and summed in bfloat16 or wider, within the bound.
A program may use at most 192 MiB of HBM per device.

```python
import math
import jax
import jax.numpy as jnp
from jax import lax

D = 1024
QUERY_HEADS = 16
KEY_VALUE_HEADS = 8
HEAD_SIZE = 64
FF = 4608
BATCH = 2
SEQUENCE_TOKENS = 2048
QKV = 2048


def draw_seq_lengths(key, part):
    first, second = jax.random.split(key)
    drawn = jax.random.randint(first, (BATCH,), SEQUENCE_TOKENS // 4, SEQUENCE_TOKENS + 1, dtype=jnp.int32)
    chosen = jax.random.randint(second, (), 0, BATCH, dtype=jnp.int32)
    return jnp.where(jnp.arange(BATCH, dtype=jnp.int32) == chosen, SEQUENCE_TOKENS, drawn).astype(jnp.int32)


def draw_positions(key, part):
    first, second = jax.random.split(key)
    spacing = max(2, SEQUENCE_TOKENS // 16)
    begins = jax.random.randint(first, (BATCH, SEQUENCE_TOKENS), 0, spacing, dtype=jnp.int32) == 0
    chosen = jax.random.randint(second, (), 0, BATCH, dtype=jnp.int32)
    counter = jnp.broadcast_to(jnp.arange(SEQUENCE_TOKENS, dtype=jnp.int32)[None, :], (BATCH, SEQUENCE_TOKENS))
    other_rows = jnp.arange(BATCH, dtype=jnp.int32)[:, None] != chosen
    begins = begins & other_rows | (counter == 0)
    latest = lax.cummax(jnp.where(begins, counter, 0), axis=1)
    return (counter - latest).astype(jnp.int32)


def level_of(key, dims, pieces, smallest, high):
    def one(dim, blocks):
        heights = jax.random.uniform(jax.random.fold_in(jax.random.fold_in(key, 6), dim), (blocks,), jnp.float32, smallest / len(pieces), high / len(pieces))
        return jnp.repeat(jnp.exp(heights), dims[dim] // blocks).reshape((-1,) + (1,) * (len(dims) - dim - 1))

    factor_of = one(*pieces[0])
    for cut in pieces[1:]:
        factor_of = factor_of * one(*cut)
    return factor_of


def normal_values(stream_key, shape, deviation, most, cuts=(), kind=jnp.bfloat16):
    result = jax.random.normal(stream_key, shape, jnp.float32) * deviation
    if len(cuts) > 0:
        result = level_of(stream_key, shape, cuts, -0.22, 0.18) * result
    return jnp.clip(result, min=-most, max=most).astype(kind)


def setup_inputs(seed: int = 0) -> dict:
    keys = jax.random.split(jax.random.key(seed), 25)
    return {
        "block_input": normal_values(keys[0], (BATCH, SEQUENCE_TOKENS, D), 1.0, 6.0, ((0, 2), (1, 4))),
        "cotangent": normal_values(keys[1], (BATCH, SEQUENCE_TOKENS, D), 1.0, 6.0, ((0, 2), (1, 4))),
        "seq_lengths": draw_seq_lengths(jax.random.fold_in(keys[24], 71), 0),
        "positions": draw_positions(jax.random.fold_in(keys[24], 71), 0),
        "w_qkv": normal_values(keys[4], (D, QKV), D ** -0.5, 0.1875, ((0, 2), (1, 4)), jnp.float32),
        "w_out": normal_values(keys[5], (QUERY_HEADS * HEAD_SIZE, D), (max(1, 4 * QUERY_HEADS * HEAD_SIZE // SEQUENCE_TOKENS)) ** -0.5, 4.0, ((0, 4), (1, 2)), jnp.float32),
        "w_gate_up": normal_values(keys[6], (D, 2, FF), D ** -0.5, 0.1875, ((0, 2), (2, 4)), jnp.float32),
        "w_down": normal_values(keys[7], (FF, D), FF ** -0.5, 0.09375, ((0, 4), (1, 2)), jnp.float32),
        "gain_attn": jnp.clip(1.0 + 0.1 * jax.random.normal(keys[8], (D,), jnp.float32), 0.5, 1.5),
        "gain_ffn": jnp.clip(1.0 + 0.1 * jax.random.normal(keys[9], (D,), jnp.float32), 0.5, 1.5),
        "gain_query": jnp.clip(1.0 + 0.1 * jax.random.normal(keys[10], (HEAD_SIZE,), jnp.float32), 0.5, 1.5),
        "gain_key": jnp.clip(1.0 + 0.1 * jax.random.normal(keys[11], (HEAD_SIZE,), jnp.float32), 0.5, 1.5),
        "row_qkv_old": jnp.clip(jnp.exp(math.log(40960.0) - 4.6051702 * jax.random.uniform(keys[12], (D,), jnp.float32) ** level_of(keys[12], (D,), ((0, 2),), -0.2, 0.2)), 409.6, 40960.0),
        "col_qkv_old": jnp.clip(jnp.exp(math.log(40960.0) - 4.6051702 * jax.random.uniform(keys[13], (QKV,), jnp.float32) ** level_of(keys[13], (QKV,), ((0, 4),), -0.2, 0.2)), 409.6, 40960.0),
        "row_out_old": jnp.clip(jnp.exp(math.log(60.0) - 4.6051701 * jax.random.uniform(keys[14], (QUERY_HEADS * HEAD_SIZE,), jnp.float32) ** level_of(keys[14], (QUERY_HEADS * HEAD_SIZE,), ((0, 4),), -0.2, 0.2)), 0.6, 60.0),
        "col_out_old": jnp.clip(jnp.exp(math.log(60.0) - 4.6051701 * jax.random.uniform(keys[15], (D,), jnp.float32) ** level_of(keys[15], (D,), ((0, 2),), -0.2, 0.2)), 0.6, 60.0),
        "row_gate_up_old": jnp.clip(jnp.exp(math.log(2048.0) - 4.6051702 * jax.random.uniform(keys[16], (D,), jnp.float32) ** level_of(keys[16], (D,), ((0, 2),), -0.2, 0.2)), 20.48, 2048.0),
        "col_gate_up_old": jnp.clip(jnp.exp(math.log(2048.0) - 4.6051702 * jax.random.uniform(keys[17], (2, FF), jnp.float32) ** level_of(keys[17], (2, FF), ((1, 4),), -0.2, 0.2)), 20.48, 2048.0),
        "row_down_old": jnp.clip(jnp.exp(math.log(8192.0) - 4.6051702 * jax.random.uniform(keys[18], (FF,), jnp.float32) ** level_of(keys[18], (FF,), ((0, 4),), -0.2, 0.2)), 81.92, 8192.0),
        "col_down_old": jnp.clip(jnp.exp(math.log(8192.0) - 4.6051702 * jax.random.uniform(keys[19], (D,), jnp.float32) ** level_of(keys[19], (D,), ((0, 2),), -0.2, 0.2)), 81.92, 8192.0),
        "var_attn_old": jnp.clip(jnp.exp(jax.random.uniform(keys[20], (D,), jnp.float32, math.log(819.2), math.log(81920.0))), 819.2, 81920.0),
        "var_ffn_old": jnp.clip(jnp.exp(jax.random.uniform(keys[21], (D,), jnp.float32, math.log(204.8), math.log(20480.0))), 204.8, 20480.0),
        "var_query_old": jnp.clip(jnp.exp(jax.random.uniform(keys[22], (HEAD_SIZE,), jnp.float32, math.log(6553.6), math.log(655360.0))), 6553.6, 655360.0),
        "var_key_old": jnp.clip(jnp.exp(jax.random.uniform(keys[23], (HEAD_SIZE,), jnp.float32, math.log(3276.8), math.log(327680.0))), 3276.8, 327680.0),
    }


EPS = 1e-05
THETA = 1000000.0
DECAY = 0.5
CLIP = 0.15
RATE = 1.0
NEG = -1e+30
HIGH = lax.Precision.HIGHEST

@jax.custom_vjp
def lower_precision(v):
    return lax.optimization_barrier(v.astype(jnp.bfloat16)).astype(jnp.float32)

@jax.custom_vjp
def lower_backward(v):
    return v

def low_keep(v):
    return (lower_precision(v), None)

def low_pass(kept, grad):
    return (grad,)

def back_keep(v):
    return (v, None)

def back_low(kept, grad):
    return (lower_precision(grad),)
lower_precision.defvjp(low_keep, low_pass)
lower_backward.defvjp(back_keep, back_low)

def matrix_multiply(left, right):
    return jnp.dot(left, right, precision=HIGH, preferred_element_type=jnp.float32)

def rms_norm(values, gain):
    return values * lax.rsqrt(lax.optimization_barrier(jnp.mean(values * values, axis=-1, keepdims=True)) + EPS) * gain

def rotate(values, cos_t, sin_t):
    half = values.shape[-1] // 2
    turned = jnp.concatenate([-values[..., half:], values[..., :half]], axis=-1)
    return values * cos_t + turned * sin_t

def tables(pos_row, head_dim):
    half = head_dim // 2
    freq = jnp.exp(jnp.arange(half, dtype=jnp.float32) * (-2.0 * math.log(THETA) / head_dim))
    angle = pos_row.astype(jnp.float32)[:, None] * freq[None, :]
    angle = jnp.concatenate([angle, angle], axis=-1)
    return (jnp.cos(angle), jnp.sin(angle))

def head_part(item):
    query_h, key_h, value_h, sequence_length = item
    scores = jnp.einsum('gid,jd->gij', query_h, key_h, precision=HIGH) * (1.0 / math.sqrt(HEAD_SIZE))
    scores = lower_backward(scores)
    rows_idx = lax.broadcasted_iota(jnp.int32, (SEQUENCE_TOKENS, SEQUENCE_TOKENS), 0)
    cols_idx = lax.broadcasted_iota(jnp.int32, (SEQUENCE_TOKENS, SEQUENCE_TOKENS), 1)
    visible = (cols_idx <= rows_idx) & (cols_idx < sequence_length)
    scores = jnp.where(visible[None], scores, NEG)
    top = lax.optimization_barrier(jnp.max(scores, axis=-1, keepdims=True))
    expd = jnp.exp(scores - top)
    probs = expd / lax.optimization_barrier(jnp.sum(expd, axis=-1, keepdims=True))
    return jnp.einsum('gij,jd->gid', lower_precision(probs), value_h, precision=HIGH)

def layer(params, x_seq, pos_seq, sequence_length):
    query_weight, wo, wg, wd, gain_a, gain_f, gain_q, gain_k = params
    query_group = QUERY_HEADS // KEY_VALUE_HEADS
    cos_t, sin_t = tables(pos_seq, HEAD_SIZE)
    hidden_first = lower_precision(rms_norm(x_seq, gain_a))
    query_key_value = lower_backward(matrix_multiply(hidden_first, lower_precision(query_weight))).reshape(SEQUENCE_TOKENS, KEY_VALUE_HEADS, query_group + 2, HEAD_SIZE)
    queries = lower_precision(rotate(rms_norm(query_key_value[:, :, :query_group], gain_q), cos_t[:, None, None, :], sin_t[:, None, None, :]))
    keys_rot = lower_precision(rotate(rms_norm(query_key_value[:, :, query_group], gain_k), cos_t[:, None, :], sin_t[:, None, :]))
    values = lower_precision(query_key_value[:, :, query_group + 1])
    sequence_lengths = jnp.full((KEY_VALUE_HEADS,), sequence_length, dtype=jnp.int32)
    heads = lax.map(jax.checkpoint(head_part), (queries.transpose(1, 2, 0, 3), keys_rot.transpose(1, 0, 2), values.transpose(1, 0, 2), sequence_lengths))
    attn_heads = lower_backward(lower_precision(heads.transpose(2, 0, 1, 3).reshape(SEQUENCE_TOKENS, QUERY_HEADS * HEAD_SIZE)))
    attn = lower_backward(matrix_multiply(attn_heads, lower_precision(wo)))
    resid = x_seq + attn
    h_two = lower_precision(rms_norm(resid, gain_f))
    gate_up = lower_backward(matrix_multiply(h_two, lower_precision(wg).reshape(D, 2 * FF)))
    hidden = lower_precision(jax.nn.silu(gate_up[:, :FF]) * gate_up[:, FF:])
    return resid + matrix_multiply(hidden, lower_precision(wd))

def factored(grad, row_old, col_old):
    squares = grad * grad
    row_new = DECAY * row_old + (1.0 - DECAY) * lax.optimization_barrier(jnp.mean(squares, axis=1))
    col_new = DECAY * col_old + (1.0 - DECAY) * lax.optimization_barrier(jnp.mean(squares, axis=0))
    approx = row_new[:, None] * col_new[None, :] / jnp.mean(row_new)
    return (row_new, col_new, grad * lax.rsqrt(approx))

def reference(block_input, cotangent, seq_lengths, positions, w_qkv, w_out, w_gate_up, w_down, gain_attn, gain_ffn, gain_query, gain_key, row_qkv_old, col_qkv_old, row_out_old, col_out_old, row_gate_up_old, col_gate_up_old, row_down_old, col_down_old, var_attn_old, var_ffn_old, var_query_old, var_key_old):
    params = (w_qkv, w_out, w_gate_up, w_down, gain_attn, gain_ffn, gain_query, gain_key)
    inputs32 = block_input.astype(jnp.float32)
    grads32 = cotangent.astype(jnp.float32)
    zeros_tree = jax.tree.map(jnp.zeros_like, params)

    def one_seq(carry, item):
        x_seq, d_seq, pos_seq, sequence_length = item
        out_seq, pull = jax.vjp(lambda inner, x_in: layer(inner, x_in, pos_seq, sequence_length), params, x_seq)
        d_params, d_input = pull(d_seq)
        return (jax.tree.map(lambda left, right: left + right, carry, d_params), (out_seq, d_input))
    grads, (block_output, input_grad) = lax.scan(one_seq, zeros_tree, (inputs32, grads32, positions, seq_lengths))
    g_qkv, g_out, g_gu, g_down, g_attn, g_ffn, g_query, g_key = grads
    row_qkv, col_qkv, raw_qkv = factored(g_qkv, row_qkv_old, col_qkv_old)
    row_out, col_out, raw_out = factored(g_out, row_out_old, col_out_old)
    row_gu, col_gu_flat, raw_gu = factored(g_gu.reshape(D, 2 * FF), row_gate_up_old, col_gate_up_old.reshape(2 * FF))
    row_down, col_down, raw_down = factored(g_down, row_down_old, col_down_old)
    raw_gu = raw_gu.reshape(D, 2, FF)
    col_gu = col_gu_flat.reshape(2, FF)
    var_attn = DECAY * var_attn_old + (1.0 - DECAY) * g_attn * g_attn
    var_ffn = DECAY * var_ffn_old + (1.0 - DECAY) * g_ffn * g_ffn
    var_query = DECAY * var_query_old + (1.0 - DECAY) * g_query * g_query
    var_key = DECAY * var_key_old + (1.0 - DECAY) * g_key * g_key
    raws = [raw_qkv, raw_out, raw_gu, raw_down, g_attn * lax.rsqrt(var_attn), g_ffn * lax.rsqrt(var_ffn), g_query * lax.rsqrt(var_query), g_key * lax.rsqrt(var_key)]
    count = D * QKV + QUERY_HEADS * HEAD_SIZE * D + 2 * D * FF + FF * D + 2 * D + 2 * HEAD_SIZE
    total = sum((jnp.sum(raw * raw) for raw in raws))
    update_rms = jnp.sqrt(total / count)
    clip = jnp.maximum(1.0, update_rms / CLIP)
    olds = [w_qkv, w_out, w_gate_up, w_down, gain_attn, gain_ffn, gain_query, gain_key]
    steps = [-RATE * jnp.sqrt(jnp.mean(weight * weight)) * raw / clip for weight, raw in zip(olds, raws)]
    return (block_output, input_grad, g_qkv, g_out, g_gu, g_down, g_attn, g_ffn, g_query, g_key, row_qkv, col_qkv, row_out, col_out, row_gu, col_gu, row_down, col_down, var_attn, var_ffn, var_query, var_key, steps[0], steps[1], steps[2], steps[3], steps[4], steps[5], steps[6], steps[7], update_rms)
```

```python
import functools
import math

import jax
import jax.numpy as jnp
from jax import lax
from jax.experimental import pallas as pl
from jax.experimental.pallas import tpu as pltpu
from jax.sharding import PartitionSpec as P

D = 1024
QUERY_HEADS = 16
KEY_VALUE_HEADS = 8
HEAD_SIZE = 64
FF = 4608
QKV = 2048

EPS = 1e-05
THETA = 1000000.0
DECAY = 0.5
CLIP = 0.15
RATE = 1.0

BF = jnp.bfloat16
F32 = jnp.float32
GROUP = QUERY_HEADS // KEY_VALUE_HEADS
LANES = (GROUP + 2) * HEAD_SIZE
KEY_TILE = 256


def mm(left, right, left_dim, right_dim):
    return lax.dot_general(
        left, right, (((left_dim,), (right_dim,)), ((), ())), preferred_element_type=F32
    )


def params(vmem=48 << 20):
    return pltpu.CompilerParams(vmem_limit_bytes=vmem)


def prep_kernel(qkv_ref, cos_ref, sin_ref, gq_ref, gk_ref, q_ref, kv_ref):
    half = HEAD_SIZE // 2
    cos_t, sin_t = cos_ref[...], sin_ref[...]
    for piece in range(GROUP + 1):
        rows = qkv_ref[piece * HEAD_SIZE : (piece + 1) * HEAD_SIZE, :]
        inv = lax.rsqrt(jnp.mean(rows * rows, axis=0, keepdims=True) + EPS)
        gain = gq_ref[...] if piece < GROUP else gk_ref[...]
        normed = rows * inv * gain
        low, high = normed[:half], normed[half:]
        out_low = low * cos_t - high * sin_t
        out_high = high * cos_t + low * sin_t
        if piece < GROUP:
            scale = 1.0 / math.sqrt(HEAD_SIZE)
            base = piece * HEAD_SIZE
            q_ref[base : base + half, :] = (out_low.astype(BF) * scale).astype(BF)
            q_ref[base + half : base + 2 * half, :] = (out_high.astype(BF) * scale).astype(BF)
        else:
            kv_ref[:half, :] = out_low.astype(BF)
            kv_ref[half : 2 * half, :] = out_high.astype(BF)
    kv_ref[HEAD_SIZE:, :] = qkv_ref[(GROUP + 1) * HEAD_SIZE :, :].astype(BF)


def prep(qkv_t, cos_t, sin_t, gain_q, gain_k):
    rows, tokens = qkv_t.shape
    groups = rows // LANES
    half = HEAD_SIZE // 2
    fixed = lambda g: (0, 0)
    return pl.pallas_call(
        prep_kernel,
        grid=(groups,),
        in_specs=[
            pl.BlockSpec((LANES, tokens), lambda g: (g, 0)),
            pl.BlockSpec((half, tokens), fixed),
            pl.BlockSpec((half, tokens), fixed),
            pl.BlockSpec((HEAD_SIZE, 1), fixed),
            pl.BlockSpec((HEAD_SIZE, 1), fixed),
        ],
        out_specs=[
            pl.BlockSpec((GROUP * HEAD_SIZE, tokens), lambda g: (g, 0)),
            pl.BlockSpec((2 * HEAD_SIZE, tokens), lambda g: (g, 0)),
        ],
        out_shape=[
            jax.ShapeDtypeStruct((groups * GROUP * HEAD_SIZE, tokens), BF),
            jax.ShapeDtypeStruct((groups * 2 * HEAD_SIZE, tokens), BF),
        ],
        cost_estimate=pl.CostEstimate(
            flops=20 * rows * tokens, bytes_accessed=6 * rows * tokens, transcendentals=0
        ),
        compiler_params=params(),
        name="prep",
    )(qkv_t, cos_t, sin_t, gain_q, gain_k)


def prep_back_kernel(parts, *refs):
    qkv_ref, cos_ref, sin_ref, gq_ref, gk_ref, dq_ref = refs[:6]
    dkv_refs = refs[6 : 6 + parts]
    out_ref, sum_q_ref, sum_k_ref = refs[6 + parts :]
    half = HEAD_SIZE // 2
    cos_t, sin_t = cos_ref[...], sin_ref[...]
    d_kv = dkv_refs[0][...]
    for ref in dkv_refs[1:]:
        d_kv = d_kv + ref[...].astype(F32)

    @pl.when(pl.program_id(0) == 0)
    def _():
        sum_q_ref[...] = jnp.zeros_like(sum_q_ref)
        sum_k_ref[...] = jnp.zeros_like(sum_k_ref)

    for piece in range(GROUP + 1):
        base = piece * HEAD_SIZE
        rows = qkv_ref[base : base + HEAD_SIZE, :]
        inv = lax.rsqrt(jnp.mean(rows * rows, axis=0, keepdims=True) + EPS)
        unit = rows * inv
        if piece < GROUP:
            grad = dq_ref[base : base + HEAD_SIZE, :] * (1.0 / math.sqrt(HEAD_SIZE))
            gain, sum_ref = gq_ref[...], sum_q_ref
        else:
            grad = d_kv[:HEAD_SIZE]
            gain, sum_ref = gk_ref[...], sum_k_ref
        low, high = grad[:half], grad[half:]
        turned = jnp.concatenate([low * cos_t + high * sin_t, high * cos_t - low * sin_t], axis=0)
        sum_ref[...] += jnp.sum(turned * unit, axis=1, keepdims=True)
        scaled = turned * gain
        mean = jnp.mean(scaled * unit, axis=0, keepdims=True)
        out_ref[base : base + HEAD_SIZE, :] = ((scaled - unit * mean) * inv).astype(BF)
    out_ref[(GROUP + 1) * HEAD_SIZE :, :] = d_kv[HEAD_SIZE:].astype(BF)


def prep_back(qkv_t, cos_t, sin_t, gain_q, gain_k, d_q, d_kv_parts):
    rows, tokens = qkv_t.shape
    groups = rows // LANES
    half = HEAD_SIZE // 2
    fixed = lambda g: (0, 0)
    block = lambda size: pl.BlockSpec((size, tokens), lambda g: (g, 0))
    return pl.pallas_call(
        functools.partial(prep_back_kernel, len(d_kv_parts)),
        grid=(groups,),
        in_specs=[
            block(LANES),
            pl.BlockSpec((half, tokens), fixed),
            pl.BlockSpec((half, tokens), fixed),
            pl.BlockSpec((HEAD_SIZE, 1), fixed),
            pl.BlockSpec((HEAD_SIZE, 1), fixed),
            block(GROUP * HEAD_SIZE),
        ]
        + [block(2 * HEAD_SIZE)] * len(d_kv_parts),
        out_specs=[
            block(LANES),
            pl.BlockSpec((HEAD_SIZE, 128), fixed),
            pl.BlockSpec((HEAD_SIZE, 128), fixed),
        ],
        out_shape=[
            jax.ShapeDtypeStruct((rows, tokens), BF),
            jax.ShapeDtypeStruct((HEAD_SIZE, 128), F32),
            jax.ShapeDtypeStruct((HEAD_SIZE, 128), F32),
        ],
        cost_estimate=pl.CostEstimate(
            flops=30 * rows * tokens, bytes_accessed=9 * rows * tokens, transcendentals=0
        ),
        compiler_params=params(),
        name="prep_back",
    )(qkv_t, cos_t, sin_t, gain_q, gain_k, d_q, *d_kv_parts)


def tiles_of(diagonal, tokens):
    for key_start in range(0, tokens, KEY_TILE):
        yield key_start, key_start if diagonal else 0


def tile_probs(kv_ref, query, key_start, query_start, valid, diagonal):
    keys = kv_ref[:HEAD_SIZE, key_start : key_start + KEY_TILE]
    scores = mm(keys, query, 0, 0)
    key_index = key_start + lax.broadcasted_iota(jnp.int32, scores.shape, 0)
    visible = key_index < valid
    if diagonal:
        query_index = query_start + lax.broadcasted_iota(jnp.int32, scores.shape, 1)
        visible = visible & (key_index <= query_index)
    return keys, visible, jnp.exp(scores)


def attend_kernel(diagonal, valid_ref, q_ref, kv_ref, *refs):
    if diagonal:
        acc_ref, sum_ref = refs
        acc_ref[...] = jnp.zeros_like(acc_ref)
        sum_ref[...] = jnp.zeros_like(sum_ref)
    else:
        acc_in_ref, sum_in_ref, acc_ref, sum_ref = refs
        acc_ref[...] = acc_in_ref[...]
        sum_ref[...] = sum_in_ref[...]
    valid = valid_ref[0]
    tokens = q_ref.shape[1]

    @pl.when(valid > 0)
    def _():
        for key_start, query_start in tiles_of(diagonal, tokens):
            query = q_ref[:, query_start:]
            keys, visible, raised = tile_probs(
                kv_ref, query, key_start, query_start, valid, diagonal
            )
            probs = jnp.where(visible, raised, 0.0)
            sum_ref[:, query_start:] += jnp.sum(probs, axis=0, keepdims=True)
            values = kv_ref[HEAD_SIZE:, key_start : key_start + KEY_TILE]
            acc_ref[:, query_start:] += mm(values, probs.astype(BF), 1, 0)


def attend(diagonal, valid, q_t, kv_t, state):
    rows, tokens = q_t.shape
    heads = rows // HEAD_SIZE
    per_head = pl.BlockSpec((HEAD_SIZE, tokens), lambda h: (h, 0))
    sums = pl.BlockSpec((8, tokens), lambda h: (h, 0))
    carried = [] if diagonal else [per_head, sums]
    return pl.pallas_call(
        functools.partial(attend_kernel, diagonal),
        grid=(heads,),
        in_specs=[
            pl.BlockSpec(memory_space=pltpu.SMEM),
            per_head,
            pl.BlockSpec((2 * HEAD_SIZE, tokens), lambda h: (h // GROUP, 0)),
        ]
        + carried,
        out_specs=[per_head, sums],
        out_shape=[
            jax.ShapeDtypeStruct((rows, tokens), F32),
            jax.ShapeDtypeStruct((heads * 8, tokens), F32),
        ],
        input_output_aliases={} if diagonal else {3: 0, 4: 1},
        cost_estimate=pl.CostEstimate(
            flops=4 * rows * tokens * tokens,
            bytes_accessed=10 * rows * tokens,
            transcendentals=heads * tokens * tokens,
        ),
        compiler_params=params(),
        name="attend",
    )(valid, q_t, kv_t, *state)


def attend_back_kernel(diagonal, first, valid_ref, q_ref, kv_ref, out_ref, sum_ref, do_ref, *refs):
    if first:
        dq_ref, dkv_ref, dkv_acc = refs
        dq_ref[...] = jnp.zeros_like(dq_ref)
    else:
        dq_in_ref, dq_ref, dkv_ref, dkv_acc = refs
        dq_ref[...] = dq_in_ref[...]
    head = pl.program_id(0)
    valid = valid_ref[0]
    tokens = q_ref.shape[1]

    @pl.when(head % GROUP == 0)
    def _():
        dkv_acc[...] = jnp.zeros_like(dkv_acc)

    @pl.when(valid > 0)
    def _():
        inverse = 1.0 / sum_ref[0:1, :]
        delta = jnp.sum(do_ref[...].astype(F32) * out_ref[...], axis=0, keepdims=True)
        for key_start, query_start in tiles_of(diagonal, tokens):
            query = q_ref[:, query_start:]
            grads = do_ref[:, query_start:]
            keys, visible, raised = tile_probs(
                kv_ref, query, key_start, query_start, valid, diagonal
            )
            probs = jnp.where(visible, raised * inverse[:, query_start:], 0.0)
            span = slice(key_start, key_start + KEY_TILE)
            values = kv_ref[HEAD_SIZE:, span]
            d_probs = mm(values, grads, 0, 0)
            d_scores = (probs * (d_probs - delta[:, query_start:])).astype(BF)
            dq_ref[:, query_start:] += mm(keys, d_scores, 1, 0)
            dkv_acc[:HEAD_SIZE, span] += mm(query, d_scores, 1, 1)
            dkv_acc[HEAD_SIZE:, span] += mm(grads, probs.astype(BF), 1, 1)

    @pl.when(head % GROUP == GROUP - 1)
    def _():
        dkv_ref[...] = dkv_acc[...].astype(dkv_ref.dtype)


def attend_back(diagonal, valid, q_t, kv_t, out_t, sums, d_out_t, d_q):
    rows, tokens = q_t.shape
    heads = rows // HEAD_SIZE
    first = d_q is None
    per_head = pl.BlockSpec((HEAD_SIZE, tokens), lambda h: (h, 0))
    per_group = pl.BlockSpec((2 * HEAD_SIZE, tokens), lambda h: (h // GROUP, 0))
    return pl.pallas_call(
        functools.partial(attend_back_kernel, diagonal, first),
        grid=(heads,),
        in_specs=[
            pl.BlockSpec(memory_space=pltpu.SMEM),
            per_head,
            per_group,
            per_head,
            pl.BlockSpec((8, tokens), lambda h: (h, 0)),
            per_head,
        ]
        + ([] if first else [per_head]),
        out_specs=[per_head, per_group],
        out_shape=[
            jax.ShapeDtypeStruct((rows, tokens), F32),
            jax.ShapeDtypeStruct(kv_t.shape, F32 if diagonal else BF),
        ],
        scratch_shapes=[pltpu.VMEM((2 * HEAD_SIZE, tokens), F32)],
        input_output_aliases={} if first else {6: 0},
        cost_estimate=pl.CostEstimate(
            flops=10 * rows * tokens * tokens,
            bytes_accessed=14 * rows * tokens,
            transcendentals=heads * tokens * tokens,
        ),
        compiler_params=params(),
        name="attend_back",
    )(valid, q_t, kv_t, out_t, sums, d_out_t, *([] if first else [d_q]))


def unit_rows(values):
    inv = lax.rsqrt(jnp.mean(values * values, axis=-1, keepdims=True) + EPS)
    return values * inv, inv


def norm_back(unit, inv, gain, grad):
    scaled = grad * gain
    return (scaled - unit * jnp.mean(scaled * unit, axis=-1, keepdims=True)) * inv


def kept(value):
    return lax.optimization_barrier(value)


def on_device(
    sizes,
    block_input,
    cotangent,
    seq_lengths,
    positions,
    w_qkv,
    w_out,
    w_gate_up,
    w_down,
    gain_attn,
    gain_ffn,
    gain_query,
    gain_key,
    row_qkv_old,
    col_qkv_old,
    row_out_old,
    col_out_old,
    row_gate_up_old,
    col_gate_up_old,
    row_down_old,
    col_down_old,
    var_attn_old,
    var_ffn_old,
    var_query_old,
    var_key_old,
):
    n_fsdp, n_ctx, n_tp = sizes["fsdp"], sizes["ctx"], sizes["tp"]
    paired = n_fsdp == 2
    me_f, me_z, me_t = (lax.axis_index(name) for name in ("fsdp", "ctx", "tp"))
    tokens = block_input.shape[1]
    half = tokens // 2
    mine_row = (me_t % 2) * half
    other_row = half - mine_row

    def turn(values):
        if not paired:
            return values
        size = values.shape[-1] // 2
        swapped = jnp.concatenate([values[..., size:], values[..., :size]], axis=-1)
        return jnp.where(me_f == 0, values, swapped)

    def over(values, axis, pairs):
        return lax.ppermute(values, axis, pairs)

    def to_core(values):
        return over(values, "tp", [(i, i ^ 1) for i in range(n_tp)])

    def to_pair(values):
        return over(values, "fsdp", [(0, 1), (1, 0)])

    def gather_weight(shard, axis):
        if not paired:
            return lax.all_gather(shard, "fsdp", axis=axis, tiled=True)
        return jnp.concatenate([shard, to_pair(shard)], axis=axis)

    def gather_split(shard, axis):
        if not paired or n_ctx % 2:
            return gather_weight(shard, axis)
        size = shard.shape[0] // 2
        odd = me_z % 2
        want = lax.dynamic_slice_in_dim(shard, odd * size, size, 0)
        direct = to_pair(want)
        routed = over(direct, "ctx", [(i, i ^ 1) for i in range(n_ctx)])
        first = jnp.where(odd == 0, direct, routed)
        second = jnp.where(odd == 0, routed, direct)
        other = jnp.concatenate([first, second], axis=0)
        return jnp.concatenate([shard, other], axis=axis)

    def sum_tp(mine, other_low):
        total = mine + to_core(other_low).astype(F32)
        step = 2
        while step < n_tp:
            low = kept(total.astype(BF))
            pairs = [(i, i ^ step) for i in range(n_tp)]
            total = low.astype(F32) + over(low, "tp", pairs).astype(F32)
            step *= 2
        return total

    def whole_rows(values):
        other = to_core(values)
        first = jnp.where(mine_row == 0, values, other)
        second = jnp.where(mine_row == 0, other, values)
        return jnp.concatenate([first, second], axis=0)

    def rows_of(values, start):
        return lax.dynamic_slice_in_dim(values, start, half, 0)

    def line_sum(part):
        if n_ctx != 4:
            return kept(lax.psum(part.astype(F32), "ctx").astype(BF))
        inner = kept((part.astype(F32) + over(part, "ctx", [(0, 1), (3, 2)]).astype(F32)).astype(BF))
        across = over(inner, "ctx", [(1, 2), (2, 1)])
        total = kept((inner.astype(F32) + across.astype(F32)).astype(BF))
        back = over(total, "ctx", [(1, 0), (2, 3)])
        at_end = (me_z == 0) | (me_z == n_ctx - 1)
        return kept(jnp.where(at_end, back, total))

    def reduce_grad(make, axis):
        if not paired:
            whole = make(None)
            return line_sum(lax.psum_scatter(whole, "fsdp", scatter_dimension=axis, tiled=True).astype(BF))
        theirs = to_pair(make(1).astype(BF))
        return line_sum(kept((make(0) + theirs.astype(F32)).astype(BF)))

    def part_of(values, part):
        if part is None:
            return values
        size = values.shape[-1] // 2
        return values[..., part * size : (part + 1) * size]

    full_qkv = gather_weight(w_qkv.astype(BF), 0)
    full_out = gather_weight(w_out.astype(BF), 1)
    shard = w_gate_up.shape[0]
    ff_local = w_gate_up.shape[2]
    flat_gate_up = gather_split(w_gate_up.astype(BF).reshape(shard, 2 * ff_local), 0)
    full_down = gather_split(w_down.astype(BF), 1)

    inputs32 = turn(block_input[0].astype(F32))
    grad_rows = turn(cotangent[0])
    gain_a, gain_f = turn(gain_attn), turn(gain_ffn)
    unit_one, inv_one = unit_rows(inputs32)
    h_one = (unit_one * gain_a).astype(BF)
    freq = jnp.exp(
        jnp.arange(HEAD_SIZE // 2, dtype=F32) * (-2.0 * math.log(THETA) / HEAD_SIZE)
    )
    angle = freq[:, None] * positions[0].astype(F32)[None, :]
    cos_t, sin_t = jnp.cos(angle), jnp.sin(angle)
    gain_q, gain_k = gain_query[:, None], gain_key[:, None]
    qkv_t = mm(full_qkv, h_one, 0, 1)
    q_t, kv_t = prep(qkv_t, cos_t, sin_t, gain_q, gain_k)

    length = seq_lengths[0]
    kv_blocks, valids = [], []
    for back in range(n_ctx):
        moved = kv_t
        if back > 0:
            moved = over(kv_t, "ctx", [(i, i + back) for i in range(n_ctx - back)])
        kv_blocks.append(moved)
        count = jnp.clip(length - (me_z - back) * tokens, 0, tokens)
        valids.append(jnp.where(me_z >= back, count, 0).astype(jnp.int32).reshape(1))
    state = []
    for back in range(n_ctx):
        state = attend(back == 0, valids[back], q_t, kv_blocks[back], state)
    acc_t, sums = state
    heads = acc_t.shape[0] // HEAD_SIZE
    inverse = (1.0 / sums.reshape(heads, 8, tokens)[:, :1, :])
    out_t = (acc_t.reshape(heads, HEAD_SIZE, tokens) * inverse).reshape(acc_t.shape)
    attn_t = kept(out_t.astype(BF))

    def cols_of(values, start):
        return lax.dynamic_slice_in_dim(values, start, half, 1)

    attn_other = mm(cols_of(attn_t, other_row), full_out, 0, 0).astype(BF)
    attn_mine = mm(cols_of(attn_t, mine_row), full_out, 0, 0)
    resid = rows_of(inputs32, mine_row) + sum_tp(attn_mine, attn_other)
    unit_two, inv_two = unit_rows(resid)
    h_two = whole_rows((unit_two * gain_f).astype(BF))

    d_hidden = mm(grad_rows, full_down, 1, 1)
    gate_up = mm(h_two, flat_gate_up, 1, 0)
    gate, up = gate_up[:, :ff_local], gate_up[:, ff_local:]
    gate_sigmoid = 1.0 / (1.0 + jnp.exp(-gate))
    gate_silu = gate * gate_sigmoid
    hidden = (gate_silu * up).astype(BF)
    slope = gate_sigmoid * (1.0 + gate * (1.0 - gate_sigmoid))
    d_gate = (d_hidden * up * slope).astype(BF)
    d_up = (d_hidden * gate_silu).astype(BF)
    d_gate_up = jnp.concatenate([d_gate, d_up], axis=1)

    d_two_other = mm(rows_of(d_gate_up, other_row), flat_gate_up, 1, 1).astype(BF)
    d_two_mine = mm(rows_of(d_gate_up, mine_row), flat_gate_up, 1, 1)
    d_two = sum_tp(d_two_mine, d_two_other)
    grad_down = reduce_grad(lambda part: mm(hidden, part_of(grad_rows, part), 0, 0), 1)
    grad_gate = reduce_grad(lambda part: mm(part_of(h_two, part), d_gate, 0, 0), 0)
    grad_up = reduce_grad(lambda part: mm(part_of(h_two, part), d_up, 0, 0), 0)
    ffn_other = mm(rows_of(hidden, other_row), full_down, 1, 0).astype(BF)
    ffn_mine = mm(rows_of(hidden, mine_row), full_down, 1, 0)
    block_output = turn(whole_rows(resid + sum_tp(ffn_mine, ffn_other)))

    part_ffn_gain = jnp.sum(d_two * unit_two, axis=0)
    d_resid = rows_of(grad_rows, mine_row).astype(F32) + norm_back(unit_two, inv_two, gain_f, d_two)
    d_attn = whole_rows(d_resid.astype(BF))

    d_heads_t = mm(full_out, d_attn, 1, 1).astype(BF)
    d_q = None
    d_kv_parts = [None] * n_ctx
    for back in reversed(range(n_ctx)):
        d_q, d_kv = attend_back(
            back == 0, valids[back], q_t, kv_blocks[back], out_t, sums, d_heads_t, d_q
        )
        if back > 0:
            d_kv = over(d_kv, "ctx", [(i, i - back) for i in range(back, n_ctx)])
        d_kv_parts[back] = d_kv
    grad_out = reduce_grad(lambda part: mm(attn_t, part_of(d_attn, part), 1, 0), 1)
    d_qkv_t, sum_q, sum_k = prep_back(qkv_t, cos_t, sin_t, gain_q, gain_k, d_q, d_kv_parts)
    grad_qkv = reduce_grad(lambda part: mm(part_of(h_one, part), d_qkv_t, 0, 1), 0)
    d_one_other = mm(cols_of(d_qkv_t, other_row), full_qkv, 0, 1).astype(BF)
    d_one_mine = mm(cols_of(d_qkv_t, mine_row), full_qkv, 0, 1)
    d_one = sum_tp(d_one_mine, d_one_other)
    unit_half, inv_half = rows_of(unit_one, mine_row), rows_of(inv_one, mine_row)
    part_attn_gain = jnp.sum(d_one * unit_half, axis=0)
    input_grad = turn(whole_rows(d_resid + norm_back(unit_half, inv_half, gain_a, d_one)))

    share = 2.0 / n_tp
    gains = lax.psum(
        jnp.concatenate(
            [turn(part_attn_gain) * share, turn(part_ffn_gain) * share, sum_q[:, 0], sum_k[:, 0]]
        ),
        ("fsdp", "ctx", "tp"),
    )
    grad_gains = [
        gains[:D],
        gains[D : 2 * D],
        gains[2 * D : 2 * D + HEAD_SIZE],
        gains[2 * D + HEAD_SIZE :],
    ]

    g_qkv, g_out, g_gate, g_up, g_down = (
        grad.astype(F32) for grad in (grad_qkv, grad_out, grad_gate, grad_up, grad_down)
    )
    sq_qkv, sq_out, sq_gate, sq_up, sq_down = (g * g for g in (g_qkv, g_out, g_gate, g_up, g_down))
    by_tp = jnp.concatenate(
        [
            jnp.sum(sq_qkv, axis=1),
            jnp.sum(sq_gate, axis=1) + jnp.sum(sq_up, axis=1),
            jnp.sum(sq_out, axis=0),
            jnp.sum(sq_down, axis=0),
        ]
    )
    by_fsdp = jnp.concatenate(
        [
            jnp.sum(sq_qkv, axis=0),
            jnp.sum(sq_gate, axis=0),
            jnp.sum(sq_up, axis=0),
            jnp.sum(sq_out, axis=1),
            jnp.sum(sq_down, axis=1),
        ]
    )
    local_totals = jnp.stack(
        [jnp.sum(sq_qkv), jnp.sum(sq_out), jnp.sum(sq_gate) + jnp.sum(sq_up), jnp.sum(sq_down)]
    )
    by_tp = lax.psum(by_tp, "tp")
    by_fsdp = lax.psum(by_fsdp, "fsdp")

    def split(vector, lengths):
        out, at = [], 0
        for size in lengths:
            out.append(vector[at : at + size])
            at += size
        return out

    rows_qkv, rows_gu, cols_out, cols_down = split(
        by_tp, [w_qkv.shape[0], shard, w_out.shape[1], w_down.shape[1]]
    )
    cols_qkv, cols_gate, cols_up, rows_out, rows_down = split(
        by_fsdp, [w_qkv.shape[1], ff_local, ff_local, w_out.shape[0], w_down.shape[0]]
    )
    keep = lambda old, total, count: DECAY * old + (1.0 - DECAY) * (total / count)
    row_qkv, col_qkv = keep(row_qkv_old, rows_qkv, QKV), keep(col_qkv_old, cols_qkv, D)
    row_out, col_out = keep(row_out_old, rows_out, D), keep(col_out_old, cols_out, D)
    row_gu = keep(row_gate_up_old, rows_gu, 2 * FF)
    col_gu = keep(col_gate_up_old, jnp.stack([cols_gate, cols_up]), D)
    row_down, col_down = keep(row_down_old, rows_down, D), keep(col_down_old, cols_down, FF)

    left_qkv, left_out, left_gu, left_down = (
        lax.rsqrt(row)[:, None] for row in (row_qkv, row_out, row_gu, row_down)
    )
    right_qkv, right_out, right_gate, right_up, right_down = (
        lax.rsqrt(col)[None, :] for col in (col_qkv, col_out, col_gu[0], col_gu[1], col_down)
    )
    square = lambda value: value * value
    scaled_sums = jnp.stack(
        [
            jnp.sum(square(g_qkv * left_qkv * right_qkv)),
            jnp.sum(square(g_out * left_out * right_out)),
            jnp.sum(square(g_gate * left_gu * right_gate))
            + jnp.sum(square(g_up * left_gu * right_up)),
            jnp.sum(square(g_down * left_down * right_down)),
        ]
    )
    weight_sums = jnp.stack([jnp.sum(square(w)) for w in (w_qkv, w_out, w_gate_up, w_down)])
    old_sums = jnp.stack(
        [
            jnp.sum(row_qkv_old) / n_tp,
            jnp.sum(row_out_old) / n_fsdp,
            jnp.sum(row_gate_up_old) / n_tp,
            jnp.sum(row_down_old) / n_fsdp,
        ]
    )
    totals = lax.psum(
        jnp.concatenate([scaled_sums, local_totals, weight_sums, old_sums]), ("fsdp", "tp")
    )
    n_rows = jnp.array([D, D, D, FF], F32)
    n_cols = jnp.array([QKV, D, 2 * FF, D], F32)
    mean_rows = DECAY * totals[12:16] / n_rows + (1.0 - DECAY) * totals[4:8] / (n_rows * n_cols)
    var_olds = [var_attn_old, var_ffn_old, var_query_old, var_key_old]
    var_news = [
        DECAY * old + (1.0 - DECAY) * grad * grad for old, grad in zip(var_olds, grad_gains)
    ]
    raw_gains = [grad * lax.rsqrt(var) for grad, var in zip(grad_gains, var_news)]
    gain_sq = sum(jnp.sum(raw * raw) for raw in raw_gains)
    count = D * QKV + D * D + 2 * D * FF + FF * D + 2 * D + 2 * HEAD_SIZE
    rms_value = jnp.sqrt((jnp.sum(totals[:4] * mean_rows) + gain_sq) / count)
    clip = jnp.maximum(1.0, rms_value / CLIP)
    factors = -RATE * jnp.sqrt(totals[8:12] / (n_rows * n_cols)) * jnp.sqrt(mean_rows) / clip
    step_qkv = g_qkv * left_qkv * (right_qkv * factors[0])
    step_out = g_out * left_out * (right_out * factors[1])
    step_gate = g_gate * left_gu * (right_gate * factors[2])
    step_up = g_up * left_gu * (right_up * factors[2])
    step_down = g_down * left_down * (right_down * factors[3])
    gain_olds = [gain_attn, gain_ffn, gain_query, gain_key]
    gain_steps = [
        -RATE * jnp.sqrt(jnp.mean(old * old)) * raw / clip for old, raw in zip(gain_olds, raw_gains)
    ]
    return (
        block_output[None],
        input_grad[None],
        g_qkv,
        g_out,
        jnp.stack([g_gate, g_up], axis=1),
        g_down,
        *grad_gains,
        row_qkv,
        col_qkv,
        row_out,
        col_out,
        row_gu,
        col_gu,
        row_down,
        col_down,
        *var_news,
        step_qkv,
        step_out,
        jnp.stack([step_gate, step_up], axis=1),
        step_down,
        *gain_steps,
        rms_value,
    )


def solution(mesh):
    tokens, vector = P("fsdp", "ctx", None), P()
    by_f, by_t = P("fsdp"), P("tp")
    w_specs = (P("fsdp", "tp"), P("tp", "fsdp"), P("fsdp", None, "tp"), P("tp", "fsdp"))
    stats = (by_f, by_t, by_t, by_f, by_f, P(None, "tp"), by_t, by_f) + (vector,) * 4
    return jax.shard_map(
        functools.partial(on_device, dict(mesh.shape)),
        mesh=mesh,
        in_specs=(tokens, tokens, by_f, P("fsdp", "ctx")) + w_specs + (vector,) * 4 + stats,
        out_specs=(tokens, tokens)
        + w_specs
        + (vector,) * 4
        + stats
        + w_specs
        + (vector,) * 4
        + (vector,),
        check_vma=False,
    )
```

```python
import functools
import math

import jax
import jax.numpy as jnp
from jax import lax
from jax.experimental import pallas as pl
from jax.experimental.pallas import tpu as pltpu
from jax.sharding import PartitionSpec as P

D = 1024
QUERY_HEADS = 16
KEY_VALUE_HEADS = 8
HEAD_SIZE = 64
FF = 4608
QKV = 2048

EPS = 1e-05
THETA = 1000000.0
DECAY = 0.5
CLIP = 0.15
RATE = 1.0

BF = jnp.bfloat16
F32 = jnp.float32
GROUP = QUERY_HEADS // KEY_VALUE_HEADS
LANES = (GROUP + 2) * HEAD_SIZE
KEY_TILE = 256
PAIR_BLOCKS = 4


def mm(left, right, left_dim, right_dim):
    return lax.dot_general(
        left, right, (((left_dim,), (right_dim,)), ((), ())), preferred_element_type=F32
    )


def params(vmem=48 << 20):
    return pltpu.CompilerParams(vmem_limit_bytes=vmem)


def squares_into(sum_ref, values):
    rows, cols = values.shape
    sum_ref[...] += jnp.sum((values * values).reshape(rows // 8, 8, cols), axis=0)


def cast_kernel(spans, w_ref, *refs):
    sum_ref = refs[-1]

    @pl.when(pl.program_id(0) == 0)
    def _():
        sum_ref[...] = jnp.zeros_like(sum_ref)

    values = w_ref[...]
    for out_ref, pieces in zip(refs, spans):
        at = 0
        for start, size in pieces:
            out_ref[:, at : at + size] = values[:, start : start + size].astype(BF)
            at += size
    squares_into(sum_ref, values)


def cast(weight, spans=None):
    rows, cols = weight.shape
    spans = spans or [[(0, cols)]]
    widths = [sum(size for _, size in pieces) for pieces in spans]
    block = min(rows, 128)
    return pl.pallas_call(
        functools.partial(cast_kernel, spans),
        grid=(rows // block,),
        in_specs=[pl.BlockSpec((block, cols), lambda i: (i, 0))],
        out_specs=[pl.BlockSpec((block, width), lambda i: (i, 0)) for width in widths]
        + [pl.BlockSpec((8, cols), lambda i: (0, 0))],
        out_shape=[jax.ShapeDtypeStruct((rows, width), BF) for width in widths]
        + [jax.ShapeDtypeStruct((8, cols), F32)],
        cost_estimate=pl.CostEstimate(
            flops=3 * rows * cols, bytes_accessed=6 * rows * cols, transcendentals=0
        ),
        compiler_params=params(),
        name="cast",
    )(weight)


def cast_pair_kernel(w_ref, gate_ref, up_ref, sum_ref, held, sems):
    rows = w_ref.shape[0]
    block = rows // PAIR_BLOCKS
    copies = []
    for step in range(PAIR_BLOCKS):
        for which in range(2):
            span = pl.ds(step * block, block)
            copies.append(
                pltpu.make_async_copy(
                    w_ref.at[span, which, :], held.at[which, span, :], sems.at[which, step]
                )
            )
            copies[-1].start()
    sum_ref[...] = jnp.zeros_like(sum_ref)
    for step in range(PAIR_BLOCKS):
        for which, out_ref in enumerate((gate_ref, up_ref)):
            copies[2 * step + which].wait()

            @pl.loop(0, block // 16)
            def _(piece):
                at = pl.multiple_of(step * block + piece * 16, 16)
                values = held[which, pl.ds(at, 16), :]
                out_ref[pl.ds(at, 16), :] = values.astype(BF)
                squares_into(sum_ref, values)


def cast_pair(weight):
    rows, _, cols = weight.shape
    vmem = pl.BlockSpec(memory_space=pltpu.VMEM)
    return pl.pallas_call(
        cast_pair_kernel,
        in_specs=[pl.BlockSpec(memory_space=pl.ANY)],
        out_specs=[vmem] * 3,
        out_shape=[jax.ShapeDtypeStruct((rows, cols), BF)] * 2
        + [jax.ShapeDtypeStruct((8, cols), F32)],
        scratch_shapes=[
            pltpu.VMEM((2, rows, cols), F32),
            pltpu.SemaphoreType.DMA((2, PAIR_BLOCKS)),
        ],
        cost_estimate=pl.CostEstimate(
            flops=6 * rows * cols, bytes_accessed=12 * rows * cols, transcendentals=0
        ),
        compiler_params=params(),
        name="cast_pair",
    )(weight)


def lane_total(values):
    lanes = min(128, values.shape[1])
    total = values[:, :lanes]
    for at in range(lanes, values.shape[1], lanes):
        total = total + values[:, at : at + lanes]
    return total


def padded(size):
    return -(-size // 128) * 128


def spans_of(sizes):
    out, at = [], 0
    for size in sizes:
        out.append(slice(at, at + size))
        at += padded(size)
    return out


def layout_of(grads):
    qkv, out, gate, up, down = (g.shape for g in grads)
    tp_spans = spans_of([qkv[0], gate[0], out[1], down[1]])
    fsdp_spans = spans_of([qkv[1], gate[1], up[1], out[0], down[0]])
    return (
        ((0, tp_spans[0]), (1, fsdp_spans[0])),
        ((1, fsdp_spans[3]), (0, tp_spans[2])),
        ((0, tp_spans[1]), (1, fsdp_spans[1])),
        ((0, tp_spans[1]), (1, fsdp_spans[2])),
        ((1, fsdp_spans[4]), (0, tp_spans[3])),
    )


def packed_sizes(grads):
    qkv, out, gate, up, down = (g.shape for g in grads)
    return (
        sum(map(padded, (qkv[0], gate[0], out[1], down[1]))),
        sum(map(padded, (qkv[1], gate[1], up[1], out[0], down[0]))),
    )


def over_blocks(n_rows, block, body, init=None):
    if n_rows == block:
        return body(0, init)
    aligned = lambda step, carry: body(pl.multiple_of(step * block, block), carry)
    return lax.fori_loop(0, n_rows // block, aligned, init)


def stats_kernel(*refs):
    grads, packed = refs[:5], refs[5:]
    for ref in packed:
        ref[...] = jnp.zeros_like(ref)
    for index, (grad_ref, places) in enumerate(zip(grads, layout_of(grads))):
        n_rows = grad_ref.shape[0]
        block = min(n_rows, 128)
        (row_at, row_span), (col_at, col_span) = places
        row_ref, col_ref = packed[row_at], packed[col_at]

        def add_block(at, carry):
            values = grad_ref[pl.ds(at, block), :].astype(F32)
            square = values * values
            col_ref[:, col_span] += jnp.sum(square, axis=0, keepdims=True)
            folded = jnp.sum(lane_total(square).T, axis=0, keepdims=True)
            start = row_span.start + at
            place = pl.ds(start if n_rows == block else pl.multiple_of(start, block), block)
            row_ref[:, place] += folded
            return carry

        over_blocks(n_rows, block, add_block, 0)


def stats(grads):
    vmem = pl.BlockSpec(memory_space=pltpu.VMEM)
    return pl.pallas_call(
        stats_kernel,
        in_specs=[vmem] * 5,
        out_specs=[vmem] * 2,
        out_shape=[jax.ShapeDtypeStruct((1, size), F32) for size in packed_sizes(grads)],
        cost_estimate=pl.CostEstimate(
            flops=4 * sum(g.size for g in grads),
            bytes_accessed=2 * sum(g.size for g in grads),
            transcendentals=0,
        ),
        compiler_params=params(),
        name="stats",
    )(*grads)


def columns_of(row, width):
    return jnp.broadcast_to(row, (min(128, width), row.shape[1])).T


def total_of(values):
    return jnp.sum(jnp.sum(values, axis=0, keepdims=True), axis=1, keepdims=True)


def out_views(outs):
    qkv, out, gate_up, down = outs
    return (
        lambda span: qkv.at[span, :],
        lambda span: out.at[span, :],
        lambda span: gate_up.at[span, 0, :],
        lambda span: gate_up.at[span, 1, :],
        lambda span: down.at[span, :],
    )


def tiles_in(grads):
    for index, grad_ref in enumerate(grads):
        block = min(grad_ref.shape[0], 128)
        for at in range(0, grad_ref.shape[0], block):
            yield index, at, block


def write_shapes(grads):
    qkv, out, gate, _, down = (g.shape for g in grads)
    return [
        jax.ShapeDtypeStruct(shape, F32) for shape in (qkv, out, (gate[0], 2, gate[1]), down)
    ]


def write_scratch(grads):
    count = len(list(tiles_in(grads)))
    return [pltpu.VMEM(g.shape, F32) for g in grads] + [pltpu.SemaphoreType.DMA((count,))]


def scaled_kernel(shares, *refs):
    grads, sums, olds, squares = refs[:5], refs[5:7], refs[7:9], refs[9:13]
    outs, news, scale_refs, scalar_ref = refs[13:17], refs[17:19], refs[19:21], refs[21]
    held, sems = refs[22:27], refs[27]
    copies = []
    views = out_views(outs)
    for number, (index, at, block) in enumerate(tiles_in(grads)):
        span = pl.ds(at, block)
        held[index][span, :] = grads[index][span, :].astype(F32)
        copies.append(
            pltpu.make_async_copy(held[index].at[span, :], views[index](span), sems.at[number])
        )
        copies[-1].start()
    places = layout_of(grads)
    counts = ((QKV, D), (D, D), (2 * FF, D), (2 * FF, D), (D, FF))
    scalars = []
    for (row_place, col_place), count in zip(places, counts):
        for (at, span), size in zip((row_place, col_place), count):
            new = DECAY * olds[at][:, span] + (1.0 - DECAY) * (sums[at][:, span] / size)
            news[at][:, span] = new
            scale_refs[at][:, span] = lax.rsqrt(new)
    scaled = []
    for index, (row_place, col_place) in enumerate(places):
        grad_ref = grads[index]
        n_rows, n_cols = grad_ref.shape
        block = min(n_rows, 128)
        lanes = min(128, n_cols)
        left_ref, row_start = scale_refs[row_place[0]], row_place[1].start
        right = scale_refs[col_place[0]][:, col_place[1]]

        def step_of(at, total):
            values = held[index][pl.ds(at, block), :] * right
            start = row_start + at
            place = pl.ds(start if n_rows == block else pl.multiple_of(start, block), block)
            left = columns_of(left_ref[:, place], n_cols)
            folded = lane_total(values * values) * (left * left)
            return total + jnp.sum(folded.reshape(block // 8, 8, lanes), axis=0)

        total = over_blocks(n_rows, block, step_of, jnp.zeros((8, lanes), F32))
        scaled.append(total_of(total))
    scalars += [scaled[0], scaled[1], scaled[2] + scaled[3], scaled[4]]
    row_places = [places[index][0] for index in (0, 1, 2, 4)]
    scalars += [total_of(sums[at][:, span]) * shares[at] for at, span in row_places]
    scalars += [total_of(ref[...]) for ref in squares]
    scalars += [total_of(olds[at][:, span]) * shares[at] for at, span in row_places]
    lane = lax.broadcasted_iota(jnp.int32, (8, 128), 1)
    packed = jnp.zeros((8, 128), F32)
    for number, value in enumerate(scalars):
        packed = jnp.where(lane == number, value, packed)
    scalar_ref[...] = packed
    for copy in copies:
        copy.wait()


def scaled(shares, grads, sums, olds, squares):
    vmem, hbm = pl.BlockSpec(memory_space=pltpu.VMEM), pl.BlockSpec(memory_space=pl.ANY)
    vectors = [jax.ShapeDtypeStruct((1, size), F32) for size in packed_sizes(grads)]
    out = pl.pallas_call(
        functools.partial(scaled_kernel, shares),
        in_specs=[vmem] * 13,
        out_specs=[hbm] * 4 + [vmem] * 5,
        out_shape=write_shapes(grads) + vectors * 2 + [jax.ShapeDtypeStruct((8, 128), F32)],
        scratch_shapes=write_scratch(grads),
        cost_estimate=pl.CostEstimate(
            flops=6 * sum(g.size for g in grads),
            bytes_accessed=6 * sum(g.size for g in grads),
            transcendentals=0,
        ),
        compiler_params=params(),
        name="scaled",
    )(*grads, *sums, *olds, *squares)
    return out[:4], out[4:6], out[6:8], out[8]


def finish_kernel(*refs):
    grads, scale_refs, total_ref = refs[:5], refs[5:7], refs[7]
    gain_grad_ref, var_ref, gain_ref = refs[8:11]
    outs, new_var_ref, gain_step_ref, rms_ref = refs[11:15], refs[15], refs[16], refs[17]
    held, sems = refs[18:23], refs[23]
    value = lambda number: total_ref[0:1, number : number + 1]
    sizes = ((D, QKV), (D, D), (D, 2 * FF), (FF, D))
    means = [
        DECAY * value(12 + index) / rows + (1.0 - DECAY) * value(4 + index) / (rows * cols)
        for index, (rows, cols) in enumerate(sizes)
    ]
    gain_grad = gain_grad_ref[...]
    new_var = DECAY * var_ref[...] + (1.0 - DECAY) * gain_grad * gain_grad
    new_var_ref[...] = new_var
    raw_gain = gain_grad * lax.rsqrt(new_var)
    total = jnp.sum(raw_gain * raw_gain, axis=1, keepdims=True)
    for index, mean in enumerate(means):
        total = total + value(index) * mean
    count = D * QKV + D * D + 2 * D * FF + FF * D + 2 * D + 2 * HEAD_SIZE
    rms = jnp.sqrt(total / count)
    rms_ref[...] = jnp.broadcast_to(rms, rms_ref.shape)
    clip = jnp.maximum(1.0, rms / CLIP)
    factors = [
        -RATE * jnp.sqrt(value(8 + index) / (rows * cols)) * jnp.sqrt(means[index]) / clip
        for index, (rows, cols) in enumerate(sizes)
    ]
    copies = []
    views, places = out_views(outs), layout_of(grads)
    tensor_of = (0, 1, 2, 2, 3)
    for number, (index, at, block) in enumerate(tiles_in(grads)):
        span = pl.ds(at, block)
        (row_at, row_span), (col_at, col_span) = places[index]
        start = row_span.start + at
        n_cols = grads[index].shape[1]
        left = columns_of(scale_refs[row_at][:, start : start + block], n_cols)
        right = scale_refs[col_at][:, col_span] * factors[tensor_of[index]]
        for first in range(0, n_cols, left.shape[1]):
            lanes = slice(first, first + left.shape[1])
            tile = grads[index][span, lanes].astype(F32)
            held[index][span, lanes] = tile * left * right[:, lanes]
        copies.append(
            pltpu.make_async_copy(held[index].at[span, :], views[index](span), sems.at[number])
        )
        copies[-1].start()
    for start, size in ((0, D), (D, D)):
        span = slice(start, start + size)
        gain = gain_ref[:, span]
        scale = -RATE * jnp.sqrt(jnp.sum(gain * gain, axis=1, keepdims=True) / size) / clip
        gain_step_ref[:, span] = raw_gain[:, span] * scale
    span = slice(2 * D, 2 * D + 2 * HEAD_SIZE)
    gain = gain_ref[:, span]
    low = lax.broadcasted_iota(jnp.int32, gain.shape, 1) < HEAD_SIZE
    square = gain * gain
    low_sum = jnp.sum(jnp.where(low, square, 0.0), axis=1, keepdims=True)
    high_sum = jnp.sum(jnp.where(low, 0.0, square), axis=1, keepdims=True)
    scale = -RATE * jnp.sqrt(jnp.where(low, low_sum, high_sum) / HEAD_SIZE) / clip
    gain_step_ref[:, span] = raw_gain[:, span] * scale
    for copy in copies:
        copy.wait()


def finish(grads, scales, totals, gain_grads, gain_vars, gains):
    vmem, hbm = pl.BlockSpec(memory_space=pltpu.VMEM), pl.BlockSpec(memory_space=pl.ANY)
    vector = jax.ShapeDtypeStruct(gains.shape, F32)
    out = pl.pallas_call(
        finish_kernel,
        in_specs=[vmem] * 11,
        out_specs=[hbm] * 4 + [vmem] * 3,
        out_shape=write_shapes(grads) + [vector, vector, jax.ShapeDtypeStruct((8, 128), F32)],
        scratch_shapes=write_scratch(grads),
        cost_estimate=pl.CostEstimate(
            flops=4 * sum(g.size for g in grads),
            bytes_accessed=6 * sum(g.size for g in grads),
            transcendentals=0,
        ),
        compiler_params=params(),
        name="finish",
    )(*grads, *scales, totals, gain_grads, gain_vars, gains)
    return out[:4], out[4], out[5], out[6]


def turned_head(rows, gain, cos_t, sin_t):
    half = HEAD_SIZE // 2
    inv = lax.rsqrt(jnp.mean(rows * rows, axis=0, keepdims=True) + EPS)
    normed = rows * inv * gain
    low, high = normed[:half], normed[half:]
    return jnp.concatenate([low * cos_t - high * sin_t, high * cos_t + low * sin_t], axis=0)


def queries_kernel(raw_ref, cos_ref, sin_ref, gain_ref, q_ref):
    turned = turned_head(raw_ref[...], gain_ref[...], cos_ref[...], sin_ref[...])
    scale = 1.0 / math.sqrt(HEAD_SIZE)
    q_ref[...] = (turned.astype(BF).astype(F32) * scale).astype(BF)


def keys_kernel(raw_ref, cos_ref, sin_ref, gain_ref, kv_ref):
    turned = turned_head(raw_ref[:HEAD_SIZE, :], gain_ref[...], cos_ref[...], sin_ref[...])
    kv_ref[:HEAD_SIZE, :] = turned.astype(BF)
    kv_ref[HEAD_SIZE:, :] = raw_ref[HEAD_SIZE:, :].astype(BF)


def prep_call(kernel, size, raw_t, cos_t, sin_t, gain):
    rows, tokens = raw_t.shape
    half = HEAD_SIZE // 2
    fixed = lambda g: (0, 0)
    return pl.pallas_call(
        kernel,
        grid=(rows // size,),
        in_specs=[
            pl.BlockSpec((size, tokens), lambda g: (g, 0)),
            pl.BlockSpec((half, tokens), fixed),
            pl.BlockSpec((half, tokens), fixed),
            pl.BlockSpec((HEAD_SIZE, 1), fixed),
        ],
        out_specs=pl.BlockSpec((size, tokens), lambda g: (g, 0)),
        out_shape=jax.ShapeDtypeStruct(raw_t.shape, BF),
        cost_estimate=pl.CostEstimate(
            flops=20 * rows * tokens, bytes_accessed=6 * rows * tokens, transcendentals=0
        ),
        compiler_params=params(),
        name="prep",
    )(raw_t, cos_t, sin_t, gain)


prep_queries = functools.partial(prep_call, queries_kernel, HEAD_SIZE)
prep_keys = functools.partial(prep_call, keys_kernel, 2 * HEAD_SIZE)


def prep_back_kernel(parts, *refs):
    raw_q_ref, raw_kv_ref, cos_ref, sin_ref, gq_ref, gk_ref, dq_ref = refs[:7]
    dkv_refs = refs[7 : 7 + parts]
    out_q_ref, out_kv_ref, sum_q_ref, sum_k_ref = refs[7 + parts :]
    half = HEAD_SIZE // 2
    cos_t, sin_t = cos_ref[...], sin_ref[...]
    d_kv = dkv_refs[0][...]
    for ref in dkv_refs[1:]:
        d_kv = d_kv + ref[...].astype(F32)

    @pl.when(pl.program_id(0) == 0)
    def _():
        sum_q_ref[...] = jnp.zeros_like(sum_q_ref)
        sum_k_ref[...] = jnp.zeros_like(sum_k_ref)

    for piece in range(GROUP + 1):
        base = piece * HEAD_SIZE
        if piece < GROUP:
            rows = raw_q_ref[base : base + HEAD_SIZE, :]
            grad = dq_ref[base : base + HEAD_SIZE, :] * (1.0 / math.sqrt(HEAD_SIZE))
            gain, sum_ref = gq_ref[...], sum_q_ref
        else:
            rows = raw_kv_ref[:HEAD_SIZE, :]
            grad = d_kv[:HEAD_SIZE]
            gain, sum_ref = gk_ref[...], sum_k_ref
        inv = lax.rsqrt(jnp.mean(rows * rows, axis=0, keepdims=True) + EPS)
        unit = rows * inv
        low, high = grad[:half], grad[half:]
        turned = jnp.concatenate([low * cos_t + high * sin_t, high * cos_t - low * sin_t], axis=0)
        sum_ref[...] += jnp.sum(turned * unit, axis=1, keepdims=True)
        scaled = turned * gain
        mean = jnp.mean(scaled * unit, axis=0, keepdims=True)
        result = ((scaled - unit * mean) * inv).astype(BF)
        if piece < GROUP:
            out_q_ref[base : base + HEAD_SIZE, :] = result
        else:
            out_kv_ref[:HEAD_SIZE, :] = result
    out_kv_ref[HEAD_SIZE:, :] = d_kv[HEAD_SIZE:].astype(BF)


def prep_back(raw_q_t, raw_kv_t, cos_t, sin_t, gain_q, gain_k, d_q, d_kv_parts):
    tokens = raw_q_t.shape[1]
    groups = raw_kv_t.shape[0] // (2 * HEAD_SIZE)
    rows = raw_q_t.shape[0] + raw_kv_t.shape[0]
    half = HEAD_SIZE // 2
    fixed = lambda g: (0, 0)
    block = lambda size: pl.BlockSpec((size, tokens), lambda g: (g, 0))
    return pl.pallas_call(
        functools.partial(prep_back_kernel, len(d_kv_parts)),
        grid=(groups,),
        in_specs=[
            block(GROUP * HEAD_SIZE),
            block(2 * HEAD_SIZE),
            pl.BlockSpec((half, tokens), fixed),
            pl.BlockSpec((half, tokens), fixed),
            pl.BlockSpec((HEAD_SIZE, 1), fixed),
            pl.BlockSpec((HEAD_SIZE, 1), fixed),
            block(GROUP * HEAD_SIZE),
        ]
        + [block(2 * HEAD_SIZE)] * len(d_kv_parts),
        out_specs=[
            block(GROUP * HEAD_SIZE),
            block(2 * HEAD_SIZE),
            pl.BlockSpec((HEAD_SIZE, 128), fixed),
            pl.BlockSpec((HEAD_SIZE, 128), fixed),
        ],
        out_shape=[
            jax.ShapeDtypeStruct(raw_q_t.shape, BF),
            jax.ShapeDtypeStruct(raw_kv_t.shape, BF),
            jax.ShapeDtypeStruct((HEAD_SIZE, 128), F32),
            jax.ShapeDtypeStruct((HEAD_SIZE, 128), F32),
        ],
        cost_estimate=pl.CostEstimate(
            flops=30 * rows * tokens, bytes_accessed=9 * rows * tokens, transcendentals=0
        ),
        compiler_params=params(),
        name="prep_back",
    )(raw_q_t, raw_kv_t, cos_t, sin_t, gain_q, gain_k, d_q, *d_kv_parts)


def tiles_of(diagonal, tokens):
    for key_start in range(0, tokens, KEY_TILE):
        yield key_start, key_start if diagonal else 0


def tile_probs(kv_ref, query, key_start, query_start, valid, diagonal):
    keys = kv_ref[:HEAD_SIZE, key_start : key_start + KEY_TILE]
    scores = mm(keys, query, 0, 0)
    key_index = key_start + lax.broadcasted_iota(jnp.int32, scores.shape, 0)
    visible = key_index < valid
    if diagonal:
        query_index = query_start + lax.broadcasted_iota(jnp.int32, scores.shape, 1)
        visible = visible & (key_index <= query_index)
    return keys, visible, jnp.exp(scores)


def attend_kernel(diagonal, valid_ref, q_ref, kv_ref, *refs):
    if diagonal:
        acc_ref, sum_ref = refs
        acc_ref[...] = jnp.zeros_like(acc_ref)
        sum_ref[...] = jnp.zeros_like(sum_ref)
    else:
        acc_in_ref, sum_in_ref, acc_ref, sum_ref = refs
        acc_ref[...] = acc_in_ref[...]
        sum_ref[...] = sum_in_ref[...]
    valid = valid_ref[0]
    tokens = q_ref.shape[1]

    @pl.when(valid > 0)
    def _():
        for key_start, query_start in tiles_of(diagonal, tokens):
            query = q_ref[:, query_start:]
            keys, visible, raised = tile_probs(
                kv_ref, query, key_start, query_start, valid, diagonal
            )
            probs = jnp.where(visible, raised, 0.0)
            sum_ref[:, query_start:] += jnp.sum(probs, axis=0, keepdims=True)
            values = kv_ref[HEAD_SIZE:, key_start : key_start + KEY_TILE]
            acc_ref[:, query_start:] += mm(values, probs.astype(BF), 1, 0)


def attend(diagonal, valid, q_t, kv_t, state):
    rows, tokens = q_t.shape
    heads = rows // HEAD_SIZE
    per_head = pl.BlockSpec((HEAD_SIZE, tokens), lambda h: (h, 0))
    sums = pl.BlockSpec((8, tokens), lambda h: (h, 0))
    carried = [] if diagonal else [per_head, sums]
    return pl.pallas_call(
        functools.partial(attend_kernel, diagonal),
        grid=(heads,),
        in_specs=[
            pl.BlockSpec(memory_space=pltpu.SMEM),
            per_head,
            pl.BlockSpec((2 * HEAD_SIZE, tokens), lambda h: (h // GROUP, 0)),
        ]
        + carried,
        out_specs=[per_head, sums],
        out_shape=[
            jax.ShapeDtypeStruct((rows, tokens), F32),
            jax.ShapeDtypeStruct((heads * 8, tokens), F32),
        ],
        input_output_aliases={} if diagonal else {3: 0, 4: 1},
        cost_estimate=pl.CostEstimate(
            flops=4 * rows * tokens * tokens,
            bytes_accessed=10 * rows * tokens,
            transcendentals=heads * tokens * tokens,
        ),
        compiler_params=params(),
        name="attend",
    )(valid, q_t, kv_t, *state)


def attend_back_kernel(diagonal, first, valid_ref, q_ref, kv_ref, out_ref, sum_ref, do_ref, *refs):
    if first:
        dq_ref, dkv_ref, dkv_acc = refs
        dq_ref[...] = jnp.zeros_like(dq_ref)
    else:
        dq_in_ref, dq_ref, dkv_ref, dkv_acc = refs
        dq_ref[...] = dq_in_ref[...]
    head = pl.program_id(0)
    valid = valid_ref[0]
    tokens = q_ref.shape[1]

    @pl.when(head % GROUP == 0)
    def _():
        dkv_acc[...] = jnp.zeros_like(dkv_acc)

    @pl.when(valid > 0)
    def _():
        inverse = 1.0 / sum_ref[0:1, :]
        delta = jnp.sum(do_ref[...].astype(F32) * out_ref[...], axis=0, keepdims=True)
        for key_start, query_start in tiles_of(diagonal, tokens):
            query = q_ref[:, query_start:]
            grads = do_ref[:, query_start:]
            keys, visible, raised = tile_probs(
                kv_ref, query, key_start, query_start, valid, diagonal
            )
            probs = jnp.where(visible, raised * inverse[:, query_start:], 0.0)
            span = slice(key_start, key_start + KEY_TILE)
            values = kv_ref[HEAD_SIZE:, span]
            d_probs = mm(values, grads, 0, 0)
            d_scores = (probs * (d_probs - delta[:, query_start:])).astype(BF)
            dq_ref[:, query_start:] += mm(keys, d_scores, 1, 0)
            dkv_acc[:HEAD_SIZE, span] += mm(query, d_scores, 1, 1)
            dkv_acc[HEAD_SIZE:, span] += mm(grads, probs.astype(BF), 1, 1)

    @pl.when(head % GROUP == GROUP - 1)
    def _():
        dkv_ref[...] = dkv_acc[...].astype(dkv_ref.dtype)


def attend_back(diagonal, valid, q_t, kv_t, out_t, sums, d_out_t, d_q):
    rows, tokens = q_t.shape
    heads = rows // HEAD_SIZE
    first = d_q is None
    per_head = pl.BlockSpec((HEAD_SIZE, tokens), lambda h: (h, 0))
    per_group = pl.BlockSpec((2 * HEAD_SIZE, tokens), lambda h: (h // GROUP, 0))
    return pl.pallas_call(
        functools.partial(attend_back_kernel, diagonal, first),
        grid=(heads,),
        in_specs=[
            pl.BlockSpec(memory_space=pltpu.SMEM),
            per_head,
            per_group,
            per_head,
            pl.BlockSpec((8, tokens), lambda h: (h, 0)),
            per_head,
        ]
        + ([] if first else [per_head]),
        out_specs=[per_head, per_group],
        out_shape=[
            jax.ShapeDtypeStruct((rows, tokens), F32),
            jax.ShapeDtypeStruct(kv_t.shape, F32 if diagonal else BF),
        ],
        scratch_shapes=[pltpu.VMEM((2 * HEAD_SIZE, tokens), F32)],
        input_output_aliases={} if first else {6: 0},
        cost_estimate=pl.CostEstimate(
            flops=10 * rows * tokens * tokens,
            bytes_accessed=14 * rows * tokens,
            transcendentals=heads * tokens * tokens,
        ),
        compiler_params=params(),
        name="attend_back",
    )(valid, q_t, kv_t, out_t, sums, d_out_t, *([] if first else [d_q]))


def unit_rows(values):
    inv = lax.rsqrt(jnp.mean(values * values, axis=-1, keepdims=True) + EPS)
    return values * inv, inv


def norm_back(unit, inv, gain, grad):
    scaled = grad * gain
    return (scaled - unit * jnp.mean(scaled * unit, axis=-1, keepdims=True)) * inv


def kept(value):
    return lax.optimization_barrier(value)


def on_device(
    sizes,
    block_input,
    cotangent,
    seq_lengths,
    positions,
    w_qkv,
    w_out,
    w_gate_up,
    w_down,
    gain_attn,
    gain_ffn,
    gain_query,
    gain_key,
    row_qkv_old,
    col_qkv_old,
    row_out_old,
    col_out_old,
    row_gate_up_old,
    col_gate_up_old,
    row_down_old,
    col_down_old,
    var_attn_old,
    var_ffn_old,
    var_query_old,
    var_key_old,
):
    n_fsdp, n_ctx, n_tp = sizes["fsdp"], sizes["ctx"], sizes["tp"]
    paired = n_fsdp == 2
    me_f, me_z, me_t = (lax.axis_index(name) for name in ("fsdp", "ctx", "tp"))
    tokens = block_input.shape[1]
    half = tokens // 2
    mine_row = (me_t % 2) * half
    other_row = half - mine_row

    def turn(values):
        if not paired:
            return values
        size = values.shape[-1] // 2
        swapped = jnp.concatenate([values[..., size:], values[..., :size]], axis=-1)
        return jnp.where(me_f == 0, values, swapped)

    def over(values, axis, pairs):
        return lax.ppermute(values, axis, pairs)

    def to_core(values):
        return over(values, "tp", [(i, i ^ 1) for i in range(n_tp)])

    def to_pair(values):
        return over(values, "fsdp", [(0, 1), (1, 0)])

    def gather_weight(shard, axis):
        if not paired:
            return lax.all_gather(shard, "fsdp", axis=axis, tiled=True)
        return jnp.concatenate([shard, to_pair(shard)], axis=axis)

    def gather_split(shard, axis):
        if not paired or n_ctx % 2:
            return gather_weight(shard, axis)
        size = shard.shape[0] // 2
        odd = me_z % 2
        want = lax.dynamic_slice_in_dim(shard, odd * size, size, 0)
        direct = to_pair(want)
        routed = over(direct, "ctx", [(i, i ^ 1) for i in range(n_ctx)])
        first = jnp.where(odd == 0, direct, routed)
        second = jnp.where(odd == 0, routed, direct)
        other = jnp.concatenate([first, second], axis=0)
        return jnp.concatenate([shard, other], axis=axis)

    def sum_tp(mine, other_low):
        total = mine + to_core(other_low).astype(F32)
        step = 2
        while step < n_tp:
            low = kept(total.astype(BF))
            pairs = [(i, i ^ step) for i in range(n_tp)]
            total = low.astype(F32) + over(low, "tp", pairs).astype(F32)
            step *= 2
        return total

    def whole_rows(values):
        other = to_core(values)
        first = jnp.where(mine_row == 0, values, other)
        second = jnp.where(mine_row == 0, other, values)
        return jnp.concatenate([first, second], axis=0)

    def rows_of(values, start):
        return lax.dynamic_slice_in_dim(values, start, half, 0)

    def after(value, *tokens):
        return lax.optimization_barrier((value,) + tokens)[0]

    class Reduction:
        def __init__(self, make, axis):
            self.make, self.axis = make, axis
            self.value = to_pair(make(1).astype(BF)) if paired else None

        def inwards(self, *tokens):
            if paired:
                theirs = after(self.value, *tokens).astype(F32)
                part = kept((self.make(0) + theirs).astype(BF))
            else:
                whole = self.make(None)
                part = lax.psum_scatter(
                    whole, "fsdp", scatter_dimension=self.axis, tiled=True
                ).astype(BF)
            self.value = part
            if n_ctx == 4:
                self.other = over(part, "ctx", [(0, 1), (3, 2)])

        def across(self, *tokens):
            if n_ctx == 4:
                other = after(self.other, *tokens).astype(F32)
                self.value = kept((self.value.astype(F32) + other).astype(BF))
                self.other = over(self.value, "ctx", [(1, 2), (2, 1)])

        def outwards(self, *tokens):
            if n_ctx == 4:
                other = after(self.other, *tokens).astype(F32)
                self.value = kept((self.value.astype(F32) + other).astype(BF))
                self.other = over(self.value, "ctx", [(1, 0), (2, 3)])

        def result(self):
            if n_ctx != 4:
                return kept(lax.psum(self.value.astype(F32), "ctx").astype(BF))
            at_end = (me_z == 0) | (me_z == n_ctx - 1)
            return jnp.where(at_end, self.other, self.value)

    def sum_over_tp(values):
        step = 1
        while step < n_tp:
            values = values + over(values, "tp", [(i, i ^ step) for i in range(n_tp)])
            step *= 2
        return values

    def sum_over_fsdp(values):
        return values + to_pair(values) if paired else lax.psum(values, "fsdp")

    def sum_over_ctx(values):
        step = 1
        while step < n_ctx:
            values = values + over(values, "ctx", [(i, i ^ step) for i in range(n_ctx)])
            step *= 2
        return values

    def sum_all(values):
        return sum_over_ctx(sum_over_fsdp(sum_over_tp(values)))

    def part_of(values, part):
        if part is None:
            return values
        size = values.shape[-1] // 2
        return values[..., part * size : (part + 1) * size]

    groups = w_qkv.shape[1] // LANES
    split_at = GROUP * HEAD_SIZE
    q_spans = [(g * LANES, split_at) for g in range(groups)]
    kv_spans = [(g * LANES + split_at, 2 * HEAD_SIZE) for g in range(groups)]
    shard_q, shard_kv, squares_qkv = cast(w_qkv, [q_spans, kv_spans])
    full_kv = gather_weight(shard_kv, 0)
    full_q = gather_weight(shard_q, 0)
    shard_out, squares_out = cast(w_out)
    full_out = gather_weight(shard_out, 1)
    ff_local = w_gate_up.shape[2]
    shard_gate, shard_up, squares_gate_up = cast_pair(w_gate_up)
    full_gate = gather_split(shard_gate, 0)
    full_up = gather_split(shard_up, 0)
    shard_down, squares_down = cast(w_down)
    full_down = gather_split(shard_down, 1)

    olds = [
        jnp.concatenate([jnp.pad(v, (0, padded(v.size) - v.size)) for v in vectors]).reshape(1, -1)
        for vectors in (
            (row_qkv_old, row_gate_up_old, col_out_old, col_down_old),
            (col_qkv_old, col_gate_up_old[0], col_gate_up_old[1], row_out_old, row_down_old),
        )
    ]
    row_of = lambda vectors: jnp.concatenate(vectors).reshape(1, 2 * D + 2 * HEAD_SIZE)
    gain_vars = row_of([var_attn_old, var_ffn_old, var_query_old, var_key_old])
    gains_old = row_of([gain_attn, gain_ffn, gain_query, gain_key])

    inputs32 = turn(block_input[0].astype(F32))
    grad_rows = turn(cotangent[0])
    gain_a, gain_f = turn(gain_attn), turn(gain_ffn)
    unit_one, inv_one = unit_rows(inputs32)
    h_one = (unit_one * gain_a).astype(BF)
    freq = jnp.exp(
        jnp.arange(HEAD_SIZE // 2, dtype=F32) * (-2.0 * math.log(THETA) / HEAD_SIZE)
    )
    angle = freq[:, None] * positions[0].astype(F32)[None, :]
    cos_t, sin_t = jnp.cos(angle), jnp.sin(angle)
    gain_q, gain_k = gain_query[:, None], gain_key[:, None]
    raw_kv_t = mm(full_kv, h_one, 0, 1)
    kv_t = prep_keys(raw_kv_t, cos_t, sin_t, gain_k)
    raw_q_t = mm(full_q, h_one, 0, 1)
    q_t = prep_queries(raw_q_t, cos_t, sin_t, gain_q)

    length = seq_lengths[0]
    kv_blocks, valids = [], []
    for back in range(n_ctx):
        moved = kv_t
        if back > 0:
            moved = over(kv_t, "ctx", [(i, i + back) for i in range(n_ctx - back)])
        kv_blocks.append(moved)
        count = jnp.clip(length - (me_z - back) * tokens, 0, tokens)
        valids.append(jnp.where(me_z >= back, count, 0).astype(jnp.int32).reshape(1))
    state = []
    for back in range(n_ctx):
        state = attend(back == 0, valids[back], q_t, kv_blocks[back], state)
    acc_t, sums = state
    heads = acc_t.shape[0] // HEAD_SIZE
    inverse = (1.0 / sums.reshape(heads, 8, tokens)[:, :1, :])
    out_t = (acc_t.reshape(heads, HEAD_SIZE, tokens) * inverse).reshape(acc_t.shape)
    attn_t = kept(out_t.astype(BF))

    def cols_of(values, start):
        return lax.dynamic_slice_in_dim(values, start, half, 1)

    attn_other = mm(cols_of(attn_t, other_row), full_out, 0, 0).astype(BF)
    attn_mine = mm(cols_of(attn_t, mine_row), full_out, 0, 0)
    resid = rows_of(inputs32, mine_row) + sum_tp(attn_mine, attn_other)
    unit_two, inv_two = unit_rows(resid)
    h_two = whole_rows((unit_two * gain_f).astype(BF))

    d_hidden = mm(grad_rows, full_down, 1, 1)
    gate, up = mm(h_two, full_gate, 1, 0), mm(h_two, full_up, 1, 0)
    gate_sigmoid = 1.0 / (1.0 + jnp.exp(-gate))
    gate_silu = gate * gate_sigmoid
    hidden = (gate_silu * up).astype(BF)
    slope = gate_sigmoid * (1.0 + gate * (1.0 - gate_sigmoid))
    d_gate = (d_hidden * up * slope).astype(BF)
    d_up = (d_hidden * gate_silu).astype(BF)

    def d_two_of(start):
        return mm(rows_of(d_gate, start), full_gate, 1, 1) + mm(rows_of(d_up, start), full_up, 1, 1)

    d_two = sum_tp(d_two_of(mine_row), d_two_of(other_row).astype(BF))
    cut = (ff_local // 256) * 128
    spans = [slice(0, cut), slice(cut, ff_local)]

    def down_grad(span):
        return lambda part: mm(hidden[:, span], part_of(grad_rows, part), 0, 0)

    def wide_grad(grad, span):
        return lambda part: mm(part_of(h_two, part), grad[:, span], 0, 0)

    chunks = [Reduction(down_grad(span), 1) for span in spans]
    for grad in (d_gate, d_up):
        chunks += [Reduction(wide_grad(grad, span), 0) for span in spans]
    ffn_other = mm(rows_of(hidden, other_row), full_down, 1, 0).astype(BF)
    ffn_mine = mm(rows_of(hidden, mine_row), full_down, 1, 0)
    block_output = turn(whole_rows(resid + sum_tp(ffn_mine, ffn_other)))

    part_ffn_gain = jnp.sum(d_two * unit_two, axis=0)
    d_resid = rows_of(grad_rows, mine_row).astype(F32) + norm_back(unit_two, inv_two, gain_f, d_two)
    d_attn = whole_rows(d_resid.astype(BF))

    d_heads_t = mm(full_out, d_attn, 1, 1).astype(BF)
    d_q = None
    d_kv_parts = [None] * n_ctx
    tokens_of = []
    for back in reversed(range(n_ctx)):
        d_q, d_kv = attend_back(
            back == 0, valids[back], q_t, kv_blocks[back], out_t, sums, d_heads_t, d_q
        )
        if back > 0:
            d_kv = over(d_kv, "ctx", [(i, i - back) for i in range(back, n_ctx)])
        d_kv_parts[back] = d_kv
        if back > 0 and len(tokens_of) < 2:
            tokens_of.append(d_q)
            chunks[len(tokens_of) - 1].inwards(d_q)
    chunks[0].across(d_q)
    chunks[2].inwards(d_q)
    out_chunk = Reduction(lambda part: mm(attn_t, part_of(d_attn, part), 1, 0), 1)
    d_raw_q_t, d_raw_kv_t, sum_q, sum_k = prep_back(
        raw_q_t, raw_kv_t, cos_t, sin_t, gain_q, gain_k, d_q, d_kv_parts
    )
    kv_chunk = Reduction(lambda part: mm(part_of(h_one, part), d_raw_kv_t, 0, 1), 0)
    q_chunk = Reduction(lambda part: mm(part_of(h_one, part), d_raw_q_t, 0, 1), 0)
    done = d_raw_q_t
    chunks[1].across(done)
    chunks[0].outwards(done)
    chunks[3].inwards(done)
    chunks[2].across(done)
    chunks[1].outwards(done)
    waiting = chunks[4:] + [out_chunk, kv_chunk, q_chunk]
    for chunk in waiting:
        chunk.inwards(done)
    for chunk in [chunks[3]] + waiting:
        chunk.across(done)
    for chunk in chunks[2:] + [out_chunk, kv_chunk, q_chunk]:
        chunk.outwards(done)

    def d_one_of(start):
        return mm(cols_of(d_raw_kv_t, start), full_kv, 0, 1) + mm(
            cols_of(d_raw_q_t, start), full_q, 0, 1
        )

    d_one = sum_tp(d_one_of(mine_row), d_one_of(other_row).astype(BF))
    unit_half, inv_half = rows_of(unit_one, mine_row), rows_of(inv_one, mine_row)
    part_attn_gain = jnp.sum(d_one * unit_half, axis=0)
    input_grad = turn(whole_rows(d_resid + norm_back(unit_half, inv_half, gain_a, d_one)))

    share = 2.0 / n_tp
    gain_grads = sum_all(
        row_of([turn(part_attn_gain) * share, turn(part_ffn_gain) * share, sum_q[:, 0], sum_k[:, 0]])
    )

    def joined(q, kv):
        pieces = []
        for g in range(groups):
            pieces += [q[:, g * split_at : (g + 1) * split_at]]
            pieces += [kv[:, g * 2 * HEAD_SIZE : (g + 1) * 2 * HEAD_SIZE]]
        return jnp.concatenate(pieces, axis=1)

    parts = [chunk.result() for chunk in chunks]
    grads = [
        joined(q_chunk.result(), kv_chunk.result()),
        out_chunk.result(),
        jnp.concatenate(parts[2:4], axis=1),
        jnp.concatenate(parts[4:6], axis=1),
        jnp.concatenate(parts[:2], axis=0),
    ]
    by_tp, by_fsdp = stats(grads)
    sums = [sum_over_tp(by_tp), sum_over_fsdp(by_fsdp)]
    squares = [squares_qkv, squares_out, squares_gate_up, squares_down]
    whole_grads, news, scales, scalars = scaled(
        (1.0 / n_tp, 1.0 / n_fsdp), grads, sums, olds, squares
    )
    totals = lax.psum(scalars, ("fsdp", "tp"))
    steps, new_vars, gain_steps, rms = finish(
        grads, scales, totals, gain_grads, gain_vars, gains_old
    )

    def gains_of(row):
        vector = row[0]
        ends = (0, D, 2 * D, 2 * D + HEAD_SIZE, 2 * D + 2 * HEAD_SIZE)
        return [vector[start:end] for start, end in zip(ends, ends[1:])]

    places = layout_of(grads)
    stat = lambda place: news[place[0]][0, place[1]]
    (row_qkv, col_qkv), (row_out, col_out), (row_gu, col_gate), (_, col_up), (row_down, col_down) = (
        (stat(row), stat(col)) for row, col in places
    )
    return (
        block_output[None],
        input_grad[None],
        *whole_grads,
        *gains_of(gain_grads),
        row_qkv,
        col_qkv,
        row_out,
        col_out,
        row_gu,
        jnp.stack([col_gate, col_up]),
        row_down,
        col_down,
        *gains_of(new_vars),
        *steps,
        *gains_of(gain_steps),
        rms[0, 0],
    )


def solution(mesh):
    tokens, vector = P("fsdp", "ctx", None), P()
    by_f, by_t = P("fsdp"), P("tp")
    w_specs = (P("fsdp", "tp"), P("tp", "fsdp"), P("fsdp", None, "tp"), P("tp", "fsdp"))
    stats = (by_f, by_t, by_t, by_f, by_f, P(None, "tp"), by_t, by_f) + (vector,) * 4
    return jax.shard_map(
        functools.partial(on_device, dict(mesh.shape)),
        mesh=mesh,
        in_specs=(tokens, tokens, by_f, P("fsdp", "ctx")) + w_specs + (vector,) * 4 + stats,
        out_specs=(tokens, tokens)
        + w_specs
        + (vector,) * 4
        + stats
        + w_specs
        + (vector,) * 4
        + (vector,),
        check_vma=False,
    )
```

```python
import functools
import math

import jax
import jax.numpy as jnp
from jax import lax
from jax.experimental import pallas as pl
from jax.experimental.pallas import tpu as pltpu
from jax.sharding import PartitionSpec as P

D = 1024
QUERY_HEADS = 16
KEY_VALUE_HEADS = 8
HEAD_SIZE = 64
FF = 4608
QKV = 2048

EPS = 1e-05
THETA = 1000000.0
DECAY = 0.5
CLIP = 0.15
RATE = 1.0

BF = jnp.bfloat16
F32 = jnp.float32
GROUP = QUERY_HEADS // KEY_VALUE_HEADS
LANES = (GROUP + 2) * HEAD_SIZE
KEY_TILE = 256
PAIR_BLOCKS = 4


def mm(left, right, left_dim, right_dim):
    return lax.dot_general(
        left, right, (((left_dim,), (right_dim,)), ((), ())), preferred_element_type=F32
    )


def params(vmem=48 << 20):
    return pltpu.CompilerParams(vmem_limit_bytes=vmem)


def squares_into(sum_ref, values):
    rows, cols = values.shape
    sum_ref[...] += jnp.sum((values * values).reshape(rows // 8, 8, cols), axis=0)


def cast_kernel(spans, w_ref, *refs):
    sum_ref = refs[-1]

    @pl.when(pl.program_id(0) == 0)
    def _():
        sum_ref[...] = jnp.zeros_like(sum_ref)

    values = w_ref[...]
    for out_ref, pieces in zip(refs, spans):
        at = 0
        for start, size in pieces:
            out_ref[:, at : at + size] = values[:, start : start + size].astype(BF)
            at += size
    squares_into(sum_ref, values)


def cast(weight, spans=None):
    rows, cols = weight.shape
    spans = spans or [[(0, cols)]]
    widths = [sum(size for _, size in pieces) for pieces in spans]
    block = min(rows, 128)
    return pl.pallas_call(
        functools.partial(cast_kernel, spans),
        grid=(rows // block,),
        in_specs=[pl.BlockSpec((block, cols), lambda i: (i, 0))],
        out_specs=[pl.BlockSpec((block, width), lambda i: (i, 0)) for width in widths]
        + [pl.BlockSpec((8, cols), lambda i: (0, 0))],
        out_shape=[jax.ShapeDtypeStruct((rows, width), BF) for width in widths]
        + [jax.ShapeDtypeStruct((8, cols), F32)],
        cost_estimate=pl.CostEstimate(
            flops=3 * rows * cols, bytes_accessed=6 * rows * cols, transcendentals=0
        ),
        compiler_params=params(),
        name="cast",
    )(weight)


def cast_pair_kernel(w_ref, gate_ref, up_ref, sum_ref, held, sems):
    rows = w_ref.shape[0]
    block = rows // PAIR_BLOCKS
    copies = []
    for step in range(PAIR_BLOCKS):
        for which in range(2):
            span = pl.ds(step * block, block)
            copies.append(
                pltpu.make_async_copy(
                    w_ref.at[span, which, :], held.at[which, span, :], sems.at[which, step]
                )
            )
            copies[-1].start()
    sum_ref[...] = jnp.zeros_like(sum_ref)
    for step in range(PAIR_BLOCKS):
        for which, out_ref in enumerate((gate_ref, up_ref)):
            copies[2 * step + which].wait()

            @pl.loop(0, block // 16)
            def _(piece):
                at = pl.multiple_of(step * block + piece * 16, 16)
                values = held[which, pl.ds(at, 16), :]
                out_ref[pl.ds(at, 16), :] = values.astype(BF)
                squares_into(sum_ref, values)


def cast_pair(weight):
    rows, _, cols = weight.shape
    vmem = pl.BlockSpec(memory_space=pltpu.VMEM)
    return pl.pallas_call(
        cast_pair_kernel,
        in_specs=[pl.BlockSpec(memory_space=pl.ANY)],
        out_specs=[vmem] * 3,
        out_shape=[jax.ShapeDtypeStruct((rows, cols), BF)] * 2
        + [jax.ShapeDtypeStruct((8, cols), F32)],
        scratch_shapes=[
            pltpu.VMEM((2, rows, cols), F32),
            pltpu.SemaphoreType.DMA((2, PAIR_BLOCKS)),
        ],
        cost_estimate=pl.CostEstimate(
            flops=6 * rows * cols, bytes_accessed=12 * rows * cols, transcendentals=0
        ),
        compiler_params=params(),
        name="cast_pair",
    )(weight)


def lane_total(values):
    lanes = min(128, values.shape[1])
    total = values[:, :lanes]
    for at in range(lanes, values.shape[1], lanes):
        total = total + values[:, at : at + lanes]
    return total


def padded(size):
    return -(-size // 128) * 128


def spans_of(sizes):
    out, at = [], 0
    for size in sizes:
        out.append(slice(at, at + size))
        at += padded(size)
    return out


def layout_of(grads):
    qkv, out, gate, up, down = (g.shape for g in grads)
    tp_spans = spans_of([qkv[0], gate[0], out[1], down[1]])
    fsdp_spans = spans_of([qkv[1], gate[1], up[1], out[0], down[0]])
    return (
        ((0, tp_spans[0]), (1, fsdp_spans[0])),
        ((1, fsdp_spans[3]), (0, tp_spans[2])),
        ((0, tp_spans[1]), (1, fsdp_spans[1])),
        ((0, tp_spans[1]), (1, fsdp_spans[2])),
        ((1, fsdp_spans[4]), (0, tp_spans[3])),
    )


def packed_sizes(grads):
    qkv, out, gate, up, down = (g.shape for g in grads)
    return (
        sum(map(padded, (qkv[0], gate[0], out[1], down[1]))),
        sum(map(padded, (qkv[1], gate[1], up[1], out[0], down[0]))),
    )


def over_blocks(n_rows, block, body, init=None):
    if n_rows == block:
        return body(0, init)
    aligned = lambda step, carry: body(pl.multiple_of(step * block, block), carry)
    return lax.fori_loop(0, n_rows // block, aligned, init)


def stats_kernel(*refs):
    grads, packed = refs[:5], refs[5:]
    for ref in packed:
        ref[...] = jnp.zeros_like(ref)
    for index, (grad_ref, places) in enumerate(zip(grads, layout_of(grads))):
        n_rows = grad_ref.shape[0]
        block = min(n_rows, 128)
        (row_at, row_span), (col_at, col_span) = places
        row_ref, col_ref = packed[row_at], packed[col_at]

        def add_block(at, carry):
            values = grad_ref[pl.ds(at, block), :].astype(F32)
            square = values * values
            col_ref[:, col_span] += jnp.sum(square, axis=0, keepdims=True)
            folded = jnp.sum(lane_total(square).T, axis=0, keepdims=True)
            start = row_span.start + at
            place = pl.ds(start if n_rows == block else pl.multiple_of(start, block), block)
            row_ref[:, place] += folded
            return carry

        over_blocks(n_rows, block, add_block, 0)


def stats(grads):
    vmem = pl.BlockSpec(memory_space=pltpu.VMEM)
    return pl.pallas_call(
        stats_kernel,
        in_specs=[vmem] * 5,
        out_specs=[vmem] * 2,
        out_shape=[jax.ShapeDtypeStruct((1, size), F32) for size in packed_sizes(grads)],
        cost_estimate=pl.CostEstimate(
            flops=4 * sum(g.size for g in grads),
            bytes_accessed=2 * sum(g.size for g in grads),
            transcendentals=0,
        ),
        compiler_params=params(),
        name="stats",
    )(*grads)


def columns_of(row, width):
    return jnp.broadcast_to(row, (min(128, width), row.shape[1])).T


def total_of(values):
    return jnp.sum(jnp.sum(values, axis=0, keepdims=True), axis=1, keepdims=True)


def out_views(outs):
    qkv, out, gate_up, down = outs
    return (
        lambda span: qkv.at[span, :],
        lambda span: out.at[span, :],
        lambda span: gate_up.at[span, 0, :],
        lambda span: gate_up.at[span, 1, :],
        lambda span: down.at[span, :],
    )


def tiles_in(grads):
    for index, grad_ref in enumerate(grads):
        block = min(grad_ref.shape[0], 128)
        for at in range(0, grad_ref.shape[0], block):
            yield index, at, block


def write_shapes(grads):
    qkv, out, gate, _, down = (g.shape for g in grads)
    return [
        jax.ShapeDtypeStruct(shape, F32) for shape in (qkv, out, (gate[0], 2, gate[1]), down)
    ]


def write_scratch(grads):
    count = len(list(tiles_in(grads)))
    return [pltpu.VMEM(g.shape, F32) for g in grads] + [pltpu.SemaphoreType.DMA((count,))]


def scaled_kernel(shares, *refs):
    grads, sums, olds, squares = refs[:5], refs[5:7], refs[7:9], refs[9:13]
    outs, news, scale_refs, scalar_ref = refs[13:17], refs[17:19], refs[19:21], refs[21]
    held, sems = refs[22:27], refs[27]
    copies = []
    views = out_views(outs)
    for number, (index, at, block) in enumerate(tiles_in(grads)):
        span = pl.ds(at, block)
        held[index][span, :] = grads[index][span, :].astype(F32)
        copies.append(
            pltpu.make_async_copy(held[index].at[span, :], views[index](span), sems.at[number])
        )
        copies[-1].start()
    places = layout_of(grads)
    counts = ((QKV, D), (D, D), (2 * FF, D), (2 * FF, D), (D, FF))
    scalars = []
    for (row_place, col_place), count in zip(places, counts):
        for (at, span), size in zip((row_place, col_place), count):
            new = DECAY * olds[at][:, span] + (1.0 - DECAY) * (sums[at][:, span] / size)
            news[at][:, span] = new
            scale_refs[at][:, span] = lax.rsqrt(new)
    scaled = []
    for index, (row_place, col_place) in enumerate(places):
        grad_ref = grads[index]
        n_rows, n_cols = grad_ref.shape
        block = min(n_rows, 128)
        lanes = min(128, n_cols)
        left_ref, row_start = scale_refs[row_place[0]], row_place[1].start
        right = scale_refs[col_place[0]][:, col_place[1]]

        def step_of(at, total):
            values = held[index][pl.ds(at, block), :] * right
            start = row_start + at
            place = pl.ds(start if n_rows == block else pl.multiple_of(start, block), block)
            left = columns_of(left_ref[:, place], n_cols)
            folded = lane_total(values * values) * (left * left)
            return total + jnp.sum(folded.reshape(block // 8, 8, lanes), axis=0)

        total = over_blocks(n_rows, block, step_of, jnp.zeros((8, lanes), F32))
        scaled.append(total_of(total))
    scalars += [scaled[0], scaled[1], scaled[2] + scaled[3], scaled[4]]
    row_places = [places[index][0] for index in (0, 1, 2, 4)]
    scalars += [total_of(sums[at][:, span]) * shares[at] for at, span in row_places]
    scalars += [total_of(ref[...]) for ref in squares]
    scalars += [total_of(olds[at][:, span]) * shares[at] for at, span in row_places]
    lane = lax.broadcasted_iota(jnp.int32, (8, 128), 1)
    packed = jnp.zeros((8, 128), F32)
    for number, value in enumerate(scalars):
        packed = jnp.where(lane == number, value, packed)
    scalar_ref[...] = packed
    for copy in copies:
        copy.wait()


def scaled(shares, grads, sums, olds, squares):
    vmem, hbm = pl.BlockSpec(memory_space=pltpu.VMEM), pl.BlockSpec(memory_space=pl.ANY)
    vectors = [jax.ShapeDtypeStruct((1, size), F32) for size in packed_sizes(grads)]
    out = pl.pallas_call(
        functools.partial(scaled_kernel, shares),
        in_specs=[vmem] * 13,
        out_specs=[hbm] * 4 + [vmem] * 5,
        out_shape=write_shapes(grads) + vectors * 2 + [jax.ShapeDtypeStruct((8, 128), F32)],
        scratch_shapes=write_scratch(grads),
        cost_estimate=pl.CostEstimate(
            flops=6 * sum(g.size for g in grads),
            bytes_accessed=6 * sum(g.size for g in grads),
            transcendentals=0,
        ),
        compiler_params=params(),
        name="scaled",
    )(*grads, *sums, *olds, *squares)
    return out[:4], out[4:6], out[6:8], out[8]


def finish_kernel(*refs):
    grads, scale_refs, total_ref = refs[:5], refs[5:7], refs[7]
    gain_grad_ref, var_ref, gain_ref = refs[8:11]
    outs, new_var_ref, gain_step_ref, rms_ref = refs[11:15], refs[15], refs[16], refs[17]
    held, sems = refs[18:23], refs[23]
    value = lambda number: total_ref[0:1, number : number + 1]
    sizes = ((D, QKV), (D, D), (D, 2 * FF), (FF, D))
    means = [
        DECAY * value(12 + index) / rows + (1.0 - DECAY) * value(4 + index) / (rows * cols)
        for index, (rows, cols) in enumerate(sizes)
    ]
    gain_grad = gain_grad_ref[...]
    new_var = DECAY * var_ref[...] + (1.0 - DECAY) * gain_grad * gain_grad
    new_var_ref[...] = new_var
    raw_gain = gain_grad * lax.rsqrt(new_var)
    total = jnp.sum(raw_gain * raw_gain, axis=1, keepdims=True)
    for index, mean in enumerate(means):
        total = total + value(index) * mean
    count = D * QKV + D * D + 2 * D * FF + FF * D + 2 * D + 2 * HEAD_SIZE
    rms = jnp.sqrt(total / count)
    rms_ref[...] = jnp.broadcast_to(rms, rms_ref.shape)
    clip = jnp.maximum(1.0, rms / CLIP)
    factors = [
        -RATE * jnp.sqrt(value(8 + index) / (rows * cols)) * jnp.sqrt(means[index]) / clip
        for index, (rows, cols) in enumerate(sizes)
    ]
    copies = []
    views, places = out_views(outs), layout_of(grads)
    tensor_of = (0, 1, 2, 2, 3)
    for number, (index, at, block) in enumerate(tiles_in(grads)):
        span = pl.ds(at, block)
        (row_at, row_span), (col_at, col_span) = places[index]
        start = row_span.start + at
        n_cols = grads[index].shape[1]
        left = columns_of(scale_refs[row_at][:, start : start + block], n_cols)
        right = scale_refs[col_at][:, col_span] * factors[tensor_of[index]]
        for first in range(0, n_cols, left.shape[1]):
            lanes = slice(first, first + left.shape[1])
            tile = grads[index][span, lanes].astype(F32)
            held[index][span, lanes] = tile * left * right[:, lanes]
        copies.append(
            pltpu.make_async_copy(held[index].at[span, :], views[index](span), sems.at[number])
        )
        copies[-1].start()
    for start, size in ((0, D), (D, D)):
        span = slice(start, start + size)
        gain = gain_ref[:, span]
        scale = -RATE * jnp.sqrt(jnp.sum(gain * gain, axis=1, keepdims=True) / size) / clip
        gain_step_ref[:, span] = raw_gain[:, span] * scale
    span = slice(2 * D, 2 * D + 2 * HEAD_SIZE)
    gain = gain_ref[:, span]
    low = lax.broadcasted_iota(jnp.int32, gain.shape, 1) < HEAD_SIZE
    square = gain * gain
    low_sum = jnp.sum(jnp.where(low, square, 0.0), axis=1, keepdims=True)
    high_sum = jnp.sum(jnp.where(low, 0.0, square), axis=1, keepdims=True)
    scale = -RATE * jnp.sqrt(jnp.where(low, low_sum, high_sum) / HEAD_SIZE) / clip
    gain_step_ref[:, span] = raw_gain[:, span] * scale
    for copy in copies:
        copy.wait()


def finish(grads, scales, totals, gain_grads, gain_vars, gains):
    vmem, hbm = pl.BlockSpec(memory_space=pltpu.VMEM), pl.BlockSpec(memory_space=pl.ANY)
    vector = jax.ShapeDtypeStruct(gains.shape, F32)
    out = pl.pallas_call(
        finish_kernel,
        in_specs=[vmem] * 11,
        out_specs=[hbm] * 4 + [vmem] * 3,
        out_shape=write_shapes(grads) + [vector, vector, jax.ShapeDtypeStruct((8, 128), F32)],
        scratch_shapes=write_scratch(grads),
        cost_estimate=pl.CostEstimate(
            flops=4 * sum(g.size for g in grads),
            bytes_accessed=6 * sum(g.size for g in grads),
            transcendentals=0,
        ),
        compiler_params=params(),
        name="finish",
    )(*grads, *scales, totals, gain_grads, gain_vars, gains)
    return out[:4], out[4], out[5], out[6]


def pieces_of(shapes):
    out = []
    for index, (rows, cols) in enumerate(shapes):
        size = rows
        while size % 32 == 0 and size * cols > 96 * 1024:
            size //= 2 if size % 64 == 0 else 3
        out += [(index, at, size) for at in range(0, rows, size)]
    return out


def line_kernel(shapes, arrived, pairs, *refs):
    count = len(shapes)
    refs = list(refs)
    take = lambda size: [refs.pop(0) for _ in range(size)]
    mine = take(count)
    theirs = take(arrived if pairs else 0)
    sends = take(count - arrived if pairs else 0)
    final = take(count)
    work, land, cross = take(count), take(count), take(count)
    theirs += take(count - arrived if pairs else 0)
    in_send, in_recv, mid_send, mid_recv, out_send, out_recv, x_send, x_recv = refs
    me = lax.axis_index("ctx")
    partner = me + 1 - 2 * (me % 2)
    opposite = 3 - me
    at_end = (me == 0) | (me == 3)
    lanes = [{"ctx": partner}, {"ctx": opposite}]
    if pairs:
        lanes.append({"fsdp": 1 - lax.axis_index("fsdp")})
    barrier = pltpu.get_barrier_semaphore()
    for lane in lanes:
        pl.semaphore_signal(barrier, inc=1, device_id=lane, device_id_type=pl.DeviceIdType.MESH)
    pl.semaphore_wait(barrier, len(lanes))

    def remote(source, target, send, recv, number, lane):
        index, at, size = pieces[number]
        span = pl.ds(at, size)
        return pltpu.make_async_remote_copy(
            src_ref=source[index].at[span, :],
            dst_ref=target[index].at[span, :],
            send_sem=send.at[number],
            recv_sem=recv.at[number],
            device_id=lanes[lane],
            device_id_type=pl.DeviceIdType.MESH,
        )

    pieces = pieces_of(shapes)
    numbers = range(len(pieces))
    inwards = [remote(work, land, in_send, in_recv, i, 0) for i in numbers]
    across = [remote(work, cross, mid_send, mid_recv, i, 1) for i in numbers]
    outwards = [remote(final, final, out_send, out_recv, i, 0) for i in numbers]
    exchanged = {}
    if pairs:
        padded_sends = [None] * arrived + sends
        for i in numbers:
            if pieces[i][0] >= arrived:
                exchanged[i] = remote(padded_sends, theirs, x_send, x_recv, i, 2)
                exchanged[i].start()

    def add(target, number, *sources):
        index, at, size = pieces[number]
        step = 32 if size % 32 == 0 else 16

        @pl.loop(0, size // step)
        def _(piece):
            span = pl.ds(pl.multiple_of(at + piece * step, 16), step)
            total = sources[0][index][span, :].astype(F32)
            for source in sources[1:]:
                total = total + source[index][span, :].astype(F32)
            target[index][span, :] = total.astype(BF)

    own = (mine, theirs) if pairs else (mine,)

    def ready(number):
        if number in exchanged:
            exchanged[number].wait_recv()

    @pl.when(at_end)
    def _():
        for i in numbers:
            ready(i)
            add(work, i, *own)
            inwards[i].start()
        for i in numbers:
            inwards[i].wait_send()
            outwards[i].wait_recv()

    @pl.when(jnp.logical_not(at_end))
    def _():
        lag = 2
        for i in range(len(pieces) + lag):
            if i < len(pieces):
                ready(i)
                inwards[i].wait_recv()
                add(work, i, *own, land)
                across[i].start()
            if i >= lag:
                across[i - lag].wait_recv()
                add(final, i - lag, work, cross)
                outwards[i - lag].start()
        for i in numbers:
            across[i].wait_send()
            outwards[i].wait_send()

    for copy in exchanged.values():
        copy.wait_send()


def line_sums(mine, theirs, sends):
    shapes = [m.shape for m in mine]
    pairs = bool(sends) or bool(theirs)
    count, arrived = len(mine), len(theirs)
    number = len(pieces_of(shapes))
    vmem = pl.BlockSpec(memory_space=pltpu.VMEM)
    held = [pltpu.VMEM(shape, BF) for shape in shapes]
    size = sum(m.size for m in mine)
    return pl.pallas_call(
        functools.partial(line_kernel, shapes, arrived, pairs),
        in_specs=[vmem] * (count + len(theirs) + len(sends)),
        out_specs=[vmem] * count,
        out_shape=[jax.ShapeDtypeStruct(shape, BF) for shape in shapes],
        scratch_shapes=held * 3
        + (held[arrived:] if pairs else [])
        + [pltpu.SemaphoreType.DMA((number,))] * 8,
        cost_estimate=pl.CostEstimate(flops=4 * size, bytes_accessed=80 * size, transcendentals=0),
        compiler_params=pltpu.CompilerParams(
            vmem_limit_bytes=56 << 20, collective_id=0, has_side_effects=True
        ),
        name="line_sums",
    )(*mine, *theirs, *sends)


def turned_head(rows, gain, cos_t, sin_t):
    half = HEAD_SIZE // 2
    inv = lax.rsqrt(jnp.mean(rows * rows, axis=0, keepdims=True) + EPS)
    normed = rows * inv * gain
    low, high = normed[:half], normed[half:]
    return jnp.concatenate([low * cos_t - high * sin_t, high * cos_t + low * sin_t], axis=0)


def queries_kernel(raw_ref, cos_ref, sin_ref, gain_ref, q_ref):
    turned = turned_head(raw_ref[...], gain_ref[...], cos_ref[...], sin_ref[...])
    scale = 1.0 / math.sqrt(HEAD_SIZE)
    q_ref[...] = (turned.astype(BF).astype(F32) * scale).astype(BF)


def keys_kernel(raw_ref, cos_ref, sin_ref, gain_ref, kv_ref):
    turned = turned_head(raw_ref[:HEAD_SIZE, :], gain_ref[...], cos_ref[...], sin_ref[...])
    kv_ref[:HEAD_SIZE, :] = turned.astype(BF)
    kv_ref[HEAD_SIZE:, :] = raw_ref[HEAD_SIZE:, :].astype(BF)


def prep_call(kernel, size, raw_t, cos_t, sin_t, gain):
    rows, tokens = raw_t.shape
    half = HEAD_SIZE // 2
    fixed = lambda g: (0, 0)
    return pl.pallas_call(
        kernel,
        grid=(rows // size,),
        in_specs=[
            pl.BlockSpec((size, tokens), lambda g: (g, 0)),
            pl.BlockSpec((half, tokens), fixed),
            pl.BlockSpec((half, tokens), fixed),
            pl.BlockSpec((HEAD_SIZE, 1), fixed),
        ],
        out_specs=pl.BlockSpec((size, tokens), lambda g: (g, 0)),
        out_shape=jax.ShapeDtypeStruct(raw_t.shape, BF),
        cost_estimate=pl.CostEstimate(
            flops=20 * rows * tokens, bytes_accessed=6 * rows * tokens, transcendentals=0
        ),
        compiler_params=params(),
        name="prep",
    )(raw_t, cos_t, sin_t, gain)


prep_queries = functools.partial(prep_call, queries_kernel, HEAD_SIZE)
prep_keys = functools.partial(prep_call, keys_kernel, 2 * HEAD_SIZE)


def prep_back_kernel(parts, *refs):
    raw_q_ref, raw_kv_ref, cos_ref, sin_ref, gq_ref, gk_ref, dq_ref = refs[:7]
    dkv_refs = refs[7 : 7 + parts]
    out_q_ref, out_kv_ref, sum_q_ref, sum_k_ref = refs[7 + parts :]
    half = HEAD_SIZE // 2
    cos_t, sin_t = cos_ref[...], sin_ref[...]
    d_kv = dkv_refs[0][...]
    for ref in dkv_refs[1:]:
        d_kv = d_kv + ref[...].astype(F32)

    @pl.when(pl.program_id(0) == 0)
    def _():
        sum_q_ref[...] = jnp.zeros_like(sum_q_ref)
        sum_k_ref[...] = jnp.zeros_like(sum_k_ref)

    for piece in range(GROUP + 1):
        base = piece * HEAD_SIZE
        if piece < GROUP:
            rows = raw_q_ref[base : base + HEAD_SIZE, :]
            grad = dq_ref[base : base + HEAD_SIZE, :] * (1.0 / math.sqrt(HEAD_SIZE))
            gain, sum_ref = gq_ref[...], sum_q_ref
        else:
            rows = raw_kv_ref[:HEAD_SIZE, :]
            grad = d_kv[:HEAD_SIZE]
            gain, sum_ref = gk_ref[...], sum_k_ref
        inv = lax.rsqrt(jnp.mean(rows * rows, axis=0, keepdims=True) + EPS)
        unit = rows * inv
        low, high = grad[:half], grad[half:]
        turned = jnp.concatenate([low * cos_t + high * sin_t, high * cos_t - low * sin_t], axis=0)
        sum_ref[...] += jnp.sum(turned * unit, axis=1, keepdims=True)
        scaled = turned * gain
        mean = jnp.mean(scaled * unit, axis=0, keepdims=True)
        result = ((scaled - unit * mean) * inv).astype(BF)
        if piece < GROUP:
            out_q_ref[base : base + HEAD_SIZE, :] = result
        else:
            out_kv_ref[:HEAD_SIZE, :] = result
    out_kv_ref[HEAD_SIZE:, :] = d_kv[HEAD_SIZE:].astype(BF)


def prep_back(raw_q_t, raw_kv_t, cos_t, sin_t, gain_q, gain_k, d_q, d_kv_parts):
    tokens = raw_q_t.shape[1]
    groups = raw_kv_t.shape[0] // (2 * HEAD_SIZE)
    rows = raw_q_t.shape[0] + raw_kv_t.shape[0]
    half = HEAD_SIZE // 2
    fixed = lambda g: (0, 0)
    block = lambda size: pl.BlockSpec((size, tokens), lambda g: (g, 0))
    return pl.pallas_call(
        functools.partial(prep_back_kernel, len(d_kv_parts)),
        grid=(groups,),
        in_specs=[
            block(GROUP * HEAD_SIZE),
            block(2 * HEAD_SIZE),
            pl.BlockSpec((half, tokens), fixed),
            pl.BlockSpec((half, tokens), fixed),
            pl.BlockSpec((HEAD_SIZE, 1), fixed),
            pl.BlockSpec((HEAD_SIZE, 1), fixed),
            block(GROUP * HEAD_SIZE),
        ]
        + [block(2 * HEAD_SIZE)] * len(d_kv_parts),
        out_specs=[
            block(GROUP * HEAD_SIZE),
            block(2 * HEAD_SIZE),
            pl.BlockSpec((HEAD_SIZE, 128), fixed),
            pl.BlockSpec((HEAD_SIZE, 128), fixed),
        ],
        out_shape=[
            jax.ShapeDtypeStruct(raw_q_t.shape, BF),
            jax.ShapeDtypeStruct(raw_kv_t.shape, BF),
            jax.ShapeDtypeStruct((HEAD_SIZE, 128), F32),
            jax.ShapeDtypeStruct((HEAD_SIZE, 128), F32),
        ],
        cost_estimate=pl.CostEstimate(
            flops=30 * rows * tokens, bytes_accessed=9 * rows * tokens, transcendentals=0
        ),
        compiler_params=params(),
        name="prep_back",
    )(raw_q_t, raw_kv_t, cos_t, sin_t, gain_q, gain_k, d_q, *d_kv_parts)


def tiles_of(diagonal, tokens):
    for key_start in range(0, tokens, KEY_TILE):
        yield key_start, key_start if diagonal else 0


def tile_probs(kv_ref, query, key_start, query_start, valid, diagonal):
    keys = kv_ref[:HEAD_SIZE, key_start : key_start + KEY_TILE]
    scores = mm(keys, query, 0, 0)
    key_index = key_start + lax.broadcasted_iota(jnp.int32, scores.shape, 0)
    visible = key_index < valid
    if diagonal:
        query_index = query_start + lax.broadcasted_iota(jnp.int32, scores.shape, 1)
        visible = visible & (key_index <= query_index)
    return keys, visible, jnp.exp(scores)


def attend_kernel(diagonal, valid_ref, q_ref, kv_ref, *refs):
    if diagonal:
        acc_ref, sum_ref = refs
        acc_ref[...] = jnp.zeros_like(acc_ref)
        sum_ref[...] = jnp.zeros_like(sum_ref)
    else:
        acc_in_ref, sum_in_ref, acc_ref, sum_ref = refs
        acc_ref[...] = acc_in_ref[...]
        sum_ref[...] = sum_in_ref[...]
    valid = valid_ref[0]
    tokens = q_ref.shape[1]

    @pl.when(valid > 0)
    def _():
        for key_start, query_start in tiles_of(diagonal, tokens):
            query = q_ref[:, query_start:]
            keys, visible, raised = tile_probs(
                kv_ref, query, key_start, query_start, valid, diagonal
            )
            probs = jnp.where(visible, raised, 0.0)
            sum_ref[:, query_start:] += jnp.sum(probs, axis=0, keepdims=True)
            values = kv_ref[HEAD_SIZE:, key_start : key_start + KEY_TILE]
            acc_ref[:, query_start:] += mm(values, probs.astype(BF), 1, 0)


def attend(diagonal, valid, q_t, kv_t, state):
    rows, tokens = q_t.shape
    heads = rows // HEAD_SIZE
    per_head = pl.BlockSpec((HEAD_SIZE, tokens), lambda h: (h, 0))
    sums = pl.BlockSpec((8, tokens), lambda h: (h, 0))
    carried = [] if diagonal else [per_head, sums]
    return pl.pallas_call(
        functools.partial(attend_kernel, diagonal),
        grid=(heads,),
        in_specs=[
            pl.BlockSpec(memory_space=pltpu.SMEM),
            per_head,
            pl.BlockSpec((2 * HEAD_SIZE, tokens), lambda h: (h // GROUP, 0)),
        ]
        + carried,
        out_specs=[per_head, sums],
        out_shape=[
            jax.ShapeDtypeStruct((rows, tokens), F32),
            jax.ShapeDtypeStruct((heads * 8, tokens), F32),
        ],
        input_output_aliases={} if diagonal else {3: 0, 4: 1},
        cost_estimate=pl.CostEstimate(
            flops=4 * rows * tokens * tokens,
            bytes_accessed=10 * rows * tokens,
            transcendentals=heads * tokens * tokens,
        ),
        compiler_params=params(),
        name="attend",
    )(valid, q_t, kv_t, *state)


def attend_back_kernel(diagonal, first, valid_ref, q_ref, kv_ref, out_ref, sum_ref, do_ref, *refs):
    if first:
        dq_ref, dkv_ref, dkv_acc = refs
        dq_ref[...] = jnp.zeros_like(dq_ref)
    else:
        dq_in_ref, dq_ref, dkv_ref, dkv_acc = refs
        dq_ref[...] = dq_in_ref[...]
    head = pl.program_id(0)
    valid = valid_ref[0]
    tokens = q_ref.shape[1]

    @pl.when(head % GROUP == 0)
    def _():
        dkv_acc[...] = jnp.zeros_like(dkv_acc)

    @pl.when(valid > 0)
    def _():
        inverse = 1.0 / sum_ref[0:1, :]
        delta = jnp.sum(do_ref[...].astype(F32) * out_ref[...], axis=0, keepdims=True)
        for key_start, query_start in tiles_of(diagonal, tokens):
            query = q_ref[:, query_start:]
            grads = do_ref[:, query_start:]
            keys, visible, raised = tile_probs(
                kv_ref, query, key_start, query_start, valid, diagonal
            )
            probs = jnp.where(visible, raised * inverse[:, query_start:], 0.0)
            span = slice(key_start, key_start + KEY_TILE)
            values = kv_ref[HEAD_SIZE:, span]
            d_probs = mm(values, grads, 0, 0)
            d_scores = (probs * (d_probs - delta[:, query_start:])).astype(BF)
            dq_ref[:, query_start:] += mm(keys, d_scores, 1, 0)
            dkv_acc[:HEAD_SIZE, span] += mm(query, d_scores, 1, 1)
            dkv_acc[HEAD_SIZE:, span] += mm(grads, probs.astype(BF), 1, 1)

    @pl.when(head % GROUP == GROUP - 1)
    def _():
        dkv_ref[...] = dkv_acc[...].astype(dkv_ref.dtype)


def attend_back(diagonal, valid, q_t, kv_t, out_t, sums, d_out_t, d_q):
    rows, tokens = q_t.shape
    heads = rows // HEAD_SIZE
    first = d_q is None
    per_head = pl.BlockSpec((HEAD_SIZE, tokens), lambda h: (h, 0))
    per_group = pl.BlockSpec((2 * HEAD_SIZE, tokens), lambda h: (h // GROUP, 0))
    return pl.pallas_call(
        functools.partial(attend_back_kernel, diagonal, first),
        grid=(heads,),
        in_specs=[
            pl.BlockSpec(memory_space=pltpu.SMEM),
            per_head,
            per_group,
            per_head,
            pl.BlockSpec((8, tokens), lambda h: (h, 0)),
            per_head,
        ]
        + ([] if first else [per_head]),
        out_specs=[per_head, per_group],
        out_shape=[
            jax.ShapeDtypeStruct((rows, tokens), F32),
            jax.ShapeDtypeStruct(kv_t.shape, F32 if diagonal else BF),
        ],
        scratch_shapes=[pltpu.VMEM((2 * HEAD_SIZE, tokens), F32)],
        input_output_aliases={} if first else {6: 0},
        cost_estimate=pl.CostEstimate(
            flops=10 * rows * tokens * tokens,
            bytes_accessed=14 * rows * tokens,
            transcendentals=heads * tokens * tokens,
        ),
        compiler_params=params(),
        name="attend_back",
    )(valid, q_t, kv_t, out_t, sums, d_out_t, *([] if first else [d_q]))


def unit_rows(values):
    inv = lax.rsqrt(jnp.mean(values * values, axis=-1, keepdims=True) + EPS)
    return values * inv, inv


def norm_back(unit, inv, gain, grad):
    scaled = grad * gain
    return (scaled - unit * jnp.mean(scaled * unit, axis=-1, keepdims=True)) * inv


def kept(value):
    return lax.optimization_barrier(value)


def on_device(
    sizes,
    block_input,
    cotangent,
    seq_lengths,
    positions,
    w_qkv,
    w_out,
    w_gate_up,
    w_down,
    gain_attn,
    gain_ffn,
    gain_query,
    gain_key,
    row_qkv_old,
    col_qkv_old,
    row_out_old,
    col_out_old,
    row_gate_up_old,
    col_gate_up_old,
    row_down_old,
    col_down_old,
    var_attn_old,
    var_ffn_old,
    var_query_old,
    var_key_old,
):
    n_fsdp, n_ctx, n_tp = sizes["fsdp"], sizes["ctx"], sizes["tp"]
    paired = n_fsdp == 2
    me_f, me_z, me_t = (lax.axis_index(name) for name in ("fsdp", "ctx", "tp"))
    tokens = block_input.shape[1]
    half = tokens // 2
    mine_row = (me_t % 2) * half
    other_row = half - mine_row

    def turn(values):
        if not paired:
            return values
        size = values.shape[-1] // 2
        swapped = jnp.concatenate([values[..., size:], values[..., :size]], axis=-1)
        return jnp.where(me_f == 0, values, swapped)

    def over(values, axis, pairs):
        return lax.ppermute(values, axis, pairs)

    def to_core(values):
        return over(values, "tp", [(i, i ^ 1) for i in range(n_tp)])

    def to_pair(values):
        return over(values, "fsdp", [(0, 1), (1, 0)])

    def gather_weight(shard, axis):
        if not paired:
            return lax.all_gather(shard, "fsdp", axis=axis, tiled=True)
        return jnp.concatenate([shard, to_pair(shard)], axis=axis)

    routed_by_ctx = paired and n_ctx % 2 == 0

    def first_half(shard):
        if not routed_by_ctx:
            return None
        size = shard.shape[0] // 2
        return to_pair(lax.dynamic_slice_in_dim(shard, me_z % 2 * size, size, 0))

    def second_half(shard, direct, axis):
        if not routed_by_ctx:
            return gather_weight(shard, axis)
        routed = over(direct, "ctx", [(i, i ^ 1) for i in range(n_ctx)])
        odd = me_z % 2
        first = jnp.where(odd == 0, direct, routed)
        second = jnp.where(odd == 0, routed, direct)
        other = jnp.concatenate([first, second], axis=0)
        return jnp.concatenate([shard, other], axis=axis)

    def sum_tp(mine, other_low):
        total = mine + to_core(other_low).astype(F32)
        step = 2
        while step < n_tp:
            low = kept(total.astype(BF))
            pairs = [(i, i ^ step) for i in range(n_tp)]
            total = low.astype(F32) + over(low, "tp", pairs).astype(F32)
            step *= 2
        return total

    def whole_rows(values):
        other = to_core(values)
        first = jnp.where(mine_row == 0, values, other)
        second = jnp.where(mine_row == 0, other, values)
        return jnp.concatenate([first, second], axis=0)

    def rows_of(values, start):
        return lax.dynamic_slice_in_dim(values, start, half, 0)

    def after(value, *tokens):
        return lax.optimization_barrier((value,) + tokens)[0]

    def shares_of(make, axis):
        if paired:
            return make(0).astype(BF), make(1).astype(BF)
        whole = make(None)
        return (
            lax.psum_scatter(whole, "fsdp", scatter_dimension=axis, tiled=True).astype(BF),
            None,
        )

    def sum_over_tp(values):
        step = 1
        while step < n_tp:
            values = values + over(values, "tp", [(i, i ^ step) for i in range(n_tp)])
            step *= 2
        return values

    def sum_over_fsdp(values):
        return values + to_pair(values) if paired else lax.psum(values, "fsdp")

    def sum_over_ctx(values):
        step = 1
        while step < n_ctx:
            values = values + over(values, "ctx", [(i, i ^ step) for i in range(n_ctx)])
            step *= 2
        return values

    def sum_all(values):
        return sum_over_ctx(sum_over_fsdp(sum_over_tp(values)))

    def part_of(values, part):
        if part is None:
            return values
        size = values.shape[-1] // 2
        return values[..., part * size : (part + 1) * size]

    groups = w_qkv.shape[1] // LANES
    split_at = GROUP * HEAD_SIZE
    q_spans = [(g * LANES, split_at) for g in range(groups)]
    kv_spans = [(g * LANES + split_at, 2 * HEAD_SIZE) for g in range(groups)]
    shard_q, shard_kv, squares_qkv = cast(w_qkv, [q_spans, kv_spans])
    full_kv = gather_weight(shard_kv, 0)
    full_q = gather_weight(shard_q, 0)
    shard_out, squares_out = cast(w_out)
    full_out = gather_weight(shard_out, 1)
    ff_local = w_gate_up.shape[2]
    shard_gate, shard_up, squares_gate_up = cast_pair(w_gate_up)
    direct_gate, direct_up = first_half(shard_gate), first_half(shard_up)

    olds = [
        jnp.concatenate([jnp.pad(v, (0, padded(v.size) - v.size)) for v in vectors]).reshape(1, -1)
        for vectors in (
            (row_qkv_old, row_gate_up_old, col_out_old, col_down_old),
            (col_qkv_old, col_gate_up_old[0], col_gate_up_old[1], row_out_old, row_down_old),
        )
    ]
    row_of = lambda vectors: jnp.concatenate(vectors).reshape(1, 2 * D + 2 * HEAD_SIZE)
    gain_vars = row_of([var_attn_old, var_ffn_old, var_query_old, var_key_old])
    gains_old = row_of([gain_attn, gain_ffn, gain_query, gain_key])

    inputs32 = turn(block_input[0].astype(F32))
    grad_rows = turn(cotangent[0])
    gain_a, gain_f = turn(gain_attn), turn(gain_ffn)
    unit_one, inv_one = unit_rows(inputs32)
    h_one = (unit_one * gain_a).astype(BF)
    freq = jnp.exp(
        jnp.arange(HEAD_SIZE // 2, dtype=F32) * (-2.0 * math.log(THETA) / HEAD_SIZE)
    )
    angle = freq[:, None] * positions[0].astype(F32)[None, :]
    cos_t, sin_t = jnp.cos(angle), jnp.sin(angle)
    gain_q, gain_k = gain_query[:, None], gain_key[:, None]
    raw_kv_t = mm(full_kv, h_one, 0, 1)
    kv_t = prep_keys(raw_kv_t, cos_t, sin_t, gain_k)
    shard_down, squares_down = cast(after(w_down, kv_t))
    direct_down = first_half(shard_down)
    raw_q_t = mm(full_q, h_one, 0, 1)
    q_t = prep_queries(raw_q_t, cos_t, sin_t, gain_q)

    length = seq_lengths[0]
    kv_blocks, valids = [], []
    for back in range(n_ctx):
        moved = kv_t
        if back > 0:
            moved = over(kv_t, "ctx", [(i, i + back) for i in range(n_ctx - back)])
        kv_blocks.append(moved)
        count = jnp.clip(length - (me_z - back) * tokens, 0, tokens)
        valids.append(jnp.where(me_z >= back, count, 0).astype(jnp.int32).reshape(1))
    state = []
    for back in range(n_ctx):
        query = q_t
        if routed_by_ctx and 0 < back < 3:
            query = after(q_t, (direct_gate, direct_up)[back - 1])
        state = attend(back == 0, valids[back], query, kv_blocks[back], state)
        if back == 1:
            full_gate = second_half(shard_gate, direct_gate, 0)
        if back == min(2, n_ctx - 1):
            full_up = second_half(shard_up, direct_up, 0)
    acc_t, sums = state
    heads = acc_t.shape[0] // HEAD_SIZE
    inverse = (1.0 / sums.reshape(heads, 8, tokens)[:, :1, :])
    out_t = (acc_t.reshape(heads, HEAD_SIZE, tokens) * inverse).reshape(acc_t.shape)
    attn_t = kept(out_t.astype(BF))
    full_down = second_half(shard_down, direct_down, 1)

    def cols_of(values, start):
        return lax.dynamic_slice_in_dim(values, start, half, 1)

    attn_other = mm(cols_of(attn_t, other_row), full_out, 0, 0).astype(BF)
    attn_mine = mm(cols_of(attn_t, mine_row), full_out, 0, 0)
    resid = rows_of(inputs32, mine_row) + sum_tp(attn_mine, attn_other)
    unit_two, inv_two = unit_rows(resid)
    h_two = whole_rows((unit_two * gain_f).astype(BF))

    d_hidden = mm(grad_rows, full_down, 1, 1)
    gate, up = mm(h_two, full_gate, 1, 0), mm(h_two, full_up, 1, 0)
    gate_sigmoid = 1.0 / (1.0 + jnp.exp(-gate))
    gate_silu = gate * gate_sigmoid
    hidden = (gate_silu * up).astype(BF)
    slope = gate_sigmoid * (1.0 + gate * (1.0 - gate_sigmoid))
    d_gate = (d_hidden * up * slope).astype(BF)
    d_up = (d_hidden * gate_silu).astype(BF)

    def d_two_of(start):
        return mm(rows_of(d_gate, start), full_gate, 1, 1) + mm(rows_of(d_up, start), full_up, 1, 1)

    d_two = sum_tp(d_two_of(mine_row), d_two_of(other_row).astype(BF))
    down_mine, down_send = shares_of(lambda part: mm(hidden, part_of(grad_rows, part), 0, 0), 1)
    gate_mine, gate_send = shares_of(lambda part: mm(part_of(h_two, part), d_gate, 0, 0), 0)
    up_mine, up_send = shares_of(lambda part: mm(part_of(h_two, part), d_up, 0, 0), 0)
    arrived = [to_pair(send) for send in (down_send, gate_send, up_send)] if paired else []
    ffn_other = mm(rows_of(hidden, other_row), full_down, 1, 0).astype(BF)
    ffn_mine = mm(rows_of(hidden, mine_row), full_down, 1, 0)
    block_output = turn(whole_rows(resid + sum_tp(ffn_mine, ffn_other)))

    part_ffn_gain = jnp.sum(d_two * unit_two, axis=0)
    d_resid = rows_of(grad_rows, mine_row).astype(F32) + norm_back(unit_two, inv_two, gain_f, d_two)
    d_attn = whole_rows(d_resid.astype(BF))

    d_heads_t = mm(full_out, d_attn, 1, 1).astype(BF)
    d_q = None
    d_kv_parts = [None] * n_ctx
    for back in reversed(range(n_ctx)):
        d_q, d_kv = attend_back(
            back == 0, valids[back], q_t, kv_blocks[back], out_t, sums, d_heads_t, d_q
        )
        if back > 0:
            d_kv = over(d_kv, "ctx", [(i, i - back) for i in range(back, n_ctx)])
        d_kv_parts[back] = d_kv
    out_mine, out_send = shares_of(lambda part: mm(attn_t, part_of(d_attn, part), 1, 0), 1)
    d_raw_q_t, d_raw_kv_t, sum_q, sum_k = prep_back(
        raw_q_t, raw_kv_t, cos_t, sin_t, gain_q, gain_k, d_q, d_kv_parts
    )
    def joined(q, kv):
        pieces = []
        for g in range(groups):
            pieces += [q[:, g * split_at : (g + 1) * split_at]]
            pieces += [kv[:, g * 2 * HEAD_SIZE : (g + 1) * 2 * HEAD_SIZE]]
        return jnp.concatenate(pieces, axis=1)

    def qkv_grad(part):
        rows = part_of(h_one, part)
        return joined(mm(rows, d_raw_q_t, 0, 1), mm(rows, d_raw_kv_t, 0, 1))

    qkv_mine, qkv_send = shares_of(qkv_grad, 0)

    def d_one_of(start):
        return mm(cols_of(d_raw_kv_t, start), full_kv, 0, 1) + mm(
            cols_of(d_raw_q_t, start), full_q, 0, 1
        )

    d_one = sum_tp(d_one_of(mine_row), d_one_of(other_row).astype(BF))
    unit_half, inv_half = rows_of(unit_one, mine_row), rows_of(inv_one, mine_row)
    part_attn_gain = jnp.sum(d_one * unit_half, axis=0)
    input_grad = turn(whole_rows(d_resid + norm_back(unit_half, inv_half, gain_a, d_one)))

    share = 2.0 / n_tp
    gain_grads = sum_all(
        row_of([turn(part_attn_gain) * share, turn(part_ffn_gain) * share, sum_q[:, 0], sum_k[:, 0]])
    )

    mine = [down_mine, gate_mine, up_mine, out_mine, qkv_mine]
    if n_ctx == 4:
        down, gate_sum, up_sum, out_sum, qkv_sum = line_sums(
            mine, arrived, [out_send, qkv_send] if paired else []
        )
    else:
        theirs = arrived + [to_pair(send) for send in (out_send, qkv_send)] if paired else []
        if paired:
            mine = [left.astype(F32) + right.astype(F32) for left, right in zip(mine, theirs)]
        down, gate_sum, up_sum, out_sum, qkv_sum = (
            kept(lax.psum(part.astype(F32), "ctx").astype(BF)) for part in mine
        )
    grads = [qkv_sum, out_sum, gate_sum, up_sum, down]
    by_tp, by_fsdp = stats(grads)
    sums = [sum_over_tp(by_tp), sum_over_fsdp(by_fsdp)]
    squares = [squares_qkv, squares_out, squares_gate_up, squares_down]
    whole_grads, news, scales, scalars = scaled(
        (1.0 / n_tp, 1.0 / n_fsdp), grads, sums, olds, squares
    )
    totals = lax.psum(scalars, ("fsdp", "tp"))
    steps, new_vars, gain_steps, rms = finish(
        grads, scales, totals, gain_grads, gain_vars, gains_old
    )

    def gains_of(row):
        vector = row[0]
        ends = (0, D, 2 * D, 2 * D + HEAD_SIZE, 2 * D + 2 * HEAD_SIZE)
        return [vector[start:end] for start, end in zip(ends, ends[1:])]

    places = layout_of(grads)
    stat = lambda place: news[place[0]][0, place[1]]
    (row_qkv, col_qkv), (row_out, col_out), (row_gu, col_gate), (_, col_up), (row_down, col_down) = (
        (stat(row), stat(col)) for row, col in places
    )
    return (
        block_output[None],
        input_grad[None],
        *whole_grads,
        *gains_of(gain_grads),
        row_qkv,
        col_qkv,
        row_out,
        col_out,
        row_gu,
        jnp.stack([col_gate, col_up]),
        row_down,
        col_down,
        *gains_of(new_vars),
        *steps,
        *gains_of(gain_steps),
        rms[0, 0],
    )


def solution(mesh):
    tokens, vector = P("fsdp", "ctx", None), P()
    by_f, by_t = P("fsdp"), P("tp")
    w_specs = (P("fsdp", "tp"), P("tp", "fsdp"), P("fsdp", None, "tp"), P("tp", "fsdp"))
    stats = (by_f, by_t, by_t, by_f, by_f, P(None, "tp"), by_t, by_f) + (vector,) * 4
    return jax.shard_map(
        functools.partial(on_device, dict(mesh.shape)),
        mesh=mesh,
        in_specs=(tokens, tokens, by_f, P("fsdp", "ctx")) + w_specs + (vector,) * 4 + stats,
        out_specs=(tokens, tokens)
        + w_specs
        + (vector,) * 4
        + stats
        + w_specs
        + (vector,) * 4
        + (vector,),
        check_vma=False,
    )
```

```python
import functools
import math

import jax
import jax.numpy as jnp
from jax import lax
from jax.experimental import pallas as pl
from jax.experimental.pallas import tpu as pltpu
from jax.sharding import PartitionSpec as P


D = 1024
QUERY_HEADS = 16
KEY_VALUE_HEADS = 8
HEAD_SIZE = 64
FF = 4608
QKV = 2048

EPS = 1e-05
THETA = 1000000.0
DECAY = 0.5
CLIP = 0.15
RATE = 1.0

BF = jnp.bfloat16
F32 = jnp.float32
GROUP = QUERY_HEADS // KEY_VALUE_HEADS
LANES = (GROUP + 2) * HEAD_SIZE
KEY_TILE = 256
PAIR_BLOCKS = 4
LAG = 2
WINDOW = 3
GAIN_SHARE = 0.5


def mm(left, right, left_dim, right_dim):
    return lax.dot_general(
        left, right, (((left_dim,), (right_dim,)), ((), ())), preferred_element_type=F32
    )


def params(vmem=48 << 20):
    return pltpu.CompilerParams(vmem_limit_bytes=vmem)


def squares_into(sum_ref, values):
    rows, cols = values.shape
    sum_ref[...] += jnp.sum((values * values).reshape(rows // 8, 8, cols), axis=0)


def cast_kernel(spans, w_ref, *refs):
    sum_ref = refs[-1]

    @pl.when(pl.program_id(0) == 0)
    def _():
        sum_ref[...] = jnp.zeros_like(sum_ref)

    values = w_ref[...]
    for out_ref, pieces in zip(refs, spans):
        at = 0
        for start, size in pieces:
            out_ref[:, at : at + size] = values[:, start : start + size].astype(BF)
            at += size
    squares_into(sum_ref, values)


def cast(weight, spans=None):
    rows, cols = weight.shape
    spans = spans or [[(0, cols)]]
    widths = [sum(size for _, size in pieces) for pieces in spans]
    block = min(rows, 128)
    return pl.pallas_call(
        functools.partial(cast_kernel, spans),
        grid=(rows // block,),
        in_specs=[pl.BlockSpec((block, cols), lambda i: (i, 0))],
        out_specs=[pl.BlockSpec((block, width), lambda i: (i, 0)) for width in widths]
        + [pl.BlockSpec((8, cols), lambda i: (0, 0))],
        out_shape=[jax.ShapeDtypeStruct((rows, width), BF) for width in widths]
        + [jax.ShapeDtypeStruct((8, cols), F32)],
        cost_estimate=pl.CostEstimate(
            flops=3 * rows * cols, bytes_accessed=6 * rows * cols, transcendentals=0
        ),
        compiler_params=params(),
        name="cast",
    )(weight)


def cast_pair_kernel(w_ref, gate_ref, up_ref, sum_ref, held, sems):
    rows = w_ref.shape[0]
    block = rows // PAIR_BLOCKS
    copies = []
    for step in range(PAIR_BLOCKS):
        for which in range(2):
            span = pl.ds(step * block, block)
            copies.append(
                pltpu.make_async_copy(
                    w_ref.at[span, which, :], held.at[which, span, :], sems.at[which, step]
                )
            )
            copies[-1].start()
    sum_ref[...] = jnp.zeros_like(sum_ref)
    for step in range(PAIR_BLOCKS):
        for which, out_ref in enumerate((gate_ref, up_ref)):
            copies[2 * step + which].wait()

            @pl.loop(0, block // 16)
            def _(piece):
                at = pl.multiple_of(step * block + piece * 16, 16)
                values = held[which, pl.ds(at, 16), :]
                out_ref[pl.ds(at, 16), :] = values.astype(BF)
                squares_into(sum_ref, values)


def cast_pair(weight):
    rows, _, cols = weight.shape
    vmem = pl.BlockSpec(memory_space=pltpu.VMEM)
    return pl.pallas_call(
        cast_pair_kernel,
        in_specs=[pl.BlockSpec(memory_space=pl.ANY)],
        out_specs=[vmem] * 3,
        out_shape=[jax.ShapeDtypeStruct((rows, cols), BF)] * 2
        + [jax.ShapeDtypeStruct((8, cols), F32)],
        scratch_shapes=[
            pltpu.VMEM((2, rows, cols), F32),
            pltpu.SemaphoreType.DMA((2, PAIR_BLOCKS)),
        ],
        cost_estimate=pl.CostEstimate(
            flops=6 * rows * cols, bytes_accessed=12 * rows * cols, transcendentals=0
        ),
        compiler_params=params(),
        name="cast_pair",
    )(weight)


def lane_total(values):
    lanes = min(128, values.shape[1])
    total = values[:, :lanes]
    for at in range(lanes, values.shape[1], lanes):
        total = total + values[:, at : at + lanes]
    return total


def padded(size):
    return -(-size // 128) * 128


def spans_of(sizes):
    out, at = [], 0
    for size in sizes:
        out.append(slice(at, at + size))
        at += padded(size)
    return out


def layout_of(grads):
    qkv, out, gate, up, down = (g.shape for g in grads)
    tp_spans = spans_of([qkv[0], gate[0], out[1], down[1]])
    fsdp_spans = spans_of([qkv[1], gate[1], up[1], out[0], down[0]])
    return (
        ((0, tp_spans[0]), (1, fsdp_spans[0])),
        ((1, fsdp_spans[3]), (0, tp_spans[2])),
        ((0, tp_spans[1]), (1, fsdp_spans[1])),
        ((0, tp_spans[1]), (1, fsdp_spans[2])),
        ((1, fsdp_spans[4]), (0, tp_spans[3])),
    )


def packed_sizes(grads):
    qkv, out, gate, up, down = (g.shape for g in grads)
    return (
        sum(map(padded, (qkv[0], gate[0], out[1], down[1]))),
        sum(map(padded, (qkv[1], gate[1], up[1], out[0], down[0]))),
    )


def over_blocks(n_rows, block, body, init=None):
    if n_rows == block:
        return body(0, init)
    aligned = lambda step, carry: body(pl.multiple_of(step * block, block), carry)
    return lax.fori_loop(0, n_rows // block, aligned, init)


def stats_kernel(*refs):
    grads, packed = refs[:5], refs[5:]
    for ref in packed:
        ref[...] = jnp.zeros_like(ref)
    for grad_ref, places in zip(grads, layout_of(grads)):
        n_rows = grad_ref.shape[0]
        block = min(n_rows, 128)
        (row_at, row_span), (col_at, col_span) = places
        row_ref, col_ref = packed[row_at], packed[col_at]

        def add_block(at, carry):
            values = grad_ref[pl.ds(at, block), :].astype(F32)
            square = values * values
            col_ref[:, col_span] += jnp.sum(square, axis=0, keepdims=True)
            folded = jnp.sum(lane_total(square).T, axis=0, keepdims=True)
            start = row_span.start + at
            place = pl.ds(start if n_rows == block else pl.multiple_of(start, block), block)
            row_ref[:, place] += folded
            return carry

        over_blocks(n_rows, block, add_block, 0)


def stats(grads):
    vmem = pl.BlockSpec(memory_space=pltpu.VMEM)
    return pl.pallas_call(
        stats_kernel,
        in_specs=[vmem] * 5,
        out_specs=[vmem] * 2,
        out_shape=[jax.ShapeDtypeStruct((1, size), F32) for size in packed_sizes(grads)],
        cost_estimate=pl.CostEstimate(
            flops=4 * sum(g.size for g in grads),
            bytes_accessed=2 * sum(g.size for g in grads),
            transcendentals=0,
        ),
        compiler_params=params(),
        name="stats",
    )(*grads)


def columns_of(row, width):
    return jnp.broadcast_to(row, (min(128, width), row.shape[1])).T


def total_of(values):
    return jnp.sum(jnp.sum(values, axis=0, keepdims=True), axis=1, keepdims=True)


def out_views(outs):
    qkv, out, gate_up, down = outs
    return (
        lambda span: qkv.at[span, :],
        lambda span: out.at[span, :],
        lambda span: gate_up.at[span, 0, :],
        lambda span: gate_up.at[span, 1, :],
        lambda span: down.at[span, :],
    )


def tiles_in(grads):
    for index, grad_ref in enumerate(grads):
        block = min(grad_ref.shape[0], 128)
        for at in range(0, grad_ref.shape[0], block):
            yield index, at, block


def write_shapes(grads):
    qkv, out, gate, _, down = (g.shape for g in grads)
    return [
        jax.ShapeDtypeStruct(shape, F32) for shape in (qkv, out, (gate[0], 2, gate[1]), down)
    ]


def write_scratch(grads):
    count = len(list(tiles_in(grads)))
    return [pltpu.VMEM(g.shape, F32) for g in grads] + [pltpu.SemaphoreType.DMA((count,))]


COUNTS = ((QKV, D), (D, D), (2 * FF, D), (2 * FF, D), (D, FF))


def new_statistics(places, sums, olds, news, scales):
    for (row_place, col_place), count in zip(places, COUNTS):
        for (at, span), size in zip((row_place, col_place), count):
            new = DECAY * olds[at][:, span] + (1.0 - DECAY) * (sums[at][:, span] / size)
            news[at][:, span] = new
            scales[at][:, span] = lax.rsqrt(new)


def scalars_into(scalar_ref, shares, places, held, sums, olds, squares, scales):
    parts = []
    for (row_place, col_place), grad_ref in zip(places, held):
        n_rows, n_cols = grad_ref.shape
        block = min(n_rows, 128)
        lanes = min(128, n_cols)
        left_ref, row_start = scales[row_place[0]], row_place[1].start
        right = scales[col_place[0]][:, col_place[1]]

        def step_of(at, total):
            values = grad_ref[pl.ds(at, block), :].astype(F32) * right
            start = row_start + at
            place = pl.ds(start if n_rows == block else pl.multiple_of(start, block), block)
            left = columns_of(left_ref[:, place], n_cols)
            folded = lane_total(values * values) * (left * left)
            return total + jnp.sum(folded.reshape(block // 8, 8, lanes), axis=0)

        total = over_blocks(n_rows, block, step_of, jnp.zeros((8, lanes), F32))
        parts.append(total_of(total))
    scalars = [parts[0], parts[1], parts[2] + parts[3], parts[4]]
    row_places = [places[index][0] for index in (0, 1, 2, 4)]
    scalars += [total_of(sums[at][:, span]) * shares[at] for at, span in row_places]
    scalars += [total_of(ref[...]) for ref in squares]
    scalars += [total_of(olds[at][:, span]) * shares[at] for at, span in row_places]
    lane = lax.broadcasted_iota(jnp.int32, (8, 128), 1)
    packed = jnp.zeros((8, 128), F32)
    for number, value in enumerate(scalars):
        packed = jnp.where(lane == number, value, packed)
    scalar_ref[...] = packed


def scaled_kernel(shares, *refs):
    grads, sums, olds, squares = refs[:5], refs[5:7], refs[7:9], refs[9:13]
    outs, news, scale_refs, scalar_ref = refs[13:17], refs[17:19], refs[19:21], refs[21]
    held, sems = refs[22:27], refs[27]
    copies = []
    views = out_views(outs)
    for number, (index, at, block) in enumerate(tiles_in(grads)):
        span = pl.ds(at, block)
        held[index][span, :] = grads[index][span, :].astype(F32)
        copies.append(
            pltpu.make_async_copy(held[index].at[span, :], views[index](span), sems.at[number])
        )
        copies[-1].start()
    places = layout_of(grads)
    new_statistics(places, sums, olds, news, scale_refs)
    scalars_into(scalar_ref, shares, places, held, sums, olds, squares, scale_refs)
    for copy in copies:
        copy.wait()


def scaled(shares, grads, sums, olds, squares):
    vmem, hbm = pl.BlockSpec(memory_space=pltpu.VMEM), pl.BlockSpec(memory_space=pl.ANY)
    vectors = [jax.ShapeDtypeStruct((1, size), F32) for size in packed_sizes(grads)]
    out = pl.pallas_call(
        functools.partial(scaled_kernel, shares),
        in_specs=[vmem] * 13,
        out_specs=[hbm] * 4 + [vmem] * 5,
        out_shape=write_shapes(grads) + vectors * 2 + [jax.ShapeDtypeStruct((8, 128), F32)],
        scratch_shapes=write_scratch(grads),
        cost_estimate=pl.CostEstimate(
            flops=6 * sum(g.size for g in grads),
            bytes_accessed=6 * sum(g.size for g in grads),
            transcendentals=0,
        ),
        compiler_params=params(),
        name="scaled",
    )(*grads, *sums, *olds, *squares)
    return out[:4], out[4:6], out[6:8], out[8]


SIZES = ((D, QKV), (D, D), (D, 2 * FF), (FF, D))


def gain_parts(total_ref, gain_grad_ref, var_ref, gain_ref, new_var_ref, gain_step_ref, rms_ref):
    value = lambda number: total_ref[0:1, number : number + 1]
    means = [
        DECAY * value(12 + index) / rows + (1.0 - DECAY) * value(4 + index) / (rows * cols)
        for index, (rows, cols) in enumerate(SIZES)
    ]
    gain_grad = gain_grad_ref[...]
    new_var = DECAY * var_ref[...] + (1.0 - DECAY) * gain_grad * gain_grad
    new_var_ref[...] = new_var
    raw_gain = gain_grad * lax.rsqrt(new_var)
    total = jnp.sum(raw_gain * raw_gain, axis=1, keepdims=True)
    for index, mean in enumerate(means):
        total = total + value(index) * mean
    count = D * QKV + D * D + 2 * D * FF + FF * D + 2 * D + 2 * HEAD_SIZE
    rms = jnp.sqrt(total / count)
    rms_ref[...] = jnp.broadcast_to(rms, rms_ref.shape)
    clip = jnp.maximum(1.0, rms / CLIP)
    for start, size in ((0, D), (D, D)):
        span = slice(start, start + size)
        gain = gain_ref[:, span]
        scale = -RATE * jnp.sqrt(jnp.sum(gain * gain, axis=1, keepdims=True) / size) / clip
        gain_step_ref[:, span] = raw_gain[:, span] * scale
    span = slice(2 * D, 2 * D + 2 * HEAD_SIZE)
    gain = gain_ref[:, span]
    low = lax.broadcasted_iota(jnp.int32, gain.shape, 1) < HEAD_SIZE
    square = gain * gain
    low_sum = jnp.sum(jnp.where(low, square, 0.0), axis=1, keepdims=True)
    high_sum = jnp.sum(jnp.where(low, 0.0, square), axis=1, keepdims=True)
    scale = -RATE * jnp.sqrt(jnp.where(low, low_sum, high_sum) / HEAD_SIZE) / clip
    gain_step_ref[:, span] = raw_gain[:, span] * scale
    return [
        -RATE * jnp.sqrt(value(8 + index) / (rows * cols)) * jnp.sqrt(means[index]) / clip
        for index, (rows, cols) in enumerate(SIZES)
    ]


def write_steps(factors, places, grads, scales, held, views, sems, before=None):
    copies = []
    for number, (index, at, block) in enumerate(tiles_in(grads)):
        if before is not None and at == 0:
            before(index)
        span = pl.ds(at, block)
        (row_at, row_span), (col_at, col_span) = places[index]
        start = row_span.start + at
        n_cols = grads[index].shape[1]
        left = columns_of(scales[row_at][:, start : start + block], n_cols)
        right = scales[col_at][:, col_span] * factors[(0, 1, 2, 2, 3)[index]]
        for first in range(0, n_cols, left.shape[1]):
            lanes = slice(first, first + left.shape[1])
            tile = grads[index][span, lanes].astype(F32)
            held[index][span, lanes] = tile * left * right[:, lanes]
        copies.append(
            pltpu.make_async_copy(held[index].at[span, :], views[index](span), sems.at[number])
        )
        copies[-1].start()
    return copies


def finish_kernel(*refs):
    grads, scale_refs, total_ref = refs[:5], refs[5:7], refs[7]
    outs, held, sems = refs[11:15], refs[18:23], refs[23]
    factors = gain_parts(total_ref, *refs[8:11], *refs[15:18])
    copies = write_steps(
        factors, layout_of(grads), grads, scale_refs, held, out_views(outs), sems
    )
    for copy in copies:
        copy.wait()


def finish(grads, scales, totals, gain_grads, gain_vars, gains):
    vmem, hbm = pl.BlockSpec(memory_space=pltpu.VMEM), pl.BlockSpec(memory_space=pl.ANY)
    vector = jax.ShapeDtypeStruct(gains.shape, F32)
    out = pl.pallas_call(
        finish_kernel,
        in_specs=[vmem] * 11,
        out_specs=[hbm] * 4 + [vmem] * 3,
        out_shape=write_shapes(grads) + [vector, vector, jax.ShapeDtypeStruct((8, 128), F32)],
        scratch_shapes=write_scratch(grads),
        cost_estimate=pl.CostEstimate(
            flops=4 * sum(g.size for g in grads),
            bytes_accessed=6 * sum(g.size for g in grads),
            transcendentals=0,
        ),
        compiler_params=params(),
        name="finish",
    )(*grads, *scales, totals, gain_grads, gain_vars, gains)
    return out[:4], out[4], out[5], out[6]


def pieces_of(shapes):
    out = []
    for index, (rows, cols) in enumerate(shapes):
        size = rows
        while size % 32 == 0 and size * cols > 96 * 1024:
            size //= 2 if size % 64 == 0 else 3
        out += [(index, at, size) for at in range(0, rows, size)]
    return out


def line_kernel(shapes, arrived, pairs, *refs):
    count = len(shapes)
    refs = list(refs)
    take = lambda size: [refs.pop(0) for _ in range(size)]
    mine = take(count)
    theirs = take(arrived if pairs else 0)
    sends = take(count - arrived if pairs else 0)
    final = take(count)
    work, land, cross = take(count), take(count), take(count)
    theirs += take(count - arrived if pairs else 0)
    in_send, in_recv, mid_send, mid_recv, out_send, out_recv, x_send, x_recv = refs
    me = lax.axis_index("ctx")
    partner = me + 1 - 2 * (me % 2)
    opposite = 3 - me
    at_end = (me == 0) | (me == 3)
    lanes = [{"ctx": partner}, {"ctx": opposite}]
    if pairs:
        lanes.append({"fsdp": 1 - lax.axis_index("fsdp")})
    barrier = pltpu.get_barrier_semaphore()
    for lane in lanes:
        pl.semaphore_signal(barrier, inc=1, device_id=lane, device_id_type=pl.DeviceIdType.MESH)
    pl.semaphore_wait(barrier, len(lanes))

    def remote(source, target, send, recv, number, lane):
        index, at, size = pieces[number]
        span = pl.ds(at, size)
        return pltpu.make_async_remote_copy(
            src_ref=source[index].at[span, :],
            dst_ref=target[index].at[span, :],
            send_sem=send.at[number],
            recv_sem=recv.at[number],
            device_id=lanes[lane],
            device_id_type=pl.DeviceIdType.MESH,
        )

    pieces = pieces_of(shapes)
    numbers = range(len(pieces))
    inwards = [remote(work, land, in_send, in_recv, i, 0) for i in numbers]
    across = [remote(work, cross, mid_send, mid_recv, i, 1) for i in numbers]
    outwards = [remote(final, final, out_send, out_recv, i, 0) for i in numbers]
    exchanged = {}
    if pairs:
        padded_sends = [None] * arrived + sends
        for i in numbers:
            if pieces[i][0] >= arrived:
                exchanged[i] = remote(padded_sends, theirs, x_send, x_recv, i, 2)
                exchanged[i].start()

    def add(target, number, *sources):
        index, at, size = pieces[number]
        step = 32 if size % 32 == 0 else 16

        @pl.loop(0, size // step)
        def _(piece):
            span = pl.ds(pl.multiple_of(at + piece * step, 16), step)
            total = sources[0][index][span, :].astype(F32)
            for source in sources[1:]:
                total = total + source[index][span, :].astype(F32)
            target[index][span, :] = total.astype(BF)

    own = (mine, theirs) if pairs else (mine,)

    def ready(number):
        if number in exchanged:
            exchanged[number].wait_recv()

    @pl.when(at_end)
    def _():
        for i in numbers:
            ready(i)
            add(work, i, *own)
            inwards[i].start()
        for i in numbers:
            inwards[i].wait_send()
            outwards[i].wait_recv()

    @pl.when(jnp.logical_not(at_end))
    def _():
        lag = 2
        for i in range(len(pieces) + lag):
            if i < len(pieces):
                ready(i)
                inwards[i].wait_recv()
                add(work, i, *own, land)
                across[i].start()
            if i >= lag:
                across[i - lag].wait_recv()
                add(final, i - lag, work, cross)
                outwards[i - lag].start()
        for i in numbers:
            across[i].wait_send()
            outwards[i].wait_send()

    for copy in exchanged.values():
        copy.wait_send()


def line_sums(mine, theirs, sends):
    shapes = [m.shape for m in mine]
    pairs = bool(sends) or bool(theirs)
    count, arrived = len(mine), len(theirs)
    number = len(pieces_of(shapes))
    vmem = pl.BlockSpec(memory_space=pltpu.VMEM)
    held = [pltpu.VMEM(shape, BF) for shape in shapes]
    size = sum(m.size for m in mine)
    return pl.pallas_call(
        functools.partial(line_kernel, shapes, arrived, pairs),
        in_specs=[vmem] * (count + len(theirs) + len(sends)),
        out_specs=[vmem] * count,
        out_shape=[jax.ShapeDtypeStruct(shape, BF) for shape in shapes],
        scratch_shapes=held * 3
        + (held[arrived:] if pairs else [])
        + [pltpu.SemaphoreType.DMA((number,))] * 8,
        cost_estimate=pl.CostEstimate(flops=4 * size, bytes_accessed=80 * size, transcendentals=0),
        compiler_params=pltpu.CompilerParams(
            vmem_limit_bytes=56 << 20, collective_id=0, has_side_effects=True
        ),
        name="line_sums",
    )(*mine, *theirs, *sends)


def close_kernel(shapes, arrived, shares, *refs):
    count = len(shapes)
    refs = list(refs)
    take = lambda size: [refs.pop(0) for _ in range(size)]
    mine, theirs, sends = take(count), take(arrived), take(count - arrived)
    d_mine_ref, d_other_ref, d_resid_ref, x_ref, gain_a_ref, gain_row_ref = take(6)
    olds, squares = take(2), take(4)
    final, news, scales = take(count), take(2), take(2)
    gain_grad_ref, total_ref, grad_out_ref = take(3)
    work, land, cross = take(count), take(count), take(count)
    theirs += take(count - arrived)
    packed, sums = take(2), take(2)
    core_ref, low_ref, y_ref = take(3)
    rows, row_got, tp_mid, got_tp, got_fsdp = take(5), take(5), take(1)[0], take(2), take(1)[0]
    scalar_refs, scalar_got = take(3) + [total_ref], take(3)
    in_send, in_recv, mid_send, mid_recv, out_send, out_recv, x_send, x_recv = take(8)
    s_send, s_recv = take(2)

    me_f, me_z, me_t = (lax.axis_index(name) for name in ("fsdp", "ctx", "tp"))
    at_end = (me_z == 0) | (me_z == 3)
    lane = {
        "near": {"ctx": me_z + 1 - 2 * (me_z % 2)},
        "far": {"ctx": 3 - me_z},
        "x": {"fsdp": 1 - me_f},
        "core": {"tp": me_t + 1 - 2 * (me_t % 2)},
        "y": {"tp": (me_t + 2) % 4},
    }
    mesh_ids = pl.DeviceIdType.MESH
    barrier = pltpu.get_barrier_semaphore()
    for device in lane.values():
        pl.semaphore_signal(barrier, inc=1, device_id=device, device_id_type=mesh_ids)
    pl.semaphore_wait(barrier, len(lane))

    def remote(source, target, send, recv, name):
        return pltpu.make_async_remote_copy(
            src_ref=source,
            dst_ref=target,
            send_sem=send,
            recv_sem=recv,
            device_id=lane[name],
            device_id_type=mesh_ids,
        )

    pieces = pieces_of(shapes)
    numbers = range(len(pieces))

    def piece_copy(source, target, send, recv, name, number):
        index, at, size = pieces[number]
        span = pl.ds(at, size)
        return remote(
            source[index].at[span, :], target[index].at[span, :], send.at[number], recv.at[number], name
        )

    inwards = [piece_copy(work, land, in_send, in_recv, "near", i) for i in numbers]
    across = [piece_copy(work, cross, mid_send, mid_recv, "far", i) for i in numbers]
    outwards = [piece_copy(final, final, out_send, out_recv, "near", i) for i in numbers]
    late = [i for i in numbers if pieces[i][0] >= arrived]
    all_sends = [None] * arrived + sends
    exchanged = {i: piece_copy(all_sends, theirs, x_send, x_recv, "x", i) for i in late}
    small = []

    def message(source, target, name):
        number = len(small)
        small.append(remote(source, target, s_send.at[number], s_recv.at[number], name))
        small[-1].start()
        return small[-1]

    d_core = message(d_other_ref, core_ref, "core")
    for copy in exchanged.values():
        copy.start()
    for ref in packed:
        ref[...] = jnp.zeros_like(ref)

    def add(target, number, *sources):
        index, at, size = pieces[number]
        step = 32 if size % 32 == 0 else 16

        @pl.loop(0, size // step)
        def _(piece):
            span = pl.ds(pl.multiple_of(at + piece * step, 16), step)
            total = sources[0][index][span, :].astype(F32)
            for source in sources[1:]:
                total = total + source[index][span, :].astype(F32)
            target[index][span, :] = total.astype(BF)

    def ready(number):
        if number in exchanged:
            exchanged[number].wait_recv()

    def pass_on(i):
        @pl.when(at_end)
        def _():
            if 0 <= i - WINDOW < len(pieces):
                inwards[i - WINDOW].wait_send()
            if i < len(pieces):
                ready(i)
                add(work, i, mine, theirs)
                inwards[i].start()

        @pl.when(jnp.logical_not(at_end))
        def _():
            if i < len(pieces):
                ready(i)
                inwards[i].wait_recv()
                add(work, i, mine, theirs, land)
                across[i].start()
            if 0 <= i - LAG < len(pieces):
                across[i - LAG].wait_recv()
                add(final, i - LAG, work, cross)
                outwards[i - LAG].start()

    half = d_mine_ref.shape[0]
    block = 32
    state = {}

    def add_cores():
        d_core.wait_recv()

        @pl.loop(0, half // block)
        def _(step):
            span = pl.ds(pl.multiple_of(step * block, block), block)
            low_ref[span, :] = (d_mine_ref[span, :] + core_ref[span, :].astype(F32)).astype(BF)

        state["y"] = message(low_ref, y_ref, "y")

    def input_grads():
        state["y"].wait_recv()
        gain = gain_a_ref[...]
        my_rows = (me_t % 2) * half
        split = gain.shape[1] // 2

        def rows_step(step, total):
            span = pl.ds(pl.multiple_of(step * block, block), block)
            grad = low_ref[span, :].astype(F32) + y_ref[span, :].astype(F32)
            values = x_ref[span, :].astype(F32)
            inv = lax.rsqrt(jnp.mean(values * values, axis=-1, keepdims=True) + EPS)
            unit = values * inv
            shifted = grad * gain
            mean = jnp.mean(shifted * unit, axis=-1, keepdims=True)
            result = d_resid_ref[span, :] + (shifted - unit * mean) * inv
            place = pl.ds(pl.multiple_of(my_rows + step * block, block), block)

            @pl.when(me_f == 0)
            def _():
                grad_out_ref[place, :] = result

            @pl.when(me_f != 0)
            def _():
                grad_out_ref[place, :split] = result[:, split:]
                grad_out_ref[place, split:] = result[:, :split]

            return total + jnp.sum((grad * unit).reshape(block // 8, 8, 2 * split), axis=0)

        total = lax.fori_loop(0, half // block, rows_step, jnp.zeros((8, 2 * split), F32))
        total = jnp.sum(total, axis=0, keepdims=True) * GAIN_SHARE
        rows[0][...] = gain_row_ref[...]

        @pl.when(me_f == 0)
        def _():
            rows[0][:, : 2 * split] = total

        @pl.when(me_f != 0)
        def _():
            rows[0][:, :split] = total[:, split:]
            rows[0][:, split : 2 * split] = total[:, :split]

        mine_span = pl.ds(pl.multiple_of(my_rows, half), half)
        state["grad"] = message(grad_out_ref.at[mine_span, :], grad_out_ref.at[mine_span, :], "core")
        state["row"] = message(rows[0], row_got[0], "core")

    def add_row(step):
        def run():
            state["row"].wait_recv()
            total = rows[step][...] + row_got[step][...]
            if step < 4:
                rows[step + 1][...] = total
                name = ("y", "x", "near", "far")[step]
                state["row"] = message(rows[step + 1], row_got[step + 1], name)
            else:
                gain_grad_ref[...] = total

        return run

    order = (4, 2, 3, 1, 0)
    travel = [order.index(index) for index in range(count)]
    by_order = lambda values: [values[index] for index in travel]
    places = layout_of(by_order(final))

    def settle(index):
        def run():
            grad_ref = final[index]
            n_rows = grad_ref.shape[0]
            (row_at, row_span), (col_at, col_span) = places[order[index]]

            @pl.when(at_end)
            def _():
                for i in numbers:
                    if pieces[i][0] == index:
                        outwards[i].wait_recv()

            @pl.loop(0, n_rows // 128)
            def _(step):
                at = pl.multiple_of(step * 128, 128)
                values = grad_ref[pl.ds(at, 128), :].astype(F32)
                square = values * values
                packed[col_at][:, col_span] += jnp.sum(square, axis=0, keepdims=True)
                folded = jnp.sum(lane_total(square).T, axis=0, keepdims=True)
                place = pl.ds(pl.multiple_of(row_span.start + at, 128), 128)
                packed[row_at][:, place] += folded

        return run

    last = {index: max(i for i in numbers if pieces[i][0] == index) for index in range(count)}
    events = {2: [add_cores], 8: [input_grads]}
    for step in range(5):
        events.setdefault(10 + 2 * step, []).append(add_row(step))
    for index in range(arrived):
        events.setdefault(last[index] + LAG + 3, []).append(settle(index))
    for i in range(len(pieces) + max(LAG, WINDOW)):
        for run in events.pop(i, []):
            run()
        pass_on(i)
    for i in sorted(events):
        for run in events[i]:
            run()
    for index in range(arrived, count):
        settle(index)()

    over_core = message(packed[0], got_tp[0], "core")
    over_x = message(packed[1], got_fsdp, "x")
    over_core.wait_recv()
    tp_mid[...] = packed[0][...] + got_tp[0][...]
    over_y = message(tp_mid, got_tp[1], "y")
    over_x.wait_recv()
    sums[1][...] = packed[1][...] + got_fsdp[...]
    over_y.wait_recv()
    sums[0][...] = tp_mid[...] + got_tp[1][...]
    new_statistics(places, sums, olds, news, scales)
    scalars_into(scalar_refs[0], shares, places, by_order(final), sums, olds, squares, scales)
    for step, name in enumerate(("core", "y", "x")):
        copy = message(scalar_refs[step], scalar_got[step], name)
        copy.wait_recv()
        scalar_refs[step + 1][...] = scalar_refs[step][...] + scalar_got[step][...]
    state["grad"].wait_recv()
    for copy in small:
        copy.wait_send()
    for copy in exchanged.values():
        copy.wait_send()

    @pl.when(jnp.logical_not(at_end))
    def _():
        for i in numbers:
            across[i].wait_send()
            outwards[i].wait_send()


def close(mine, theirs, sends, others, shares):
    shapes = [m.shape for m in mine]
    count, arrived = len(mine), len(theirs)
    number = len(pieces_of(shapes))
    by_order = [mine[index] for index in (4, 3, 1, 2, 0)]
    d_mine = others[0]
    half, width = d_mine.shape
    row = others[5].shape
    vectors = [(1, size) for size in packed_sizes(by_order)]
    vmem, hbm = pl.BlockSpec(memory_space=pltpu.VMEM), pl.BlockSpec(memory_space=pl.ANY)
    held = [pltpu.VMEM(shape, BF) for shape in shapes]
    f32 = lambda shape: pltpu.VMEM(shape, F32)
    rows = [f32(row)] * 5
    size = sum(m.size for m in mine)
    out_shape = (
        [jax.ShapeDtypeStruct(shape, BF) for shape in shapes]
        + [jax.ShapeDtypeStruct(shape, F32) for shape in vectors * 2]
        + [jax.ShapeDtypeStruct(row, F32), jax.ShapeDtypeStruct((8, 128), F32)]
        + [jax.ShapeDtypeStruct((2 * half, width), F32)]
    )
    out = pl.pallas_call(
        functools.partial(close_kernel, shapes, arrived, shares),
        in_specs=[vmem] * (count + arrived + len(sends) + len(others)),
        out_specs=[vmem] * len(out_shape),
        out_shape=out_shape,
        scratch_shapes=held * 3
        + held[arrived:]
        + [f32(shape) for shape in vectors * 2]
        + [pltpu.VMEM((half, width), BF)] * 3
        + rows * 2
        + [f32(vectors[0])] * 3
        + [f32(vectors[1])]
        + [f32((8, 128))] * 6
        + [pltpu.SemaphoreType.DMA((number,))] * 8
        + [pltpu.SemaphoreType.DMA((16,))] * 2,
        cost_estimate=pl.CostEstimate(flops=4 * size, bytes_accessed=80 * size, transcendentals=0),
        compiler_params=pltpu.CompilerParams(
            vmem_limit_bytes=56 << 20, collective_id=0, has_side_effects=True
        ),
        name="close",
    )(*mine, *theirs, *sends, *others)
    grads = [out[index] for index in (4, 3, 1, 2, 0)]
    return grads, out[5:7], out[7:9], out[9], out[10], out[11]


GAIN_SPANS = ((0, D), (D, D), (2 * D, HEAD_SIZE), (2 * D + HEAD_SIZE, HEAD_SIZE))


def write_kernel(*refs):
    refs = list(refs)
    take = lambda size: [refs.pop(0) for _ in range(size)]
    grads, news, scales = take(5), take(2), take(2)
    gain_grad_ref, total_ref, input_grad_ref, var_ref, gain_ref = take(5)
    whole_outs, step_outs, grad_out = take(4), take(4), take(1)[0]
    stat_outs, gain_outs, rms_ref = take(9), take(12), take(1)[0]
    whole_held, step_held = take(5), take(5)
    new_var_ref, gain_step_ref, whole_sems, step_sems, grad_sem = take(5)
    moved = pltpu.make_async_copy(input_grad_ref, grad_out, grad_sem)
    moved.start()
    places, views = layout_of(grads), out_views(whole_outs)
    factors = gain_parts(
        total_ref, gain_grad_ref, var_ref, gain_ref, new_var_ref, gain_step_ref, rms_ref
    )
    copies = []
    for number, (index, at, block) in enumerate(tiles_in(grads)):
        span = pl.ds(at, block)
        whole_held[index][span, :] = grads[index][span, :].astype(F32)
        copies.append(
            pltpu.make_async_copy(
                whole_held[index].at[span, :], views[index](span), whole_sems.at[number]
            )
        )
        copies[-1].start()
    copies += write_steps(
        factors, places, grads, scales, step_held, out_views(step_outs), step_sems
    )
    spots = [place for pair in places for place in pair]
    del spots[6]
    for out_ref, (at, span) in zip(stat_outs, spots):
        out_ref[...] = news[at][:, span]
    for source, outs in zip(
        (gain_grad_ref, new_var_ref, gain_step_ref), (gain_outs[:4], gain_outs[4:8], gain_outs[8:])
    ):
        for out_ref, (start, size) in zip(outs, GAIN_SPANS):
            out_ref[...] = source[:, start : start + size]
    for copy in copies:
        copy.wait()
    moved.wait()


def write_all(grads, news, scales, gain_grads, totals, input_grad, gain_vars, gains):
    vmem, hbm = pl.BlockSpec(memory_space=pltpu.VMEM), pl.BlockSpec(memory_space=pl.ANY)
    spots = [place for pair in layout_of(grads) for place in pair]
    del spots[6]
    writes = write_shapes(grads)
    row = lambda size: jax.ShapeDtypeStruct((1, size), F32)
    out_shape = (
        writes * 2
        + [jax.ShapeDtypeStruct(input_grad.shape, F32)]
        + [row(span.stop - span.start) for _, span in spots]
        + [row(size) for _, size in GAIN_SPANS] * 3
        + [jax.ShapeDtypeStruct((8, 128), F32)]
    )
    tiles = len(list(tiles_in(grads)))
    held = [pltpu.VMEM(g.shape, F32) for g in grads]
    size = sum(g.size for g in grads)
    out = pl.pallas_call(
        write_kernel,
        in_specs=[vmem] * 14,
        out_specs=[hbm] * 9 + [vmem] * (len(out_shape) - 9),
        out_shape=out_shape,
        scratch_shapes=held * 2
        + [pltpu.VMEM(gains.shape, F32)] * 2
        + [pltpu.SemaphoreType.DMA((tiles,))] * 2
        + [pltpu.SemaphoreType.DMA(())],
        cost_estimate=pl.CostEstimate(
            flops=4 * size, bytes_accessed=10 * size, transcendentals=0
        ),
        compiler_params=params(),
        name="write_all",
    )(*grads, *news, *scales, gain_grads, totals, input_grad, gain_vars, gains)
    return out[:4], out[4:8], out[8], out[9:18], out[18:30], out[30]


def turned_head(rows, gain, cos_t, sin_t):
    half = HEAD_SIZE // 2
    inv = lax.rsqrt(jnp.mean(rows * rows, axis=0, keepdims=True) + EPS)
    normed = rows * inv * gain
    low, high = normed[:half], normed[half:]
    return jnp.concatenate([low * cos_t - high * sin_t, high * cos_t + low * sin_t], axis=0)


def queries_kernel(raw_ref, cos_ref, sin_ref, gain_ref, q_ref):
    turned = turned_head(raw_ref[...], gain_ref[...], cos_ref[...], sin_ref[...])
    scale = 1.0 / math.sqrt(HEAD_SIZE)
    q_ref[...] = (turned.astype(BF).astype(F32) * scale).astype(BF)


def keys_kernel(raw_ref, cos_ref, sin_ref, gain_ref, kv_ref):
    turned = turned_head(raw_ref[:HEAD_SIZE, :], gain_ref[...], cos_ref[...], sin_ref[...])
    kv_ref[:HEAD_SIZE, :] = turned.astype(BF)
    kv_ref[HEAD_SIZE:, :] = raw_ref[HEAD_SIZE:, :].astype(BF)


def prep_call(kernel, size, raw_t, cos_t, sin_t, gain):
    rows, tokens = raw_t.shape
    half = HEAD_SIZE // 2
    fixed = lambda g: (0, 0)
    return pl.pallas_call(
        kernel,
        grid=(rows // size,),
        in_specs=[
            pl.BlockSpec((size, tokens), lambda g: (g, 0)),
            pl.BlockSpec((half, tokens), fixed),
            pl.BlockSpec((half, tokens), fixed),
            pl.BlockSpec((HEAD_SIZE, 1), fixed),
        ],
        out_specs=pl.BlockSpec((size, tokens), lambda g: (g, 0)),
        out_shape=jax.ShapeDtypeStruct(raw_t.shape, BF),
        cost_estimate=pl.CostEstimate(
            flops=20 * rows * tokens, bytes_accessed=6 * rows * tokens, transcendentals=0
        ),
        compiler_params=params(),
        name="prep",
    )(raw_t, cos_t, sin_t, gain)


prep_queries = functools.partial(prep_call, queries_kernel, HEAD_SIZE)
prep_keys = functools.partial(prep_call, keys_kernel, 2 * HEAD_SIZE)


def prep_back_kernel(parts, *refs):
    raw_q_ref, raw_kv_ref, cos_ref, sin_ref, gq_ref, gk_ref, dq_ref = refs[:7]
    dkv_refs = refs[7 : 7 + parts]
    out_q_ref, out_kv_ref, sum_q_ref, sum_k_ref = refs[7 + parts :]
    half = HEAD_SIZE // 2
    cos_t, sin_t = cos_ref[...], sin_ref[...]
    d_kv = dkv_refs[0][...]
    for ref in dkv_refs[1:]:
        d_kv = d_kv + ref[...].astype(F32)

    @pl.when(pl.program_id(0) == 0)
    def _():
        sum_q_ref[...] = jnp.zeros_like(sum_q_ref)
        sum_k_ref[...] = jnp.zeros_like(sum_k_ref)

    for piece in range(GROUP + 1):
        base = piece * HEAD_SIZE
        if piece < GROUP:
            rows = raw_q_ref[base : base + HEAD_SIZE, :]
            grad = dq_ref[base : base + HEAD_SIZE, :] * (1.0 / math.sqrt(HEAD_SIZE))
            gain, sum_ref = gq_ref[...], sum_q_ref
        else:
            rows = raw_kv_ref[:HEAD_SIZE, :]
            grad = d_kv[:HEAD_SIZE]
            gain, sum_ref = gk_ref[...], sum_k_ref
        inv = lax.rsqrt(jnp.mean(rows * rows, axis=0, keepdims=True) + EPS)
        unit = rows * inv
        low, high = grad[:half], grad[half:]
        turned = jnp.concatenate([low * cos_t + high * sin_t, high * cos_t - low * sin_t], axis=0)
        sum_ref[...] += jnp.sum(turned * unit, axis=1, keepdims=True)
        scaled = turned * gain
        mean = jnp.mean(scaled * unit, axis=0, keepdims=True)
        result = ((scaled - unit * mean) * inv).astype(BF)
        if piece < GROUP:
            out_q_ref[base : base + HEAD_SIZE, :] = result
        else:
            out_kv_ref[:HEAD_SIZE, :] = result
    out_kv_ref[HEAD_SIZE:, :] = d_kv[HEAD_SIZE:].astype(BF)


def prep_back(raw_q_t, raw_kv_t, cos_t, sin_t, gain_q, gain_k, d_q, d_kv_parts):
    tokens = raw_q_t.shape[1]
    groups = raw_kv_t.shape[0] // (2 * HEAD_SIZE)
    rows = raw_q_t.shape[0] + raw_kv_t.shape[0]
    half = HEAD_SIZE // 2
    fixed = lambda g: (0, 0)
    block = lambda size: pl.BlockSpec((size, tokens), lambda g: (g, 0))
    return pl.pallas_call(
        functools.partial(prep_back_kernel, len(d_kv_parts)),
        grid=(groups,),
        in_specs=[
            block(GROUP * HEAD_SIZE),
            block(2 * HEAD_SIZE),
            pl.BlockSpec((half, tokens), fixed),
            pl.BlockSpec((half, tokens), fixed),
            pl.BlockSpec((HEAD_SIZE, 1), fixed),
            pl.BlockSpec((HEAD_SIZE, 1), fixed),
            block(GROUP * HEAD_SIZE),
        ]
        + [block(2 * HEAD_SIZE)] * len(d_kv_parts),
        out_specs=[
            block(GROUP * HEAD_SIZE),
            block(2 * HEAD_SIZE),
            pl.BlockSpec((HEAD_SIZE, 128), fixed),
            pl.BlockSpec((HEAD_SIZE, 128), fixed),
        ],
        out_shape=[
            jax.ShapeDtypeStruct(raw_q_t.shape, BF),
            jax.ShapeDtypeStruct(raw_kv_t.shape, BF),
            jax.ShapeDtypeStruct((HEAD_SIZE, 128), F32),
            jax.ShapeDtypeStruct((HEAD_SIZE, 128), F32),
        ],
        cost_estimate=pl.CostEstimate(
            flops=30 * rows * tokens, bytes_accessed=9 * rows * tokens, transcendentals=0
        ),
        compiler_params=params(),
        name="prep_back",
    )(raw_q_t, raw_kv_t, cos_t, sin_t, gain_q, gain_k, d_q, *d_kv_parts)


def tiles_of(diagonal, tokens):
    for key_start in range(0, tokens, KEY_TILE):
        yield key_start, key_start if diagonal else 0


def tile_probs(kv_ref, query, key_start, query_start, valid, diagonal):
    keys = kv_ref[:HEAD_SIZE, key_start : key_start + KEY_TILE]
    scores = mm(keys, query, 0, 0)
    key_index = key_start + lax.broadcasted_iota(jnp.int32, scores.shape, 0)
    visible = key_index < valid
    if diagonal:
        query_index = query_start + lax.broadcasted_iota(jnp.int32, scores.shape, 1)
        visible = visible & (key_index <= query_index)
    return keys, visible, jnp.exp(scores)


def attend_kernel(diagonal, valid_ref, q_ref, kv_ref, *refs):
    if diagonal:
        acc_ref, sum_ref = refs
        acc_ref[...] = jnp.zeros_like(acc_ref)
        sum_ref[...] = jnp.zeros_like(sum_ref)
    else:
        acc_in_ref, sum_in_ref, acc_ref, sum_ref = refs
        acc_ref[...] = acc_in_ref[...]
        sum_ref[...] = sum_in_ref[...]
    valid = valid_ref[0]
    tokens = q_ref.shape[1]

    @pl.when(valid > 0)
    def _():
        for key_start, query_start in tiles_of(diagonal, tokens):
            query = q_ref[:, query_start:]
            _, visible, raised = tile_probs(kv_ref, query, key_start, query_start, valid, diagonal)
            probs = jnp.where(visible, raised, 0.0)
            sum_ref[:, query_start:] += jnp.sum(probs, axis=0, keepdims=True)
            values = kv_ref[HEAD_SIZE:, key_start : key_start + KEY_TILE]
            acc_ref[:, query_start:] += mm(values, probs.astype(BF), 1, 0)


def attend(diagonal, valid, q_t, kv_t, state):
    rows, tokens = q_t.shape
    heads = rows // HEAD_SIZE
    per_head = pl.BlockSpec((HEAD_SIZE, tokens), lambda h: (h, 0))
    sums = pl.BlockSpec((8, tokens), lambda h: (h, 0))
    carried = [] if diagonal else [per_head, sums]
    return pl.pallas_call(
        functools.partial(attend_kernel, diagonal),
        grid=(heads,),
        in_specs=[
            pl.BlockSpec(memory_space=pltpu.SMEM),
            per_head,
            pl.BlockSpec((2 * HEAD_SIZE, tokens), lambda h: (h // GROUP, 0)),
        ]
        + carried,
        out_specs=[per_head, sums],
        out_shape=[
            jax.ShapeDtypeStruct((rows, tokens), F32),
            jax.ShapeDtypeStruct((heads * 8, tokens), F32),
        ],
        input_output_aliases={} if diagonal else {3: 0, 4: 1},
        cost_estimate=pl.CostEstimate(
            flops=4 * rows * tokens * tokens,
            bytes_accessed=10 * rows * tokens,
            transcendentals=heads * tokens * tokens,
        ),
        compiler_params=params(),
        name="attend",
    )(valid, q_t, kv_t, *state)


def attend_back_kernel(diagonal, first, valid_ref, q_ref, kv_ref, out_ref, sum_ref, do_ref, *refs):
    if first:
        dq_ref, dkv_ref, dkv_acc = refs
        dq_ref[...] = jnp.zeros_like(dq_ref)
    else:
        dq_in_ref, dq_ref, dkv_ref, dkv_acc = refs
        dq_ref[...] = dq_in_ref[...]
    head = pl.program_id(0)
    valid = valid_ref[0]
    tokens = q_ref.shape[1]

    @pl.when(head % GROUP == 0)
    def _():
        dkv_acc[...] = jnp.zeros_like(dkv_acc)

    @pl.when(valid > 0)
    def _():
        inverse = 1.0 / sum_ref[0:1, :]
        delta = jnp.sum(do_ref[...].astype(F32) * out_ref[...], axis=0, keepdims=True)
        for key_start, query_start in tiles_of(diagonal, tokens):
            query = q_ref[:, query_start:]
            grads = do_ref[:, query_start:]
            keys, visible, raised = tile_probs(
                kv_ref, query, key_start, query_start, valid, diagonal
            )
            probs = jnp.where(visible, raised * inverse[:, query_start:], 0.0)
            span = slice(key_start, key_start + KEY_TILE)
            values = kv_ref[HEAD_SIZE:, span]
            d_probs = mm(values, grads, 0, 0)
            d_scores = (probs * (d_probs - delta[:, query_start:])).astype(BF)
            dq_ref[:, query_start:] += mm(keys, d_scores, 1, 0)
            dkv_acc[:HEAD_SIZE, span] += mm(query, d_scores, 1, 1)
            dkv_acc[HEAD_SIZE:, span] += mm(grads, probs.astype(BF), 1, 1)

    @pl.when(head % GROUP == GROUP - 1)
    def _():
        dkv_ref[...] = dkv_acc[...].astype(dkv_ref.dtype)


def attend_back(diagonal, valid, q_t, kv_t, out_t, sums, d_out_t, d_q):
    rows, tokens = q_t.shape
    heads = rows // HEAD_SIZE
    first = d_q is None
    per_head = pl.BlockSpec((HEAD_SIZE, tokens), lambda h: (h, 0))
    per_group = pl.BlockSpec((2 * HEAD_SIZE, tokens), lambda h: (h // GROUP, 0))
    return pl.pallas_call(
        functools.partial(attend_back_kernel, diagonal, first),
        grid=(heads,),
        in_specs=[
            pl.BlockSpec(memory_space=pltpu.SMEM),
            per_head,
            per_group,
            per_head,
            pl.BlockSpec((8, tokens), lambda h: (h, 0)),
            per_head,
        ]
        + ([] if first else [per_head]),
        out_specs=[per_head, per_group],
        out_shape=[
            jax.ShapeDtypeStruct((rows, tokens), F32),
            jax.ShapeDtypeStruct(kv_t.shape, F32 if diagonal else BF),
        ],
        scratch_shapes=[pltpu.VMEM((2 * HEAD_SIZE, tokens), F32)],
        input_output_aliases={} if first else {6: 0},
        cost_estimate=pl.CostEstimate(
            flops=10 * rows * tokens * tokens,
            bytes_accessed=14 * rows * tokens,
            transcendentals=heads * tokens * tokens,
        ),
        compiler_params=params(),
        name="attend_back",
    )(valid, q_t, kv_t, out_t, sums, d_out_t, *([] if first else [d_q]))


def unit_rows(values):
    inv = lax.rsqrt(jnp.mean(values * values, axis=-1, keepdims=True) + EPS)
    return values * inv, inv


def norm_back(unit, inv, gain, grad):
    scaled = grad * gain
    return (scaled - unit * jnp.mean(scaled * unit, axis=-1, keepdims=True)) * inv


def kept(value):
    return lax.optimization_barrier(value)


def on_device(
    sizes,
    block_input,
    cotangent,
    seq_lengths,
    positions,
    w_qkv,
    w_out,
    w_gate_up,
    w_down,
    gain_attn,
    gain_ffn,
    gain_query,
    gain_key,
    row_qkv_old,
    col_qkv_old,
    row_out_old,
    col_out_old,
    row_gate_up_old,
    col_gate_up_old,
    row_down_old,
    col_down_old,
    var_attn_old,
    var_ffn_old,
    var_query_old,
    var_key_old,
):
    n_fsdp, n_ctx, n_tp = sizes["fsdp"], sizes["ctx"], sizes["tp"]
    paired = n_fsdp == 2
    me_f, me_z, me_t = (lax.axis_index(name) for name in ("fsdp", "ctx", "tp"))
    tokens = block_input.shape[1]
    half = tokens // 2
    mine_row = (me_t % 2) * half
    other_row = half - mine_row

    def turn(values):
        if not paired:
            return values
        size = values.shape[-1] // 2
        swapped = jnp.concatenate([values[..., size:], values[..., :size]], axis=-1)
        return jnp.where(me_f == 0, values, swapped)

    def over(values, axis, pairs):
        return lax.ppermute(values, axis, pairs)

    def to_core(values):
        return over(values, "tp", [(i, i ^ 1) for i in range(n_tp)])

    def to_pair(values):
        return over(values, "fsdp", [(0, 1), (1, 0)])

    def gather_weight(shard, axis):
        if not paired:
            return lax.all_gather(shard, "fsdp", axis=axis, tiled=True)
        return jnp.concatenate([shard, to_pair(shard)], axis=axis)

    routed_by_ctx = paired and n_ctx % 2 == 0

    def first_half(shard):
        if not routed_by_ctx:
            return None
        size = shard.shape[0] // 2
        return to_pair(lax.dynamic_slice_in_dim(shard, me_z % 2 * size, size, 0))

    def second_half(shard, direct, axis):
        if not routed_by_ctx:
            return gather_weight(shard, axis)
        routed = over(direct, "ctx", [(i, i ^ 1) for i in range(n_ctx)])
        odd = me_z % 2
        first = jnp.where(odd == 0, direct, routed)
        second = jnp.where(odd == 0, routed, direct)
        other = jnp.concatenate([first, second], axis=0)
        return jnp.concatenate([shard, other], axis=axis)

    def sum_tp(mine, other_low):
        total = mine + to_core(other_low).astype(F32)
        step = 2
        while step < n_tp:
            low = kept(total.astype(BF))
            pairs = [(i, i ^ step) for i in range(n_tp)]
            total = low.astype(F32) + over(low, "tp", pairs).astype(F32)
            step *= 2
        return total

    def whole_rows(values):
        other = to_core(values)
        first = jnp.where(mine_row == 0, values, other)
        second = jnp.where(mine_row == 0, other, values)
        return jnp.concatenate([first, second], axis=0)

    def rows_of(values, start):
        return lax.dynamic_slice_in_dim(values, start, half, 0)

    def after(value, *tokens):
        return lax.optimization_barrier((value,) + tokens)[0]

    def shares_of(make, axis):
        if paired:
            return make(0).astype(BF), make(1).astype(BF)
        whole = make(None)
        return (
            lax.psum_scatter(whole, "fsdp", scatter_dimension=axis, tiled=True).astype(BF),
            None,
        )

    def sum_over_tp(values):
        step = 1
        while step < n_tp:
            values = values + over(values, "tp", [(i, i ^ step) for i in range(n_tp)])
            step *= 2
        return values

    def sum_over_fsdp(values):
        return values + to_pair(values) if paired else lax.psum(values, "fsdp")

    def sum_over_ctx(values):
        step = 1
        while step < n_ctx:
            values = values + over(values, "ctx", [(i, i ^ step) for i in range(n_ctx)])
            step *= 2
        return values

    def sum_all(values):
        return sum_over_ctx(sum_over_fsdp(sum_over_tp(values)))

    def part_of(values, part):
        if part is None:
            return values
        size = values.shape[-1] // 2
        return values[..., part * size : (part + 1) * size]

    groups = w_qkv.shape[1] // LANES
    split_at = GROUP * HEAD_SIZE
    q_spans = [(g * LANES, split_at) for g in range(groups)]
    kv_spans = [(g * LANES + split_at, 2 * HEAD_SIZE) for g in range(groups)]
    shard_q, shard_kv, squares_qkv = cast(w_qkv, [q_spans, kv_spans])
    if paired:
        other_kv, other_q = to_pair(shard_kv), to_pair(shard_q)
    else:
        full_kv, full_q = gather_weight(shard_kv, 0), gather_weight(shard_q, 0)
    shard_out, squares_out = cast(after(w_out, shard_kv))
    full_out = gather_weight(shard_out, 1)
    shard_gate, shard_up, squares_gate_up = cast_pair(after(w_gate_up, shard_out))
    direct_gate, direct_up = first_half(shard_gate), first_half(shard_up)

    inputs32 = turn(block_input[0].astype(F32))
    grad_rows = turn(cotangent[0])
    gain_a, gain_f = turn(gain_attn), turn(gain_ffn)
    unit_one, inv_one = unit_rows(inputs32)
    h_one = (unit_one * gain_a).astype(BF)
    freq = jnp.exp(
        jnp.arange(HEAD_SIZE // 2, dtype=F32) * (-2.0 * math.log(THETA) / HEAD_SIZE)
    )
    angle = freq[:, None] * positions[0].astype(F32)[None, :]
    cos_t, sin_t = jnp.cos(angle), jnp.sin(angle)
    gain_q, gain_k = gain_query[:, None], gain_key[:, None]

    def from_features(mine, other, full):
        if not paired:
            return mm(full, h_one, 0, 1)
        return mm(mine, part_of(h_one, 0), 0, 1) + mm(other, part_of(h_one, 1), 0, 1)

    raw_kv_t = from_features(shard_kv, other_kv, None) if paired else from_features(None, None, full_kv)
    kv_t = prep_keys(raw_kv_t, cos_t, sin_t, gain_k)
    shard_down, squares_down = cast(after(w_down, kv_t))
    direct_down = first_half(shard_down)
    raw_q_t = from_features(shard_q, other_q, None) if paired else from_features(None, None, full_q)
    q_t = prep_queries(raw_q_t, cos_t, sin_t, gain_q)

    length = seq_lengths[0]
    kv_blocks, valids = [], []
    for back in range(n_ctx):
        moved = kv_t
        if back > 0:
            moved = over(kv_t, "ctx", [(i, i + back) for i in range(n_ctx - back)])
        kv_blocks.append(moved)
        count = jnp.clip(length - (me_z - back) * tokens, 0, tokens)
        valids.append(jnp.where(me_z >= back, count, 0).astype(jnp.int32).reshape(1))
    state = []
    for back in range(n_ctx):
        query = q_t
        if routed_by_ctx and 0 < back < 3:
            query = after(q_t, (direct_gate, direct_up)[back - 1])
        state = attend(back == 0, valids[back], query, kv_blocks[back], state)
        if back == 1:
            full_gate = second_half(shard_gate, direct_gate, 0)
        if back == min(2, n_ctx - 1):
            full_up = second_half(shard_up, direct_up, 0)
    acc_t, sums = state
    heads = acc_t.shape[0] // HEAD_SIZE
    inverse = (1.0 / sums.reshape(heads, 8, tokens)[:, :1, :])
    out_t = (acc_t.reshape(heads, HEAD_SIZE, tokens) * inverse).reshape(acc_t.shape)
    attn_t = kept(out_t.astype(BF))
    full_down = second_half(shard_down, direct_down, 1)

    def cols_of(values, start):
        return lax.dynamic_slice_in_dim(values, start, half, 1)

    attn_other = mm(cols_of(attn_t, other_row), full_out, 0, 0).astype(BF)
    attn_mine = mm(cols_of(attn_t, mine_row), full_out, 0, 0)
    resid = rows_of(inputs32, mine_row) + sum_tp(attn_mine, attn_other)
    unit_two, inv_two = unit_rows(resid)
    h_two = whole_rows((unit_two * gain_f).astype(BF))

    d_hidden = mm(grad_rows, full_down, 1, 1)
    gate, up = mm(h_two, full_gate, 1, 0), mm(h_two, full_up, 1, 0)
    gate_sigmoid = 1.0 / (1.0 + jnp.exp(-gate))
    gate_silu = gate * gate_sigmoid
    hidden = (gate_silu * up).astype(BF)
    slope = gate_sigmoid * (1.0 + gate * (1.0 - gate_sigmoid))
    d_gate = (d_hidden * up * slope).astype(BF)
    d_up = (d_hidden * gate_silu).astype(BF)

    def d_two_of(start):
        return mm(rows_of(d_gate, start), full_gate, 1, 1) + mm(rows_of(d_up, start), full_up, 1, 1)

    d_two = sum_tp(d_two_of(mine_row), d_two_of(other_row).astype(BF))
    down_mine, down_send = shares_of(lambda part: mm(hidden, part_of(grad_rows, part), 0, 0), 1)
    gate_mine, gate_send = shares_of(lambda part: mm(part_of(h_two, part), d_gate, 0, 0), 0)
    up_mine, up_send = shares_of(lambda part: mm(part_of(h_two, part), d_up, 0, 0), 0)
    arrived = []
    if paired:
        named = (down_send, gate_send, up_send)
        arrived = [to_pair(send) for send in named]
    d_resid = rows_of(grad_rows, mine_row).astype(F32) + norm_back(unit_two, inv_two, gain_f, d_two)
    d_attn = whole_rows(d_resid.astype(BF))

    d_heads_t = mm(full_out, d_attn, 1, 1).astype(BF)
    late_hidden = after(hidden, d_heads_t)
    ffn_other = mm(rows_of(late_hidden, other_row), full_down, 1, 0).astype(BF)
    ffn_mine = mm(rows_of(late_hidden, mine_row), full_down, 1, 0)
    block_output = turn(whole_rows(resid + sum_tp(ffn_mine, ffn_other)))

    d_q = None
    d_kv_parts = [None] * n_ctx
    for back in reversed(range(n_ctx)):
        d_q, d_kv = attend_back(
            back == 0, valids[back], q_t, kv_blocks[back], out_t, sums, d_heads_t, d_q
        )
        if back > 0:
            d_kv = over(d_kv, "ctx", [(i, i - back) for i in range(back, n_ctx)])
        d_kv_parts[back] = d_kv
    olds = [
        jnp.concatenate([jnp.pad(after(v, d_q), (0, padded(v.size) - v.size)) for v in vectors]).reshape(1, -1)
        for vectors in (
            (row_qkv_old, row_gate_up_old, col_out_old, col_down_old),
            (col_qkv_old, col_gate_up_old[0], col_gate_up_old[1], row_out_old, row_down_old),
        )
    ]
    row_of = lambda vectors: jnp.concatenate(vectors).reshape(1, 2 * D + 2 * HEAD_SIZE)
    gain_vars = row_of([after(v, d_q) for v in (var_attn_old, var_ffn_old, var_query_old, var_key_old)])
    gains_old = row_of([after(v, d_q) for v in (gain_attn, gain_ffn, gain_query, gain_key)])

    part_ffn_gain = jnp.sum(after(d_two, d_q) * unit_two, axis=0)
    out_mine, out_send = shares_of(lambda part: mm(attn_t, part_of(d_attn, part), 1, 0), 1)
    d_raw_q_t, d_raw_kv_t, sum_q, sum_k = prep_back(
        raw_q_t, raw_kv_t, cos_t, sin_t, gain_q, gain_k, d_q, d_kv_parts
    )

    def joined(q, kv):
        pieces = []
        for g in range(groups):
            pieces += [q[:, g * split_at : (g + 1) * split_at]]
            pieces += [kv[:, g * 2 * HEAD_SIZE : (g + 1) * 2 * HEAD_SIZE]]
        return jnp.concatenate(pieces, axis=1)

    def qkv_grad(part):
        rows = part_of(h_one, part)
        return joined(mm(rows, d_raw_q_t, 0, 1), mm(rows, d_raw_kv_t, 0, 1))

    qkv_mine, qkv_send = shares_of(qkv_grad, 0)

    if paired:
        full_kv = jnp.concatenate([after(shard_kv, d_q), other_kv], axis=0)
        full_q = jnp.concatenate([after(shard_q, d_q), other_q], axis=0)

    def d_one_of(start):
        return mm(cols_of(d_raw_kv_t, start), full_kv, 0, 1) + mm(
            cols_of(d_raw_q_t, start), full_q, 0, 1
        )

    mine = [down_mine, gate_mine, up_mine, out_mine, qkv_mine]
    squares = [squares_qkv, squares_out, squares_gate_up, squares_down]
    shares = (1.0 / n_tp, 1.0 / n_fsdp)
    share = 2.0 / n_tp
    row_parts = [turn(part_ffn_gain) * share, sum_q[:, 0], sum_k[:, 0]]
    if paired and n_ctx == 4 and n_tp == 4:
        others = [
            d_one_of(mine_row),
            d_one_of(other_row).astype(BF),
            d_resid,
            rows_of(turn(block_input[0]), mine_row),
            gain_a.reshape(1, D),
            row_of([jnp.zeros((D,), F32)] + row_parts),
        ]
        grads, news, scales, gain_grads, totals, input_grad = close(
            mine, arrived, [out_send, qkv_send], others + olds + squares, shares
        )
        whole_grads, steps, input_grad, stat_rows, gain_rows, rms = write_all(
            grads, news, scales, gain_grads, totals, input_grad, gain_vars, gains_old
        )
        stat_list = [value[0] for value in stat_rows]
        gain_list = [value[0] for value in gain_rows]
    else:
        d_one = sum_tp(d_one_of(mine_row), d_one_of(other_row).astype(BF))
        unit_half, inv_half = rows_of(unit_one, mine_row), rows_of(inv_one, mine_row)
        part_attn_gain = jnp.sum(d_one * unit_half, axis=0)
        input_grad = turn(whole_rows(d_resid + norm_back(unit_half, inv_half, gain_a, d_one)))
        gain_grads = sum_all(row_of([turn(part_attn_gain) * share] + row_parts))
        if n_ctx == 4:
            down, gate_sum, up_sum, out_sum, qkv_sum = line_sums(
                mine, arrived, [out_send, qkv_send] if paired else []
            )
        else:
            theirs = arrived + [to_pair(send) for send in (out_send, qkv_send)] if paired else []
            if paired:
                mine = [left.astype(F32) + right.astype(F32) for left, right in zip(mine, theirs)]
            down, gate_sum, up_sum, out_sum, qkv_sum = (
                kept(lax.psum(part.astype(F32), "ctx").astype(BF)) for part in mine
            )
        grads = [qkv_sum, out_sum, gate_sum, up_sum, down]
        by_tp, by_fsdp = stats(grads)
        sums = [sum_over_tp(by_tp), sum_over_fsdp(by_fsdp)]
        whole_grads, news, scales, scalars = scaled(shares, grads, sums, olds, squares)
        totals = lax.psum(scalars, ("fsdp", "tp"))
        steps, new_vars, gain_steps, rms = finish(
            grads, scales, totals, gain_grads, gain_vars, gains_old
        )

        places = layout_of(grads)
        spots = [place for pair in places for place in pair]
        del spots[6]
        stat_list = [news[at][0, span] for at, span in spots]
        gain_list = [
            row[0, start : start + size]
            for row in (gain_grads, new_vars, gain_steps)
            for start, size in GAIN_SPANS
        ]
    row_qkv, col_qkv, row_out, col_out, row_gu, col_gate, col_up, row_down, col_down = stat_list
    return (
        block_output[None],
        input_grad[None],
        *whole_grads,
        *gain_list[:4],
        row_qkv,
        col_qkv,
        row_out,
        col_out,
        row_gu,
        jnp.stack([col_gate, col_up]),
        row_down,
        col_down,
        *gain_list[4:8],
        *steps,
        *gain_list[8:],
        rms[0, 0],
    )


def solution(mesh):
    tokens, vector = P("fsdp", "ctx", None), P()
    by_f, by_t = P("fsdp"), P("tp")
    w_specs = (P("fsdp", "tp"), P("tp", "fsdp"), P("fsdp", None, "tp"), P("tp", "fsdp"))
    stats = (by_f, by_t, by_t, by_f, by_f, P(None, "tp"), by_t, by_f) + (vector,) * 4

    def body(*args):
        return on_device(dict(mesh.shape), *args)

    return jax.shard_map(
        body,
        mesh=mesh,
        in_specs=(tokens, tokens, by_f, P("fsdp", "ctx")) + w_specs + (vector,) * 4 + stats,
        out_specs=(tokens, tokens)
        + w_specs
        + (vector,) * 4
        + stats
        + w_specs
        + (vector,) * 4
        + (vector,),
        check_vma=False,
    )
```

```python
import functools
import math

import jax
import jax.numpy as jnp
from jax import lax
from jax.experimental import pallas as pl
from jax.experimental.pallas import tpu as pltpu
from jax.sharding import PartitionSpec as P


D = 1024
QUERY_HEADS = 16
KEY_VALUE_HEADS = 8
HEAD_SIZE = 64
FF = 4608
QKV = 2048

EPS = 1e-05
THETA = 1000000.0
DECAY = 0.5
CLIP = 0.15
RATE = 1.0

BF = jnp.bfloat16
F32 = jnp.float32
GROUP = QUERY_HEADS // KEY_VALUE_HEADS
LANES = (GROUP + 2) * HEAD_SIZE
KEY_TILE = 256
PAIR_BLOCKS = 4
LAG = 2
WINDOW = 3
GAIN_SHARE = 0.5


def mm(left, right, left_dim, right_dim):
    return lax.dot_general(
        left, right, (((left_dim,), (right_dim,)), ((), ())), preferred_element_type=F32
    )


def params(vmem=48 << 20):
    return pltpu.CompilerParams(vmem_limit_bytes=vmem)


def squares_into(sum_ref, values):
    rows, cols = values.shape
    sum_ref[...] += jnp.sum((values * values).reshape(rows // 8, 8, cols), axis=0)


def cast_kernel(spans, w_ref, *refs):
    sum_ref = refs[-1]

    @pl.when(pl.program_id(0) == 0)
    def _():
        sum_ref[...] = jnp.zeros_like(sum_ref)

    values = w_ref[...]
    for out_ref, pieces in zip(refs, spans):
        at = 0
        for start, size in pieces:
            out_ref[:, at : at + size] = values[:, start : start + size].astype(BF)
            at += size
    squares_into(sum_ref, values)


def cast(weight, spans=None):
    rows, cols = weight.shape
    spans = spans or [[(0, cols)]]
    widths = [sum(size for _, size in pieces) for pieces in spans]
    block = min(rows, 128)
    return pl.pallas_call(
        functools.partial(cast_kernel, spans),
        grid=(rows // block,),
        in_specs=[pl.BlockSpec((block, cols), lambda i: (i, 0))],
        out_specs=[pl.BlockSpec((block, width), lambda i: (i, 0)) for width in widths]
        + [pl.BlockSpec((8, cols), lambda i: (0, 0))],
        out_shape=[jax.ShapeDtypeStruct((rows, width), BF) for width in widths]
        + [jax.ShapeDtypeStruct((8, cols), F32)],
        cost_estimate=pl.CostEstimate(
            flops=3 * rows * cols, bytes_accessed=6 * rows * cols, transcendentals=0
        ),
        compiler_params=params(8 << 20),
        name="cast",
    )(weight)


def cast_pair_kernel(w_ref, gate_ref, up_ref, sum_ref, held, sems):
    rows = w_ref.shape[0]
    block = rows // PAIR_BLOCKS
    copies = []
    for step in range(PAIR_BLOCKS):
        for which in range(2):
            span = pl.ds(step * block, block)
            copies.append(
                pltpu.make_async_copy(
                    w_ref.at[span, which, :], held.at[which, span, :], sems.at[which, step]
                )
            )
            copies[-1].start()
    sum_ref[...] = jnp.zeros_like(sum_ref)
    for step in range(PAIR_BLOCKS):
        for which, out_ref in enumerate((gate_ref, up_ref)):
            copies[2 * step + which].wait()

            @pl.loop(0, block // 16)
            def _(piece):
                at = pl.multiple_of(step * block + piece * 16, 16)
                values = held[which, pl.ds(at, 16), :]
                out_ref[pl.ds(at, 16), :] = values.astype(BF)
                squares_into(sum_ref, values)


def cast_pair(weight):
    rows, _, cols = weight.shape
    vmem = pl.BlockSpec(memory_space=pltpu.VMEM)
    return pl.pallas_call(
        cast_pair_kernel,
        in_specs=[pl.BlockSpec(memory_space=pl.ANY)],
        out_specs=[vmem] * 3,
        out_shape=[jax.ShapeDtypeStruct((rows, cols), BF)] * 2
        + [jax.ShapeDtypeStruct((8, cols), F32)],
        scratch_shapes=[
            pltpu.VMEM((2, rows, cols), F32),
            pltpu.SemaphoreType.DMA((2, PAIR_BLOCKS)),
        ],
        cost_estimate=pl.CostEstimate(
            flops=6 * rows * cols, bytes_accessed=12 * rows * cols, transcendentals=0
        ),
        compiler_params=params(58 << 20),
        name="cast_pair",
    )(weight)


def lane_total(values):
    lanes = min(128, values.shape[1])
    total = values[:, :lanes]
    for at in range(lanes, values.shape[1], lanes):
        total = total + values[:, at : at + lanes]
    return total


def padded(size):
    return -(-size // 128) * 128


def spans_of(sizes):
    out, at = [], 0
    for size in sizes:
        out.append(slice(at, at + size))
        at += padded(size)
    return out


def layout_of(grads):
    qkv, out, gate, up, down = (g.shape for g in grads)
    tp_spans = spans_of([qkv[0], gate[0], out[1], down[1]])
    fsdp_spans = spans_of([qkv[1], gate[1], up[1], out[0], down[0]])
    return (
        ((0, tp_spans[0]), (1, fsdp_spans[0])),
        ((1, fsdp_spans[3]), (0, tp_spans[2])),
        ((0, tp_spans[1]), (1, fsdp_spans[1])),
        ((0, tp_spans[1]), (1, fsdp_spans[2])),
        ((1, fsdp_spans[4]), (0, tp_spans[3])),
    )


def packed_sizes(grads):
    qkv, out, gate, up, down = (g.shape for g in grads)
    return (
        sum(map(padded, (qkv[0], gate[0], out[1], down[1]))),
        sum(map(padded, (qkv[1], gate[1], up[1], out[0], down[0]))),
    )


def over_blocks(n_rows, block, body, init=None):
    if n_rows == block:
        return body(0, init)
    aligned = lambda step, carry: body(pl.multiple_of(step * block, block), carry)
    return lax.fori_loop(0, n_rows // block, aligned, init)


def stats_kernel(*refs):
    grads, packed = refs[:5], refs[5:]
    for ref in packed:
        ref[...] = jnp.zeros_like(ref)
    for grad_ref, places in zip(grads, layout_of(grads)):
        n_rows = grad_ref.shape[0]
        block = min(n_rows, 128)
        (row_at, row_span), (col_at, col_span) = places
        row_ref, col_ref = packed[row_at], packed[col_at]

        def add_block(at, carry):
            values = grad_ref[pl.ds(at, block), :].astype(F32)
            square = values * values
            col_ref[:, col_span] += jnp.sum(square, axis=0, keepdims=True)
            folded = jnp.sum(lane_total(square).T, axis=0, keepdims=True)
            start = row_span.start + at
            place = pl.ds(start if n_rows == block else pl.multiple_of(start, block), block)
            row_ref[:, place] += folded
            return carry

        over_blocks(n_rows, block, add_block, 0)


def stats(grads):
    vmem = pl.BlockSpec(memory_space=pltpu.VMEM)
    return pl.pallas_call(
        stats_kernel,
        in_specs=[vmem] * 5,
        out_specs=[vmem] * 2,
        out_shape=[jax.ShapeDtypeStruct((1, size), F32) for size in packed_sizes(grads)],
        cost_estimate=pl.CostEstimate(
            flops=4 * sum(g.size for g in grads),
            bytes_accessed=2 * sum(g.size for g in grads),
            transcendentals=0,
        ),
        compiler_params=params(),
        name="stats",
    )(*grads)


def columns_of(row, width):
    return jnp.broadcast_to(row, (min(128, width), row.shape[1])).T


def total_of(values):
    return jnp.sum(jnp.sum(values, axis=0, keepdims=True), axis=1, keepdims=True)


def out_views(outs):
    qkv, out, gate_up, down = outs
    return (
        lambda span: qkv.at[span, :],
        lambda span: out.at[span, :],
        lambda span: gate_up.at[span, 0, :],
        lambda span: gate_up.at[span, 1, :],
        lambda span: down.at[span, :],
    )


def tiles_in(grads):
    for index, grad_ref in enumerate(grads):
        block = min(grad_ref.shape[0], 128)
        for at in range(0, grad_ref.shape[0], block):
            yield index, at, block


def write_shapes(grads):
    qkv, out, gate, _, down = (g.shape for g in grads)
    return [
        jax.ShapeDtypeStruct(shape, F32) for shape in (qkv, out, (gate[0], 2, gate[1]), down)
    ]


def write_scratch(grads):
    count = len(list(tiles_in(grads)))
    return [pltpu.VMEM(g.shape, F32) for g in grads] + [pltpu.SemaphoreType.DMA((count,))]


COUNTS = ((QKV, D), (D, D), (2 * FF, D), (2 * FF, D), (D, FF))


def new_statistics(places, sums, olds, news, scales):
    for (row_place, col_place), count in zip(places, COUNTS):
        for (at, span), size in zip((row_place, col_place), count):
            new = DECAY * olds[at][:, span] + (1.0 - DECAY) * (sums[at][:, span] / size)
            news[at][:, span] = new
            scales[at][:, span] = lax.rsqrt(new)


def scalars_into(scalar_ref, shares, places, held, sums, olds, squares, scales):
    parts = []
    for (row_place, col_place), grad_ref in zip(places, held):
        n_rows, n_cols = grad_ref.shape
        block = min(n_rows, 128)
        lanes = min(128, n_cols)
        left_ref, row_start = scales[row_place[0]], row_place[1].start
        right = scales[col_place[0]][:, col_place[1]]

        def step_of(at, total):
            values = grad_ref[pl.ds(at, block), :].astype(F32) * right
            start = row_start + at
            place = pl.ds(start if n_rows == block else pl.multiple_of(start, block), block)
            left = columns_of(left_ref[:, place], n_cols)
            folded = lane_total(values * values) * (left * left)
            return total + jnp.sum(folded.reshape(block // 8, 8, lanes), axis=0)

        total = over_blocks(n_rows, block, step_of, jnp.zeros((8, lanes), F32))
        parts.append(total_of(total))
    scalars = [parts[0], parts[1], parts[2] + parts[3], parts[4]]
    row_places = [places[index][0] for index in (0, 1, 2, 4)]
    scalars += [total_of(sums[at][:, span]) * shares[at] for at, span in row_places]
    scalars += [total_of(ref[...]) for ref in squares]
    scalars += [total_of(olds[at][:, span]) * shares[at] for at, span in row_places]
    lane = lax.broadcasted_iota(jnp.int32, (8, 128), 1)
    packed = jnp.zeros((8, 128), F32)
    for number, value in enumerate(scalars):
        packed = jnp.where(lane == number, value, packed)
    scalar_ref[...] = packed


def scaled_kernel(shares, *refs):
    grads, sums, olds, squares = refs[:5], refs[5:7], refs[7:9], refs[9:13]
    outs, news, scale_refs, scalar_ref = refs[13:17], refs[17:19], refs[19:21], refs[21]
    held, sems = refs[22:27], refs[27]
    copies = []
    views = out_views(outs)
    for number, (index, at, block) in enumerate(tiles_in(grads)):
        span = pl.ds(at, block)
        held[index][span, :] = grads[index][span, :].astype(F32)
        copies.append(
            pltpu.make_async_copy(held[index].at[span, :], views[index](span), sems.at[number])
        )
        copies[-1].start()
    places = layout_of(grads)
    new_statistics(places, sums, olds, news, scale_refs)
    scalars_into(scalar_ref, shares, places, held, sums, olds, squares, scale_refs)
    for copy in copies:
        copy.wait()


def scaled(shares, grads, sums, olds, squares):
    vmem, hbm = pl.BlockSpec(memory_space=pltpu.VMEM), pl.BlockSpec(memory_space=pl.ANY)
    vectors = [jax.ShapeDtypeStruct((1, size), F32) for size in packed_sizes(grads)]
    out = pl.pallas_call(
        functools.partial(scaled_kernel, shares),
        in_specs=[vmem] * 13,
        out_specs=[hbm] * 4 + [vmem] * 5,
        out_shape=write_shapes(grads) + vectors * 2 + [jax.ShapeDtypeStruct((8, 128), F32)],
        scratch_shapes=write_scratch(grads),
        cost_estimate=pl.CostEstimate(
            flops=6 * sum(g.size for g in grads),
            bytes_accessed=6 * sum(g.size for g in grads),
            transcendentals=0,
        ),
        compiler_params=params(),
        name="scaled",
    )(*grads, *sums, *olds, *squares)
    return out[:4], out[4:6], out[6:8], out[8]


SIZES = ((D, QKV), (D, D), (D, 2 * FF), (FF, D))


def gain_parts(total_ref, gain_grad_ref, var_ref, gain_ref, new_var_ref, gain_step_ref, rms_ref):
    value = lambda number: total_ref[0:1, number : number + 1]
    means = [
        DECAY * value(12 + index) / rows + (1.0 - DECAY) * value(4 + index) / (rows * cols)
        for index, (rows, cols) in enumerate(SIZES)
    ]
    gain_grad = gain_grad_ref[...]
    new_var = DECAY * var_ref[...] + (1.0 - DECAY) * gain_grad * gain_grad
    new_var_ref[...] = new_var
    raw_gain = gain_grad * lax.rsqrt(new_var)
    total = jnp.sum(raw_gain * raw_gain, axis=1, keepdims=True)
    for index, mean in enumerate(means):
        total = total + value(index) * mean
    count = D * QKV + D * D + 2 * D * FF + FF * D + 2 * D + 2 * HEAD_SIZE
    rms = jnp.sqrt(total / count)
    rms_ref[...] = jnp.broadcast_to(rms, rms_ref.shape)
    clip = jnp.maximum(1.0, rms / CLIP)
    for start, size in ((0, D), (D, D)):
        span = slice(start, start + size)
        gain = gain_ref[:, span]
        scale = -RATE * jnp.sqrt(jnp.sum(gain * gain, axis=1, keepdims=True) / size) / clip
        gain_step_ref[:, span] = raw_gain[:, span] * scale
    span = slice(2 * D, 2 * D + 2 * HEAD_SIZE)
    gain = gain_ref[:, span]
    low = lax.broadcasted_iota(jnp.int32, gain.shape, 1) < HEAD_SIZE
    square = gain * gain
    low_sum = jnp.sum(jnp.where(low, square, 0.0), axis=1, keepdims=True)
    high_sum = jnp.sum(jnp.where(low, 0.0, square), axis=1, keepdims=True)
    scale = -RATE * jnp.sqrt(jnp.where(low, low_sum, high_sum) / HEAD_SIZE) / clip
    gain_step_ref[:, span] = raw_gain[:, span] * scale
    return [
        -RATE * jnp.sqrt(value(8 + index) / (rows * cols)) * jnp.sqrt(means[index]) / clip
        for index, (rows, cols) in enumerate(SIZES)
    ]


def write_steps(factors, places, grads, scales, held, views, sems, before=None):
    copies = []
    for number, (index, at, block) in enumerate(tiles_in(grads)):
        if before is not None and at == 0:
            before(index)
        span = pl.ds(at, block)
        (row_at, row_span), (col_at, col_span) = places[index]
        start = row_span.start + at
        n_cols = grads[index].shape[1]
        left = columns_of(scales[row_at][:, start : start + block], n_cols)
        right = scales[col_at][:, col_span] * factors[(0, 1, 2, 2, 3)[index]]
        for first in range(0, n_cols, left.shape[1]):
            lanes = slice(first, first + left.shape[1])
            tile = grads[index][span, lanes].astype(F32)
            held[index][span, lanes] = tile * left * right[:, lanes]
        copies.append(
            pltpu.make_async_copy(held[index].at[span, :], views[index](span), sems.at[number])
        )
        copies[-1].start()
    return copies


def finish_kernel(*refs):
    grads, scale_refs, total_ref = refs[:5], refs[5:7], refs[7]
    outs, held, sems = refs[11:15], refs[18:23], refs[23]
    factors = gain_parts(total_ref, *refs[8:11], *refs[15:18])
    copies = write_steps(
        factors, layout_of(grads), grads, scale_refs, held, out_views(outs), sems
    )
    for copy in copies:
        copy.wait()


def finish(grads, scales, totals, gain_grads, gain_vars, gains):
    vmem, hbm = pl.BlockSpec(memory_space=pltpu.VMEM), pl.BlockSpec(memory_space=pl.ANY)
    vector = jax.ShapeDtypeStruct(gains.shape, F32)
    out = pl.pallas_call(
        finish_kernel,
        in_specs=[vmem] * 11,
        out_specs=[hbm] * 4 + [vmem] * 3,
        out_shape=write_shapes(grads) + [vector, vector, jax.ShapeDtypeStruct((8, 128), F32)],
        scratch_shapes=write_scratch(grads),
        cost_estimate=pl.CostEstimate(
            flops=4 * sum(g.size for g in grads),
            bytes_accessed=6 * sum(g.size for g in grads),
            transcendentals=0,
        ),
        compiler_params=params(),
        name="finish",
    )(*grads, *scales, totals, gain_grads, gain_vars, gains)
    return out[:4], out[4], out[5], out[6]


def pieces_of(shapes):
    out = []
    for index, (rows, cols) in enumerate(shapes):
        size = rows
        while size % 32 == 0 and size * cols > 160 * 1024:
            size //= 2 if size % 64 == 0 else 3
        out += [(index, at, size) for at in range(0, rows, size)]
    return out


def line_kernel(shapes, arrived, pairs, *refs):
    count = len(shapes)
    refs = list(refs)
    take = lambda size: [refs.pop(0) for _ in range(size)]
    mine = take(count)
    theirs = take(arrived if pairs else 0)
    sends = take(count - arrived if pairs else 0)
    final = take(count)
    work, land, cross = take(count), take(count), take(count)
    theirs += take(count - arrived if pairs else 0)
    in_send, in_recv, mid_send, mid_recv, out_send, out_recv, x_send, x_recv = refs
    me = lax.axis_index("ctx")
    partner = me + 1 - 2 * (me % 2)
    opposite = 3 - me
    at_end = (me == 0) | (me == 3)
    lanes = [{"ctx": partner}, {"ctx": opposite}]
    if pairs:
        lanes.append({"fsdp": 1 - lax.axis_index("fsdp")})
    barrier = pltpu.get_barrier_semaphore()
    for lane in lanes:
        pl.semaphore_signal(barrier, inc=1, device_id=lane, device_id_type=pl.DeviceIdType.MESH)
    pl.semaphore_wait(barrier, len(lanes))

    def remote(source, target, send, recv, number, lane):
        index, at, size = pieces[number]
        span = pl.ds(at, size)
        return pltpu.make_async_remote_copy(
            src_ref=source[index].at[span, :],
            dst_ref=target[index].at[span, :],
            send_sem=send.at[number],
            recv_sem=recv.at[number],
            device_id=lanes[lane],
            device_id_type=pl.DeviceIdType.MESH,
        )

    pieces = pieces_of(shapes)
    numbers = range(len(pieces))
    inwards = [remote(work, land, in_send, in_recv, i, 0) for i in numbers]
    across = [remote(work, cross, mid_send, mid_recv, i, 1) for i in numbers]
    outwards = [remote(final, final, out_send, out_recv, i, 0) for i in numbers]
    exchanged = {}
    if pairs:
        padded_sends = [None] * arrived + sends
        for i in numbers:
            if pieces[i][0] >= arrived:
                exchanged[i] = remote(padded_sends, theirs, x_send, x_recv, i, 2)
                exchanged[i].start()

    def add(target, number, *sources):
        index, at, size = pieces[number]
        step = 32 if size % 32 == 0 else 16

        @pl.loop(0, size // step)
        def _(piece):
            span = pl.ds(pl.multiple_of(at + piece * step, 16), step)
            total = sources[0][index][span, :].astype(F32)
            for source in sources[1:]:
                total = total + source[index][span, :].astype(F32)
            target[index][span, :] = total.astype(BF)

    own = (mine, theirs) if pairs else (mine,)

    def ready(number):
        if number in exchanged:
            exchanged[number].wait_recv()

    @pl.when(at_end)
    def _():
        for i in numbers:
            ready(i)
            add(work, i, *own)
            inwards[i].start()
        for i in numbers:
            inwards[i].wait_send()
            outwards[i].wait_recv()

    @pl.when(jnp.logical_not(at_end))
    def _():
        lag = 2
        for i in range(len(pieces) + lag):
            if i < len(pieces):
                ready(i)
                inwards[i].wait_recv()
                add(work, i, *own, land)
                across[i].start()
            if i >= lag:
                across[i - lag].wait_recv()
                add(final, i - lag, work, cross)
                outwards[i - lag].start()
        for i in numbers:
            across[i].wait_send()
            outwards[i].wait_send()

    for copy in exchanged.values():
        copy.wait_send()


def line_sums(mine, theirs, sends):
    shapes = [m.shape for m in mine]
    pairs = bool(sends) or bool(theirs)
    count, arrived = len(mine), len(theirs)
    number = len(pieces_of(shapes))
    vmem = pl.BlockSpec(memory_space=pltpu.VMEM)
    held = [pltpu.VMEM(shape, BF) for shape in shapes]
    size = sum(m.size for m in mine)
    return pl.pallas_call(
        functools.partial(line_kernel, shapes, arrived, pairs),
        in_specs=[vmem] * (count + len(theirs) + len(sends)),
        out_specs=[vmem] * count,
        out_shape=[jax.ShapeDtypeStruct(shape, BF) for shape in shapes],
        scratch_shapes=held * 3
        + (held[arrived:] if pairs else [])
        + [pltpu.SemaphoreType.DMA((number,))] * 8,
        cost_estimate=pl.CostEstimate(flops=4 * size, bytes_accessed=80 * size, transcendentals=0),
        compiler_params=pltpu.CompilerParams(
            vmem_limit_bytes=56 << 20, collective_id=0, has_side_effects=True
        ),
        name="line_sums",
    )(*mine, *theirs, *sends)


def close_kernel(shapes, arrived, shares, *refs):
    count = len(shapes)
    refs = list(refs)
    take = lambda size: [refs.pop(0) for _ in range(size)]
    mine, theirs, sends = take(count), take(arrived), take(count - arrived)
    d_mine_ref, d_other_ref, d_resid_ref, x_ref, gain_a_ref, gain_row_ref = take(6)
    olds, squares = take(2), take(4)
    final, news, scales = take(count), take(2), take(2)
    gain_grad_ref, total_ref, grad_out_ref = take(3)
    work, land, cross = take(count), take(count), take(count)
    theirs += take(count - arrived)
    packed, sums = take(2), take(2)
    core_ref, low_ref, y_ref = take(3)
    rows, row_got, tp_mid, got_tp, got_fsdp = take(5), take(5), take(1)[0], take(2), take(1)[0]
    scalar_refs, scalar_got = take(3) + [total_ref], take(3)
    in_send, in_recv, mid_send, mid_recv, out_send, out_recv, x_send, x_recv = take(8)
    s_send, s_recv = take(2)

    me_f, me_z, me_t = (lax.axis_index(name) for name in ("fsdp", "ctx", "tp"))
    at_end = (me_z == 0) | (me_z == 3)
    lane = {
        "near": {"ctx": me_z + 1 - 2 * (me_z % 2)},
        "far": {"ctx": 3 - me_z},
        "x": {"fsdp": 1 - me_f},
        "core": {"tp": me_t + 1 - 2 * (me_t % 2)},
        "y": {"tp": (me_t + 2) % 4},
    }
    mesh_ids = pl.DeviceIdType.MESH
    barrier = pltpu.get_barrier_semaphore()
    for device in lane.values():
        pl.semaphore_signal(barrier, inc=1, device_id=device, device_id_type=mesh_ids)
    pl.semaphore_wait(barrier, len(lane))

    def remote(source, target, send, recv, name):
        return pltpu.make_async_remote_copy(
            src_ref=source,
            dst_ref=target,
            send_sem=send,
            recv_sem=recv,
            device_id=lane[name],
            device_id_type=mesh_ids,
        )

    pieces = pieces_of(shapes)
    numbers = range(len(pieces))

    def piece_copy(source, target, send, recv, name, number):
        index, at, size = pieces[number]
        span = pl.ds(at, size)
        return remote(
            source[index].at[span, :], target[index].at[span, :], send.at[number], recv.at[number], name
        )

    inwards = [piece_copy(work, land, in_send, in_recv, "near", i) for i in numbers]
    across = [piece_copy(work, cross, mid_send, mid_recv, "far", i) for i in numbers]
    outwards = [piece_copy(final, final, out_send, out_recv, "near", i) for i in numbers]
    late = [i for i in numbers if pieces[i][0] >= arrived]
    all_sends = [None] * arrived + sends
    exchanged = {i: piece_copy(all_sends, theirs, x_send, x_recv, "x", i) for i in late}
    small = []

    def message(source, target, name):
        number = len(small)
        small.append(remote(source, target, s_send.at[number], s_recv.at[number], name))
        small[-1].start()
        return small[-1]

    d_core = message(d_other_ref, core_ref, "core")
    for ref in packed:
        ref[...] = jnp.zeros_like(ref)

    def add(target, number, *sources):
        index, at, size = pieces[number]
        step = 32 if size % 32 == 0 else 16

        @pl.loop(0, size // step)
        def _(piece):
            span = pl.ds(pl.multiple_of(at + piece * step, 16), step)
            total = sources[0][index][span, :].astype(F32)
            for source in sources[1:]:
                total = total + source[index][span, :].astype(F32)
            target[index][span, :] = total.astype(BF)

    def ready(number):
        if number in exchanged:
            exchanged[number].wait_recv()

    def pass_on(i):
        if i < len(late):
            exchanged[late[i]].start()

        @pl.when(at_end)
        def _():
            if 0 <= i - WINDOW < len(pieces):
                inwards[i - WINDOW].wait_send()
            if i < len(pieces):
                ready(i)
                add(work, i, mine, theirs)
                inwards[i].start()

        @pl.when(jnp.logical_not(at_end))
        def _():
            if i < len(pieces):
                ready(i)
                inwards[i].wait_recv()
                add(work, i, mine, theirs, land)
                across[i].start()
            if 0 <= i - LAG < len(pieces):
                across[i - LAG].wait_recv()
                add(final, i - LAG, work, cross)
                outwards[i - LAG].start()

    half = d_mine_ref.shape[0]
    block = 32
    state = {}

    def add_cores():
        d_core.wait_recv()

        @pl.loop(0, half // block)
        def _(step):
            span = pl.ds(pl.multiple_of(step * block, block), block)
            low_ref[span, :] = (d_mine_ref[span, :] + core_ref[span, :].astype(F32)).astype(BF)

        state["y"] = message(low_ref, y_ref, "y")

    def input_grads():
        state["y"].wait_recv()
        gain = gain_a_ref[...]
        my_rows = (me_t % 2) * half
        split = gain.shape[1] // 2

        def rows_step(step, total):
            span = pl.ds(pl.multiple_of(step * block, block), block)
            grad = low_ref[span, :].astype(F32) + y_ref[span, :].astype(F32)
            values = x_ref[span, :].astype(F32)
            inv = lax.rsqrt(jnp.mean(values * values, axis=-1, keepdims=True) + EPS)
            unit = values * inv
            shifted = grad * gain
            mean = jnp.mean(shifted * unit, axis=-1, keepdims=True)
            result = d_resid_ref[span, :] + (shifted - unit * mean) * inv
            place = pl.ds(pl.multiple_of(my_rows + step * block, block), block)

            @pl.when(me_f == 0)
            def _():
                grad_out_ref[place, :] = result

            @pl.when(me_f != 0)
            def _():
                grad_out_ref[place, :split] = result[:, split:]
                grad_out_ref[place, split:] = result[:, :split]

            return total + jnp.sum((grad * unit).reshape(block // 8, 8, 2 * split), axis=0)

        total = lax.fori_loop(0, half // block, rows_step, jnp.zeros((8, 2 * split), F32))
        total = jnp.sum(total, axis=0, keepdims=True) * GAIN_SHARE
        rows[0][...] = gain_row_ref[...]

        @pl.when(me_f == 0)
        def _():
            rows[0][:, : 2 * split] = total

        @pl.when(me_f != 0)
        def _():
            rows[0][:, :split] = total[:, split:]
            rows[0][:, split : 2 * split] = total[:, :split]

        mine_span = pl.ds(pl.multiple_of(my_rows, half), half)
        state["grad"] = message(grad_out_ref.at[mine_span, :], grad_out_ref.at[mine_span, :], "core")
        state["row"] = message(rows[0], row_got[0], "core")

    def add_row(step):
        def run():
            state["row"].wait_recv()
            total = rows[step][...] + row_got[step][...]
            if step < 4:
                rows[step + 1][...] = total
                name = ("y", "x", "near", "far")[step]
                state["row"] = message(rows[step + 1], row_got[step + 1], name)
            else:
                gain_grad_ref[...] = total

        return run

    order = (4, 2, 3, 1, 0)
    travel = [order.index(index) for index in range(count)]
    by_order = lambda values: [values[index] for index in travel]
    places = layout_of(by_order(final))

    def settle(index):
        def run():
            grad_ref = final[index]
            n_rows = grad_ref.shape[0]
            (row_at, row_span), (col_at, col_span) = places[order[index]]

            @pl.when(at_end)
            def _():
                for i in numbers:
                    if pieces[i][0] == index:
                        outwards[i].wait_recv()

            @pl.loop(0, n_rows // 128)
            def _(step):
                at = pl.multiple_of(step * 128, 128)
                values = grad_ref[pl.ds(at, 128), :].astype(F32)
                square = values * values
                packed[col_at][:, col_span] += jnp.sum(square, axis=0, keepdims=True)
                folded = jnp.sum(lane_total(square).T, axis=0, keepdims=True)
                place = pl.ds(pl.multiple_of(row_span.start + at, 128), 128)
                packed[row_at][:, place] += folded

        return run

    last = {index: max(i for i in numbers if pieces[i][0] == index) for index in range(count)}
    unit = max(len(pieces) // 17, 1)
    events = {unit: [add_cores], 4 * unit: [input_grads]}
    for step in range(5):
        events.setdefault((5 + step) * unit, []).append(add_row(step))
    for index in range(3):
        events.setdefault(last[index] + LAG + 3, []).append(settle(index))
    for i in range(len(pieces) + max(LAG, WINDOW)):
        for run in events.pop(i, []):
            run()
        pass_on(i)
    for i in sorted(events):
        for run in events[i]:
            run()
    for index in range(3, count):
        settle(index)()

    over_core = message(packed[0], got_tp[0], "core")
    over_x = message(packed[1], got_fsdp, "x")
    over_core.wait_recv()
    tp_mid[...] = packed[0][...] + got_tp[0][...]
    over_y = message(tp_mid, got_tp[1], "y")
    over_x.wait_recv()
    sums[1][...] = packed[1][...] + got_fsdp[...]
    over_y.wait_recv()
    sums[0][...] = tp_mid[...] + got_tp[1][...]
    new_statistics(places, sums, olds, news, scales)
    scalars_into(scalar_refs[0], shares, places, by_order(final), sums, olds, squares, scales)
    for step, name in enumerate(("core", "y", "x")):
        copy = message(scalar_refs[step], scalar_got[step], name)
        copy.wait_recv()
        scalar_refs[step + 1][...] = scalar_refs[step][...] + scalar_got[step][...]
    state["grad"].wait_recv()
    for copy in small:
        copy.wait_send()
    for copy in exchanged.values():
        copy.wait_send()

    @pl.when(jnp.logical_not(at_end))
    def _():
        for i in numbers:
            across[i].wait_send()
            outwards[i].wait_send()


def close(mine, theirs, sends, others, shares):
    shapes = [m.shape for m in mine]
    count, arrived = len(mine), len(theirs)
    number = len(pieces_of(shapes))
    by_order = [mine[index] for index in (4, 3, 1, 2, 0)]
    d_mine = others[0]
    half, width = d_mine.shape
    row = others[5].shape
    vectors = [(1, size) for size in packed_sizes(by_order)]
    vmem, hbm = pl.BlockSpec(memory_space=pltpu.VMEM), pl.BlockSpec(memory_space=pl.ANY)
    held = [pltpu.VMEM(shape, BF) for shape in shapes]
    f32 = lambda shape: pltpu.VMEM(shape, F32)
    rows = [f32(row)] * 5
    size = sum(m.size for m in mine)
    out_shape = (
        [jax.ShapeDtypeStruct(shape, BF) for shape in shapes]
        + [jax.ShapeDtypeStruct(shape, F32) for shape in vectors * 2]
        + [jax.ShapeDtypeStruct(row, F32), jax.ShapeDtypeStruct((8, 128), F32)]
        + [jax.ShapeDtypeStruct((2 * half, width), F32)]
    )
    out = pl.pallas_call(
        functools.partial(close_kernel, shapes, arrived, shares),
        in_specs=[vmem] * (count + arrived + len(sends) + len(others)),
        out_specs=[vmem] * len(out_shape),
        out_shape=out_shape,
        scratch_shapes=held * 3
        + held[arrived:]
        + [f32(shape) for shape in vectors * 2]
        + [pltpu.VMEM((half, width), BF)] * 3
        + rows * 2
        + [f32(vectors[0])] * 3
        + [f32(vectors[1])]
        + [f32((8, 128))] * 6
        + [pltpu.SemaphoreType.DMA((number,))] * 8
        + [pltpu.SemaphoreType.DMA((16,))] * 2,
        cost_estimate=pl.CostEstimate(flops=4 * size, bytes_accessed=80 * size, transcendentals=0),
        compiler_params=pltpu.CompilerParams(
            vmem_limit_bytes=56 << 20, collective_id=0, has_side_effects=True
        ),
        name="close",
    )(*mine, *theirs, *sends, *others)
    grads = [out[index] for index in (4, 3, 1, 2, 0)]
    return grads, out[5:7], out[7:9], out[9], out[10], out[11]


GAIN_SPANS = ((0, D), (D, D), (2 * D, HEAD_SIZE), (2 * D + HEAD_SIZE, HEAD_SIZE))


def write_kernel(*refs):
    refs = list(refs)
    take = lambda size: [refs.pop(0) for _ in range(size)]
    sources, news, scales = take(5), take(2), take(2)
    gain_grad_ref, total_ref, input_grad_ref, var_ref, gain_ref = take(5)
    whole_outs, step_outs, grad_out = take(4), take(4), take(1)[0]
    stat_outs, gain_outs, rms_ref = take(8), take(12), take(1)[0]
    grads, whole_held, step_held = take(5), take(5), take(5)
    new_var_ref, gain_step_ref, whole_sems, step_sems, load_sems, grad_sem = take(6)
    order = (4, 2, 3, 0, 1)
    loads = [pltpu.make_async_copy(sources[i], grads[i], load_sems.at[i]) for i in range(5)]
    for index in order:
        loads[index].start()
    moved = pltpu.make_async_copy(input_grad_ref, grad_out, grad_sem)
    moved.start()
    places = layout_of(grads)
    whole_views, step_views = out_views(whole_outs), out_views(step_outs)
    factors = gain_parts(
        total_ref, gain_grad_ref, var_ref, gain_ref, new_var_ref, gain_step_ref, rms_ref
    )
    firsts, number = [], 0
    for grad_ref in grads:
        firsts.append(number)
        number += grad_ref.shape[0] // 128

    def tile_copies(index, at, number):
        span = pl.ds(at, 128)
        return (
            pltpu.make_async_copy(
                whole_held[index].at[span, :], whole_views[index](span), whole_sems.at[number]
            ),
            pltpu.make_async_copy(
                step_held[index].at[span, :], step_views[index](span), step_sems.at[number]
            ),
        )

    for index in order:
        loads[index].wait()
        (row_at, row_span), (col_at, col_span) = places[index]
        n_rows, n_cols = grads[index].shape
        right = scales[col_at][:, col_span] * factors[(0, 1, 2, 2, 3)[index]]

        @pl.loop(0, n_rows // 128)
        def _(step):
            at = pl.multiple_of(step * 128, 128)
            start = pl.multiple_of(row_span.start + at, 128)
            left = columns_of(scales[row_at][:, pl.ds(start, 128)], n_cols)
            for first in range(0, n_cols, 128):
                lanes = slice(first, first + 128)
                tile = grads[index][pl.ds(at, 128), lanes].astype(F32)
                whole_held[index][pl.ds(at, 128), lanes] = tile
                step_held[index][pl.ds(at, 128), lanes] = tile * left * right[:, lanes]
            for copy in tile_copies(index, at, firsts[index] + step):
                copy.start()

    spots = [place for pair in places for place in pair]
    del spots[6]
    for out_ref, (at, span) in zip(stat_outs[:5] + stat_outs[6:], spots[:5] + spots[7:]):
        out_ref[...] = news[at][:, span]
    for which, (at, span) in enumerate(spots[5:7]):
        stat_outs[5][which : which + 1, :] = news[at][:, span]
    for source, outs in zip(
        (gain_grad_ref, new_var_ref, gain_step_ref), (gain_outs[:4], gain_outs[4:8], gain_outs[8:])
    ):
        for out_ref, (start, size) in zip(outs, GAIN_SPANS):
            out_ref[...] = source[:, start : start + size]
    for index in order:

        @pl.loop(0, grads[index].shape[0] // 128)
        def _(step):
            at = pl.multiple_of(step * 128, 128)
            for copy in tile_copies(index, at, firsts[index] + step):
                copy.wait()

    moved.wait()


def write_all(grads, news, scales, gain_grads, totals, input_grad, gain_vars, gains):
    vmem, hbm = pl.BlockSpec(memory_space=pltpu.VMEM), pl.BlockSpec(memory_space=pl.ANY)
    spots = [place for pair in layout_of(grads) for place in pair]
    del spots[6]
    writes = write_shapes(grads)
    row = lambda size: jax.ShapeDtypeStruct((1, size), F32)
    out_shape = (
        writes * 2
        + [jax.ShapeDtypeStruct(input_grad.shape, F32)]
        + [row(span.stop - span.start) for _, span in spots[:5]]
        + [jax.ShapeDtypeStruct((2, grads[2].shape[1]), F32)]
        + [row(span.stop - span.start) for _, span in spots[7:]]
        + [row(size) for _, size in GAIN_SPANS] * 3
        + [jax.ShapeDtypeStruct((1, 1), F32)]
    )
    tiles = len(list(tiles_in(grads)))
    held = [pltpu.VMEM(g.shape, F32) for g in grads]
    size = sum(g.size for g in grads)
    out = pl.pallas_call(
        write_kernel,
        in_specs=[hbm] * 5 + [vmem] * 9,
        out_specs=[hbm] * 9 + [vmem] * (len(out_shape) - 9),
        out_shape=out_shape,
        scratch_shapes=[pltpu.VMEM(g.shape, BF) for g in grads]
        + held * 2
        + [pltpu.VMEM(gains.shape, F32)] * 2
        + [pltpu.SemaphoreType.DMA((tiles,))] * 2
        + [pltpu.SemaphoreType.DMA((5,))]
        + [pltpu.SemaphoreType.DMA(())],
        cost_estimate=pl.CostEstimate(
            flops=4 * size, bytes_accessed=10 * size, transcendentals=0
        ),
        compiler_params=params(57 << 20),
        name="write_all",
    )(*grads, *news, *scales, gain_grads, totals, input_grad, gain_vars, gains)
    return out[:4], out[4:8], out[8], out[9:17], out[17:29], out[29]


def norm_in_kernel(order_ref, x_ref, gain_ref, low_ref, high_ref, turned_ref):
    values = x_ref[...].astype(F32)
    inv = lax.rsqrt(jnp.mean(values * values, axis=-1, keepdims=True) + EPS)
    normed = (values * inv * gain_ref[...]).astype(BF)
    split = values.shape[1] // 2
    swapped = order_ref[0] != 0

    @pl.when(swapped)
    def _():
        low_ref[...], high_ref[...] = normed[:, split:], normed[:, :split]
        turned_ref[:, :split] = x_ref[:, split:]
        turned_ref[:, split:] = x_ref[:, :split]

    @pl.when(jnp.logical_not(swapped))
    def _():
        low_ref[...], high_ref[...] = normed[:, :split], normed[:, split:]
        turned_ref[...] = x_ref[...]


def norm_in(order, values, gain):
    rows, cols = values.shape
    tile = pl.BlockSpec((128, cols), lambda i: (i, 0))
    half = pl.BlockSpec((128, cols // 2), lambda i: (i, 0))
    return pl.pallas_call(
        norm_in_kernel,
        grid=(rows // 128,),
        in_specs=[
            pl.BlockSpec(memory_space=pltpu.SMEM),
            tile,
            pl.BlockSpec((1, cols), lambda i: (0, 0)),
        ],
        out_specs=[half, half, tile],
        out_shape=[jax.ShapeDtypeStruct((rows, cols // 2), BF)] * 2
        + [jax.ShapeDtypeStruct(values.shape, BF)],
        cost_estimate=pl.CostEstimate(
            flops=6 * values.size, bytes_accessed=6 * values.size, transcendentals=0
        ),
        compiler_params=params(8 << 20),
        name="norm_in",
    )(order, values, gain.reshape(1, cols))


def turned_head(rows, gain, cos_t, sin_t):
    half = HEAD_SIZE // 2
    inv = lax.rsqrt(jnp.mean(rows * rows, axis=0, keepdims=True) + EPS)
    normed = rows * inv * gain
    low, high = normed[:half], normed[half:]
    return jnp.concatenate([low * cos_t - high * sin_t, high * cos_t + low * sin_t], axis=0)


def queries_kernel(raw_ref, cos_ref, sin_ref, gain_ref, q_ref):
    turned = turned_head(raw_ref[...], gain_ref[...], cos_ref[...], sin_ref[...])
    scale = 1.0 / math.sqrt(HEAD_SIZE)
    q_ref[...] = (turned.astype(BF).astype(F32) * scale).astype(BF)


def keys_kernel(raw_ref, cos_ref, sin_ref, gain_ref, kv_ref):
    turned = turned_head(raw_ref[:HEAD_SIZE, :], gain_ref[...], cos_ref[...], sin_ref[...])
    kv_ref[:HEAD_SIZE, :] = turned.astype(BF)
    kv_ref[HEAD_SIZE:, :] = raw_ref[HEAD_SIZE:, :].astype(BF)


def prep_call(kernel, size, raw_t, cos_t, sin_t, gain):
    rows, tokens = raw_t.shape
    half = HEAD_SIZE // 2
    fixed = lambda g: (0, 0)
    return pl.pallas_call(
        kernel,
        grid=(rows // size,),
        in_specs=[
            pl.BlockSpec((size, tokens), lambda g: (g, 0)),
            pl.BlockSpec((half, tokens), fixed),
            pl.BlockSpec((half, tokens), fixed),
            pl.BlockSpec((HEAD_SIZE, 1), fixed),
        ],
        out_specs=pl.BlockSpec((size, tokens), lambda g: (g, 0)),
        out_shape=jax.ShapeDtypeStruct(raw_t.shape, BF),
        cost_estimate=pl.CostEstimate(
            flops=20 * rows * tokens, bytes_accessed=6 * rows * tokens, transcendentals=0
        ),
        compiler_params=params(6 << 20),
        name="prep",
    )(raw_t, cos_t, sin_t, gain)


prep_queries = functools.partial(prep_call, queries_kernel, HEAD_SIZE)
prep_keys = functools.partial(prep_call, keys_kernel, 2 * HEAD_SIZE)


def prep_back_kernel(parts, *refs):
    raw_q_ref, raw_kv_ref, cos_ref, sin_ref, gq_ref, gk_ref, dq_ref = refs[:7]
    dkv_refs = refs[7 : 7 + parts]
    out_q_ref, out_kv_ref, sum_q_ref, sum_k_ref = refs[7 + parts :]
    half = HEAD_SIZE // 2
    cos_t, sin_t = cos_ref[...], sin_ref[...]
    d_kv = dkv_refs[0][...]
    for ref in dkv_refs[1:]:
        d_kv = d_kv + ref[...].astype(F32)

    @pl.when(pl.program_id(0) == 0)
    def _():
        sum_q_ref[...] = jnp.zeros_like(sum_q_ref)
        sum_k_ref[...] = jnp.zeros_like(sum_k_ref)

    for piece in range(GROUP + 1):
        base = piece * HEAD_SIZE
        if piece < GROUP:
            rows = raw_q_ref[base : base + HEAD_SIZE, :]
            grad = dq_ref[base : base + HEAD_SIZE, :] * (1.0 / math.sqrt(HEAD_SIZE))
            gain, sum_ref = gq_ref[...], sum_q_ref
        else:
            rows = raw_kv_ref[:HEAD_SIZE, :]
            grad = d_kv[:HEAD_SIZE]
            gain, sum_ref = gk_ref[...], sum_k_ref
        inv = lax.rsqrt(jnp.mean(rows * rows, axis=0, keepdims=True) + EPS)
        unit = rows * inv
        low, high = grad[:half], grad[half:]
        turned = jnp.concatenate([low * cos_t + high * sin_t, high * cos_t - low * sin_t], axis=0)
        sum_ref[...] += jnp.sum(turned * unit, axis=1, keepdims=True)
        scaled = turned * gain
        mean = jnp.mean(scaled * unit, axis=0, keepdims=True)
        result = ((scaled - unit * mean) * inv).astype(BF)
        if piece < GROUP:
            out_q_ref[base : base + HEAD_SIZE, :] = result
        else:
            out_kv_ref[:HEAD_SIZE, :] = result
    out_kv_ref[HEAD_SIZE:, :] = d_kv[HEAD_SIZE:].astype(BF)


def prep_back(raw_q_t, raw_kv_t, cos_t, sin_t, gain_q, gain_k, d_q, d_kv_parts):
    tokens = raw_q_t.shape[1]
    groups = raw_kv_t.shape[0] // (2 * HEAD_SIZE)
    rows = raw_q_t.shape[0] + raw_kv_t.shape[0]
    half = HEAD_SIZE // 2
    fixed = lambda g: (0, 0)
    block = lambda size: pl.BlockSpec((size, tokens), lambda g: (g, 0))
    return pl.pallas_call(
        functools.partial(prep_back_kernel, len(d_kv_parts)),
        grid=(groups,),
        in_specs=[
            block(GROUP * HEAD_SIZE),
            block(2 * HEAD_SIZE),
            pl.BlockSpec((half, tokens), fixed),
            pl.BlockSpec((half, tokens), fixed),
            pl.BlockSpec((HEAD_SIZE, 1), fixed),
            pl.BlockSpec((HEAD_SIZE, 1), fixed),
            block(GROUP * HEAD_SIZE),
        ]
        + [block(2 * HEAD_SIZE)] * len(d_kv_parts),
        out_specs=[
            block(GROUP * HEAD_SIZE),
            block(2 * HEAD_SIZE),
            pl.BlockSpec((HEAD_SIZE, 128), fixed),
            pl.BlockSpec((HEAD_SIZE, 128), fixed),
        ],
        out_shape=[
            jax.ShapeDtypeStruct(raw_q_t.shape, BF),
            jax.ShapeDtypeStruct(raw_kv_t.shape, BF),
            jax.ShapeDtypeStruct((HEAD_SIZE, 128), F32),
            jax.ShapeDtypeStruct((HEAD_SIZE, 128), F32),
        ],
        cost_estimate=pl.CostEstimate(
            flops=30 * rows * tokens, bytes_accessed=9 * rows * tokens, transcendentals=0
        ),
        compiler_params=params(8 << 20),
        name="prep_back",
    )(raw_q_t, raw_kv_t, cos_t, sin_t, gain_q, gain_k, d_q, *d_kv_parts)


def over_tiles(diagonal, tokens, body):
    for key_start in range(0, tokens, KEY_TILE):
        body(key_start, key_start if diagonal else 0)


def tile_probs(kv_ref, query, key_start, query_start, valid, diagonal):
    keys = kv_ref[:HEAD_SIZE, pl.ds(key_start, KEY_TILE)]
    scores = mm(keys, query, 0, 0)
    key_index = key_start + lax.broadcasted_iota(jnp.int32, scores.shape, 0)
    visible = key_index < valid
    if diagonal:
        query_index = query_start + lax.broadcasted_iota(jnp.int32, scores.shape, 1)
        visible = visible & (key_index <= query_index)
    return keys, visible, jnp.exp(scores)


def attend_kernel(diagonal, valid_ref, q_ref, kv_ref, *refs):
    if diagonal:
        acc_ref, sum_ref = refs
        acc_ref[...] = jnp.zeros_like(acc_ref)
        sum_ref[...] = jnp.zeros_like(sum_ref)
    else:
        acc_in_ref, sum_in_ref, acc_ref, sum_ref = refs
        acc_ref[...] = acc_in_ref[...]
        sum_ref[...] = sum_in_ref[...]
    valid = valid_ref[0]
    tokens = q_ref.shape[1]

    @pl.when(valid > 0)
    def _():
        def tile(key_start, query_start):
            query = q_ref[:, query_start:]
            _, visible, raised = tile_probs(kv_ref, query, key_start, query_start, valid, diagonal)
            probs = jnp.where(visible, raised, 0.0)
            sum_ref[:, query_start:] += jnp.sum(probs, axis=0, keepdims=True)
            values = kv_ref[HEAD_SIZE:, pl.ds(key_start, KEY_TILE)]
            acc_ref[:, query_start:] += mm(values, probs.astype(BF), 1, 0)

        over_tiles(diagonal, tokens, tile)


def attend(diagonal, valid, q_t, kv_t, state):
    rows, tokens = q_t.shape
    heads = rows // HEAD_SIZE
    per_head = pl.BlockSpec((HEAD_SIZE, tokens), lambda h: (h, 0))
    sums = pl.BlockSpec((8, tokens), lambda h: (h, 0))
    carried = [] if diagonal else [per_head, sums]
    return pl.pallas_call(
        functools.partial(attend_kernel, diagonal),
        grid=(heads,),
        in_specs=[
            pl.BlockSpec(memory_space=pltpu.SMEM),
            per_head,
            pl.BlockSpec((2 * HEAD_SIZE, tokens), lambda h: (h // GROUP, 0)),
        ]
        + carried,
        out_specs=[per_head, sums],
        out_shape=[
            jax.ShapeDtypeStruct((rows, tokens), F32),
            jax.ShapeDtypeStruct((heads * 8, tokens), F32),
        ],
        input_output_aliases={} if diagonal else {3: 0, 4: 1},
        cost_estimate=pl.CostEstimate(
            flops=4 * rows * tokens * tokens,
            bytes_accessed=10 * rows * tokens,
            transcendentals=heads * tokens * tokens,
        ),
        compiler_params=params(8 << 20),
        name="attend",
    )(valid, q_t, kv_t, *state)


def attend_back_kernel(diagonal, first, valid_ref, q_ref, kv_ref, out_ref, sum_ref, do_ref, *refs):
    if first:
        dq_ref, dkv_ref, dkv_acc = refs
        dq_ref[...] = jnp.zeros_like(dq_ref)
    else:
        dq_in_ref, dq_ref, dkv_ref, dkv_acc = refs
        dq_ref[...] = dq_in_ref[...]
    head = pl.program_id(0)
    valid = valid_ref[0]
    tokens = q_ref.shape[1]

    @pl.when(head % GROUP == 0)
    def _():
        dkv_acc[...] = jnp.zeros_like(dkv_acc)

    @pl.when(valid > 0)
    def _():
        inverse = 1.0 / sum_ref[0:1, :]
        delta = jnp.sum(do_ref[...].astype(F32) * out_ref[...], axis=0, keepdims=True)

        def tile(key_start, query_start):
            query = q_ref[:, query_start:]
            grads = do_ref[:, query_start:]
            keys, visible, raised = tile_probs(
                kv_ref, query, key_start, query_start, valid, diagonal
            )
            probs = jnp.where(visible, raised * inverse[:, query_start:], 0.0)
            span = pl.ds(key_start, KEY_TILE)
            values = kv_ref[HEAD_SIZE:, span]
            d_probs = mm(values, grads, 0, 0)
            d_scores = (probs * (d_probs - delta[:, query_start:])).astype(BF)
            dq_ref[:, query_start:] += mm(keys, d_scores, 1, 0)
            dkv_acc[:HEAD_SIZE, span] += mm(query, d_scores, 1, 1)
            dkv_acc[HEAD_SIZE:, span] += mm(grads, probs.astype(BF), 1, 1)

        over_tiles(diagonal, tokens, tile)

    @pl.when(head % GROUP == GROUP - 1)
    def _():
        dkv_ref[...] = dkv_acc[...].astype(dkv_ref.dtype)


def attend_back(diagonal, valid, q_t, kv_t, out_t, sums, d_out_t, d_q):
    rows, tokens = q_t.shape
    heads = rows // HEAD_SIZE
    first = d_q is None
    per_head = pl.BlockSpec((HEAD_SIZE, tokens), lambda h: (h, 0))
    per_group = pl.BlockSpec((2 * HEAD_SIZE, tokens), lambda h: (h // GROUP, 0))
    return pl.pallas_call(
        functools.partial(attend_back_kernel, diagonal, first),
        grid=(heads,),
        in_specs=[
            pl.BlockSpec(memory_space=pltpu.SMEM),
            per_head,
            per_group,
            per_head,
            pl.BlockSpec((8, tokens), lambda h: (h, 0)),
            per_head,
        ]
        + ([] if first else [per_head]),
        out_specs=[per_head, per_group],
        out_shape=[
            jax.ShapeDtypeStruct((rows, tokens), F32),
            jax.ShapeDtypeStruct(kv_t.shape, F32 if diagonal else BF),
        ],
        scratch_shapes=[pltpu.VMEM((2 * HEAD_SIZE, tokens), F32)],
        input_output_aliases={} if first else {6: 0},
        cost_estimate=pl.CostEstimate(
            flops=10 * rows * tokens * tokens,
            bytes_accessed=14 * rows * tokens,
            transcendentals=heads * tokens * tokens,
        ),
        compiler_params=params(8 << 20),
        name="attend_back",
    )(valid, q_t, kv_t, out_t, sums, d_out_t, *([] if first else [d_q]))


def unit_rows(values):
    inv = lax.rsqrt(jnp.mean(values * values, axis=-1, keepdims=True) + EPS)
    return values * inv, inv


def norm_back(unit, inv, gain, grad):
    scaled = grad * gain
    return (scaled - unit * jnp.mean(scaled * unit, axis=-1, keepdims=True)) * inv


def kept(value):
    return lax.optimization_barrier(value)


def on_device(
    sizes,
    block_input,
    cotangent,
    seq_lengths,
    positions,
    w_qkv,
    w_out,
    w_gate_up,
    w_down,
    gain_attn,
    gain_ffn,
    gain_query,
    gain_key,
    row_qkv_old,
    col_qkv_old,
    row_out_old,
    col_out_old,
    row_gate_up_old,
    col_gate_up_old,
    row_down_old,
    col_down_old,
    var_attn_old,
    var_ffn_old,
    var_query_old,
    var_key_old,
):
    n_fsdp, n_ctx, n_tp = sizes["fsdp"], sizes["ctx"], sizes["tp"]
    paired = n_fsdp == 2
    me_f, me_z, me_t = (lax.axis_index(name) for name in ("fsdp", "ctx", "tp"))
    tokens = block_input.shape[1]
    half = tokens // 2
    mine_row = (me_t % 2) * half
    other_row = half - mine_row

    def turn(values):
        if not paired:
            return values
        size = values.shape[-1] // 2
        swapped = jnp.concatenate([values[..., size:], values[..., :size]], axis=-1)
        return jnp.where(me_f == 0, values, swapped)

    def over(values, axis, pairs):
        return lax.ppermute(values, axis, pairs)

    def to_core(values):
        return over(values, "tp", [(i, i ^ 1) for i in range(n_tp)])

    def to_pair(values):
        return over(values, "fsdp", [(0, 1), (1, 0)])

    def gather_weight(shard, axis):
        if not paired:
            return lax.all_gather(shard, "fsdp", axis=axis, tiled=True)
        return jnp.concatenate([shard, to_pair(shard)], axis=axis)

    routed_by_ctx = paired and n_ctx % 2 == 0

    def first_half(shard):
        if not routed_by_ctx:
            return None
        size = shard.shape[0] // 2
        return to_pair(lax.dynamic_slice_in_dim(shard, me_z % 2 * size, size, 0))

    def second_half(shard, direct, axis):
        if not routed_by_ctx:
            return gather_weight(shard, axis)
        routed = over(direct, "ctx", [(i, i ^ 1) for i in range(n_ctx)])
        odd = me_z % 2
        first = jnp.where(odd == 0, direct, routed)
        second = jnp.where(odd == 0, routed, direct)
        other = jnp.concatenate([first, second], axis=0)
        return jnp.concatenate([shard, other], axis=axis)

    def sum_tp(mine, other_low):
        total = mine + to_core(other_low).astype(F32)
        step = 2
        while step < n_tp:
            low = kept(total.astype(BF))
            pairs = [(i, i ^ step) for i in range(n_tp)]
            moved = over(low, "tp", pairs)
            total = low.astype(F32) + moved.astype(F32)
            step *= 2
        return total

    def whole_rows(values):
        other = to_core(values)
        first = jnp.where(mine_row == 0, values, other)
        second = jnp.where(mine_row == 0, other, values)
        return jnp.concatenate([first, second], axis=0)

    def rows_of(values, start):
        return lax.dynamic_slice_in_dim(values, start, half, 0)

    def after(value, *tokens):
        return lax.optimization_barrier((value,) + tokens)[0]

    def shares_of(make, axis):
        if paired:
            return make(0).astype(BF), make(1).astype(BF)
        whole = make(None)
        return (
            lax.psum_scatter(whole, "fsdp", scatter_dimension=axis, tiled=True).astype(BF),
            None,
        )

    def sum_over_tp(values):
        step = 1
        while step < n_tp:
            values = values + over(values, "tp", [(i, i ^ step) for i in range(n_tp)])
            step *= 2
        return values

    def sum_over_fsdp(values):
        return values + to_pair(values) if paired else lax.psum(values, "fsdp")

    def sum_over_ctx(values):
        step = 1
        while step < n_ctx:
            values = values + over(values, "ctx", [(i, i ^ step) for i in range(n_ctx)])
            step *= 2
        return values

    def sum_all(values):
        return sum_over_ctx(sum_over_fsdp(sum_over_tp(values)))

    def part_of(values, part):
        if part is None:
            return values
        size = values.shape[-1] // 2
        return values[..., part * size : (part + 1) * size]

    groups = w_qkv.shape[1] // LANES
    split_at = GROUP * HEAD_SIZE
    q_spans = [(g * LANES, split_at) for g in range(groups)]
    kv_spans = [(g * LANES + split_at, 2 * HEAD_SIZE) for g in range(groups)]
    shard_q, shard_kv, squares_qkv = cast(w_qkv, [q_spans, kv_spans])
    if paired:
        other_kv, other_q = to_pair(shard_kv), to_pair(shard_q)
    else:
        full_kv, full_q = gather_weight(shard_kv, 0), gather_weight(shard_q, 0)

    order = (me_f if paired else me_f * 0).astype(jnp.int32).reshape(1)
    *h_halves, turned_input = norm_in(order, block_input[0], gain_attn)
    h_one = None if paired else jnp.concatenate(h_halves, axis=1)
    inputs32 = turned_input.astype(F32)
    grad_rows = turn(cotangent[0])
    gain_a, gain_f = turn(gain_attn), turn(gain_ffn)
    freq = jnp.exp(
        jnp.arange(HEAD_SIZE // 2, dtype=F32) * (-2.0 * math.log(THETA) / HEAD_SIZE)
    )
    angle = freq[:, None] * positions[0].astype(F32)[None, :]
    cos_t, sin_t = jnp.cos(angle), jnp.sin(angle)
    gain_q, gain_k = gain_query[:, None], gain_key[:, None]

    def from_features(mine, other, full):
        if not paired:
            return mm(full, h_one, 0, 1)
        return mm(mine, h_halves[0], 0, 1) + mm(other, h_halves[1], 0, 1)

    shard_out, squares_out = cast(w_out)
    full_out = gather_weight(shard_out, 1)
    raw_kv_t = from_features(shard_kv, other_kv, None) if paired else from_features(None, None, full_kv)
    kv_t = prep_keys(raw_kv_t, cos_t, sin_t, gain_k)
    shard_gate, shard_up, squares_gate_up = cast_pair(w_gate_up)
    direct_gate, direct_up = first_half(shard_gate), first_half(shard_up)
    raw_q_t = (
        from_features(shard_q, other_q, None) if paired else from_features(None, None, full_q)
    )
    q_t = prep_queries(raw_q_t, cos_t, sin_t, gain_q)

    shard_down, squares_down = cast(w_down)
    full_down = gather_weight(shard_down, 1)
    length = seq_lengths[0]
    kv_blocks, valids = [], []
    for back in range(n_ctx):
        moved = kv_t
        if back > 0:
            moved = over(kv_t, "ctx", [(i, i + back) for i in range(n_ctx - back)])
        kv_blocks.append(moved)
        count = jnp.clip(length - (me_z - back) * tokens, 0, tokens)
        valids.append(jnp.where(me_z >= back, count, 0).astype(jnp.int32).reshape(1))
    state = []
    for back in range(n_ctx):
        query = q_t
        if routed_by_ctx and back == 2:
            query = after(q_t, direct_gate)
        state = attend(back == 0, valids[back], query, kv_blocks[back], state)
        if back == min(1, n_ctx - 1):
            full_gate = second_half(shard_gate, direct_gate, 0)
        if back == min(2, n_ctx - 1):
            full_up = second_half(shard_up, direct_up, 0)
    acc_t, sums = state
    heads = acc_t.shape[0] // HEAD_SIZE
    inverse = (1.0 / sums.reshape(heads, 8, tokens)[:, :1, :])
    out_t = (acc_t.reshape(heads, HEAD_SIZE, tokens) * inverse).reshape(acc_t.shape)
    attn_t = kept(out_t.astype(BF))

    def cols_of(values, start):
        return lax.dynamic_slice_in_dim(values, start, half, 1)

    attn_other = mm(cols_of(attn_t, other_row), full_out, 0, 0).astype(BF)
    attn_mine = mm(cols_of(attn_t, mine_row), full_out, 0, 0)
    resid = rows_of(inputs32, mine_row) + sum_tp(attn_mine, attn_other)
    unit_two, inv_two = unit_rows(resid)
    h_two = whole_rows((unit_two * gain_f).astype(BF))

    d_hidden = mm(grad_rows, full_down, 1, 1)
    gate, up = mm(h_two, full_gate, 1, 0), mm(h_two, full_up, 1, 0)
    gate_sigmoid = 1.0 / (1.0 + jnp.exp(-gate))
    gate_silu = gate * gate_sigmoid
    hidden = (gate_silu * up).astype(BF)
    slope = gate_sigmoid * (1.0 + gate * (1.0 - gate_sigmoid))
    d_gate = (d_hidden * up * slope).astype(BF)
    d_up = (d_hidden * gate_silu).astype(BF)

    def d_two_of(start):
        return mm(rows_of(d_gate, start), full_gate, 1, 1) + mm(rows_of(d_up, start), full_up, 1, 1)

    d_two = sum_tp(d_two_of(mine_row), d_two_of(other_row).astype(BF))
    down_mine, down_send = shares_of(lambda part: mm(hidden, part_of(grad_rows, part), 0, 0), 1)
    gate_mine, gate_send = shares_of(lambda part: mm(part_of(h_two, part), d_gate, 0, 0), 0)
    up_mine, up_send = shares_of(lambda part: mm(part_of(h_two, part), d_up, 0, 0), 0)
    arrived = []
    if paired:
        named = (down_send, gate_send)
        arrived = [to_pair(send) for send in named]
    d_resid = rows_of(grad_rows, mine_row).astype(F32) + norm_back(unit_two, inv_two, gain_f, d_two)
    d_attn = whole_rows(d_resid.astype(BF))

    d_heads_t = mm(full_out, d_attn, 1, 1).astype(BF)
    late_hidden = hidden
    ffn_other = mm(rows_of(late_hidden, other_row), full_down, 1, 0).astype(BF)
    ffn_mine = mm(rows_of(late_hidden, mine_row), full_down, 1, 0)
    block_output = turn(whole_rows(resid + sum_tp(ffn_mine, ffn_other)))

    d_q = None
    d_kv_parts = [None] * n_ctx
    for back in reversed(range(n_ctx)):
        d_q, d_kv = attend_back(
            back == 0, valids[back], q_t, kv_blocks[back], out_t, sums, d_heads_t, d_q
        )
        if back > 0:
            d_kv = over(d_kv, "ctx", [(i, i - back) for i in range(back, n_ctx)])
        d_kv_parts[back] = d_kv
    olds = [
        jnp.concatenate([jnp.pad(after(v, d_q), (0, padded(v.size) - v.size)) for v in vectors]).reshape(1, -1)
        for vectors in (
            (row_qkv_old, row_gate_up_old, col_out_old, col_down_old),
            (col_qkv_old, col_gate_up_old[0], col_gate_up_old[1], row_out_old, row_down_old),
        )
    ]
    row_of = lambda vectors: jnp.concatenate(vectors).reshape(1, 2 * D + 2 * HEAD_SIZE)
    gain_vars = row_of([after(v, d_q) for v in (var_attn_old, var_ffn_old, var_query_old, var_key_old)])
    gains_old = row_of([after(v, d_q) for v in (gain_attn, gain_ffn, gain_query, gain_key)])

    part_ffn_gain = jnp.sum(after(d_two, d_q) * unit_two, axis=0)
    out_mine, out_send = shares_of(lambda part: mm(attn_t, part_of(d_attn, part), 1, 0), 1)
    d_raw_q_t, d_raw_kv_t, sum_q, sum_k = prep_back(
        raw_q_t, raw_kv_t, cos_t, sin_t, gain_q, gain_k, d_q, d_kv_parts
    )

    def joined(q, kv):
        pieces = []
        for g in range(groups):
            pieces += [q[:, g * split_at : (g + 1) * split_at]]
            pieces += [kv[:, g * 2 * HEAD_SIZE : (g + 1) * 2 * HEAD_SIZE]]
        return jnp.concatenate(pieces, axis=1)

    def qkv_grad(part):
        rows = h_one if part is None else h_halves[part]
        return joined(mm(rows, d_raw_q_t, 0, 1), mm(rows, d_raw_kv_t, 0, 1))

    qkv_mine, qkv_send = shares_of(qkv_grad, 0)

    if paired:
        full_kv = jnp.concatenate([after(shard_kv, d_q), other_kv], axis=0)
        full_q = jnp.concatenate([after(shard_q, d_q), other_q], axis=0)

    def d_one_of(start):
        return mm(cols_of(d_raw_kv_t, start), full_kv, 0, 1) + mm(
            cols_of(d_raw_q_t, start), full_q, 0, 1
        )

    mine = [down_mine, gate_mine, up_mine, out_mine, qkv_mine]
    squares = [squares_qkv, squares_out, squares_gate_up, squares_down]
    shares = (1.0 / n_tp, 1.0 / n_fsdp)
    share = 2.0 / n_tp
    row_parts = [turn(part_ffn_gain) * share, sum_q[:, 0], sum_k[:, 0]]
    if paired and n_ctx == 4 and n_tp == 4:
        others = [
            d_one_of(mine_row),
            d_one_of(other_row).astype(BF),
            d_resid,
            rows_of(after(turned_input, d_q), mine_row),
            gain_a.reshape(1, D),
            row_of([jnp.zeros((D,), F32)] + row_parts),
        ]
        grads, news, scales, gain_grads, totals, input_grad = close(
            mine, arrived, [up_send, out_send, qkv_send], others + olds + squares, shares
        )
        whole_grads, steps, input_grad, stat_rows, gain_rows, rms = write_all(
            grads, news, scales, gain_grads, totals, input_grad, gain_vars, gains_old
        )
        stat_list = [value if at == 5 else value[0] for at, value in enumerate(stat_rows)]
        gain_list = [value[0] for value in gain_rows]
    else:
        d_one = sum_tp(d_one_of(mine_row), d_one_of(other_row).astype(BF))
        unit_half, inv_half = unit_rows(rows_of(inputs32, mine_row))
        part_attn_gain = jnp.sum(d_one * unit_half, axis=0)
        input_grad = turn(whole_rows(d_resid + norm_back(unit_half, inv_half, gain_a, d_one)))
        gain_grads = sum_all(row_of([turn(part_attn_gain) * share] + row_parts))
        if n_ctx == 4:
            down, gate_sum, up_sum, out_sum, qkv_sum = line_sums(
                mine, arrived, [up_send, out_send, qkv_send] if paired else []
            )
        else:
            theirs = arrived + [to_pair(send) for send in (up_send, out_send, qkv_send)] if paired else []
            if paired:
                mine = [left.astype(F32) + right.astype(F32) for left, right in zip(mine, theirs)]
            down, gate_sum, up_sum, out_sum, qkv_sum = (
                kept(lax.psum(part.astype(F32), "ctx").astype(BF)) for part in mine
            )
        grads = [qkv_sum, out_sum, gate_sum, up_sum, down]
        by_tp, by_fsdp = stats(grads)
        sums = [sum_over_tp(by_tp), sum_over_fsdp(by_fsdp)]
        whole_grads, news, scales, scalars = scaled(shares, grads, sums, olds, squares)
        totals = lax.psum(scalars, ("fsdp", "tp"))
        steps, new_vars, gain_steps, rms = finish(
            grads, scales, totals, gain_grads, gain_vars, gains_old
        )

        places = layout_of(grads)
        spots = [place for pair in places for place in pair]
        del spots[6]
        stat_list = [news[at][0, span] for at, span in spots]
        stat_list[5:7] = [jnp.stack(stat_list[5:7])]
        gain_list = [
            row[0, start : start + size]
            for row in (gain_grads, new_vars, gain_steps)
            for start, size in GAIN_SPANS
        ]
    row_qkv, col_qkv, row_out, col_out, row_gu, col_gate_up, row_down, col_down = stat_list
    return (
        block_output[None],
        input_grad[None],
        *whole_grads,
        *gain_list[:4],
        row_qkv,
        col_qkv,
        row_out,
        col_out,
        row_gu,
        col_gate_up,
        row_down,
        col_down,
        *gain_list[4:8],
        *steps,
        *gain_list[8:],
        rms[:1, :1].reshape(()),
    )


def solution(mesh):
    tokens, vector = P("fsdp", "ctx", None), P()
    by_f, by_t = P("fsdp"), P("tp")
    w_specs = (P("fsdp", "tp"), P("tp", "fsdp"), P("fsdp", None, "tp"), P("tp", "fsdp"))
    stats = (by_f, by_t, by_t, by_f, by_f, P(None, "tp"), by_t, by_f) + (vector,) * 4

    def body(*args):
        return on_device(dict(mesh.shape), *args)

    return jax.shard_map(
        body,
        mesh=mesh,
        in_specs=(tokens, tokens, by_f, P("fsdp", "ctx")) + w_specs + (vector,) * 4 + stats,
        out_specs=(tokens, tokens)
        + w_specs
        + (vector,) * 4
        + stats
        + w_specs
        + (vector,) * 4
        + (vector,),
        check_vma=False,
    )
```
